32 devices in a mesh: gx: 4 (over z), gy: 2 (over y), gz: 4 (over x, core).
Axes of the slice: x: 2, y: 2, z: 4, core: 2. Of those that a mesh axis runs over, the one named last changes fastest.
Arguments:
- iterate: float32 [32, 32, 512], P('gx', 'gy', 'gz'), may hold values from -6 to 6
- source: float32 [32, 32, 512], P('gx', 'gy', 'gz'), may hold values from -6 to 6
- reaction: float32 [32, 32, 512], P('gx', 'gy', 'gz'), may hold values from 0.05 to 1
- trial_powers: int32 [4], replicated, may hold values from 0 to 5
Outputs:
- newton_dir: float32 [32, 32, 512], P('gx', 'gy', 'gz')
- remnant: float32 [32, 32, 512], P('gx', 'gy', 'gz')
- layer_energies: float32 [4, 32], P(None, 'gx')
- energies: float32 [4], replicated
The draws below stay inside these ranges and needn't reach their ends.
Inputs may be any that keep to these rules, and one draw needn't show every extreme that they name: `trial_powers`: trial k takes the step length 2 to the power minus entry k.
All inputs are finite; a program needn't handle non-finite values.
Results may differ from the reference program's by a relative error of at most 0.0003.
Values sent between devices are 32-bit elements; how exact they have to be, the bound alone decides.
A program may use at most 128 MiB of HBM per device.

```python
import math
import jax
import jax.numpy as jnp
from jax import lax

ITERS = 4
LEVELS = 4
TRIALS = 4
NX = 32
NY = 32
NZ = 512


def place_ends(array, rng, smallest, high):
    longest = array.shape.index(max(array.shape))
    spots = []
    for shift in (0, 1):
        where = [jax.random.randint(jax.random.fold_in(rng, axis), (), 0, length) for axis, length in enumerate(array.shape)]
        where[longest] = (where[longest] + shift) % array.shape[longest]
        spots.append(tuple(where))
    return array.at[spots[0]].set(smallest).at[spots[1]].set(high)


def level_of(key, extent, split, smallest, largest):
    def one(axis_at, shards_of):
        draws = jax.random.uniform(jax.random.fold_in(jax.random.fold_in(key, 6), axis_at), (shards_of,), jnp.float32, smallest / len(split), largest / len(split))
        return jnp.repeat(jnp.exp(draws), extent[axis_at] // shards_of).reshape((-1,) + (1,) * (len(extent) - axis_at - 1))

    loudness = one(*split[0])
    for cut in split[1:]:
        loudness = loudness * one(*cut)
    return loudness


def noise(rng, shape, spread, limit, split=(), kind=jnp.bfloat16):
    loudness = level_of(rng, shape, split, -0.22, 0.18) if split else 1.0
    entries = jax.random.normal(rng, shape, jnp.float32) * spread * loudness
    return jnp.minimum(jnp.maximum(entries, -limit), limit).astype(kind)


def setup_inputs(seed: int = 0) -> dict:
    key_list = jax.random.split(jax.random.key(seed), 5)
    return {
        "iterate": noise(key_list[0], (NX, NY, NZ), 1.0, 6.0, ((0, 4), (1, 2), (2, 4)), jnp.float32),
        "source": noise(key_list[1], (NX, NY, NZ), 1.0, 6.0, ((0, 4), (1, 2), (2, 4)), jnp.float32),
        "reaction": jnp.clip(jnp.exp(math.log(1.0) - 2.9957323 * jax.random.uniform(key_list[2], (NX, NY, NZ), jnp.float32) ** level_of(key_list[2], (NX, NY, NZ), ((0, 4), (1, 2), (2, 4)), -0.2, 0.2)), 0.05, 1.0),
        "trial_powers": place_ends(jax.random.randint(key_list[3], (TRIALS,), 0, 6), jax.random.fold_in(key_list[3], 1), 0, 5).astype(jnp.int32),
    }


cheb_mid = 1.15
cheb_half = 0.85

def differences(padded):
    along_x = padded[1:, 1:-1, 1:-1] - padded[:-1, 1:-1, 1:-1]
    along_y = padded[1:-1, 1:, 1:-1] - padded[1:-1, :-1, 1:-1]
    along_z = padded[1:-1, 1:-1, 1:] - padded[1:-1, 1:-1, :-1]
    return (along_x, along_y, along_z)

def stiffness(gradient):
    square = gradient * gradient
    return (1.0 + 2.0 * square) / jnp.sqrt(1.0 + square)

def fluxes(gradient):
    return gradient * jnp.sqrt(1.0 + gradient * gradient)

def face_energy(gradient):
    square = 1.0 + gradient * gradient
    return (square * jnp.sqrt(square) - 1.0) / 3.0

def divergence(face_flows):
    return face_flows[0][1:] - face_flows[0][:-1] + (face_flows[1][:, 1:] - face_flows[1][:, :-1]) + (face_flows[2][:, :, 1:] - face_flows[2][:, :, :-1])

def apply_operator(padded, weights, reaction):
    centre = padded[1:-1, 1:-1, 1:-1]
    gradient = differences(padded)
    face_flows = tuple((w * s for w, s in zip(weights, gradient)))
    return reaction * centre - divergence(face_flows)

def diagonal_of(weights, reaction):
    weight_x, weight_y, weight_z = weights
    return reaction + weight_x[1:] + weight_x[:-1] + weight_y[:, 1:] + weight_y[:, :-1] + weight_z[:, :, 1:] + weight_z[:, :, :-1]

def smooth(remnant, inverse, degree, operate):
    cheb_sigma = cheb_mid / cheb_half
    cheb_rho = 1.0 / cheb_sigma
    update = inverse * remnant / cheb_mid
    summed = update
    for sweep_idx in range(1, degree):
        remnant = remnant - operate(update)
        cheb_next = 1.0 / (2.0 * cheb_sigma - cheb_rho)
        update = cheb_next * cheb_rho * update + 2.0 * cheb_next / cheb_half * inverse * remnant
        summed = summed + update
        cheb_rho = cheb_next
    return (summed, remnant, update)

def pair_sum(values, axis_pos):
    old_shape = values.shape
    new_shape = old_shape[:axis_pos] + (old_shape[axis_pos] // 2, 2) + old_shape[axis_pos + 1:]
    return lax.optimization_barrier(jnp.sum(values.reshape(new_shape), axis=axis_pos + 1))

def restrict(values):
    return pair_sum(pair_sum(pair_sum(values, 0), 1), 2)

def prolong(values):
    return jnp.repeat(jnp.repeat(jnp.repeat(values, 2, 0), 2, 1), 2, 2)

def coarsen(weights, reaction):
    weight_x, weight_y, weight_z = weights
    coarse_x = pair_sum(pair_sum(weight_x[::2], 1), 2)
    coarse_y = pair_sum(pair_sum(weight_y[:, ::2], 0), 2)
    coarse_z = pair_sum(pair_sum(weight_z[:, :, ::2], 0), 1)
    return ((coarse_x, coarse_y, coarse_z), restrict(reaction))

def build_levels(weights, reaction):
    levels = [(weights, reaction, 1.0 / diagonal_of(weights, reaction))]
    for level_idx in range(1, LEVELS):
        weights, reaction = coarsen(weights, reaction)
        levels.append((weights, reaction, 1.0 / diagonal_of(weights, reaction)))
    return levels

def vcycle(levels, level_depth, remnant):
    weights, reaction, inverse = levels[level_depth]

    def operate(values):
        return apply_operator(jnp.pad(values, 1), weights, reaction)
    if level_depth == len(levels) - 1:
        summed, _, _ = smooth(remnant, inverse, 3, operate)
        return summed
    summed, remnant, update = smooth(remnant, inverse, 2, operate)
    remnant = remnant - operate(update)
    correction = prolong(vcycle(levels, level_depth + 1, restrict(remnant)))
    summed = summed + correction
    remnant = remnant - operate(correction)
    smoothed, _, _ = smooth(remnant, inverse, 2, operate)
    return summed + smoothed

def reference(iterate, source, reaction, trial_powers):
    gradient = differences(jnp.pad(iterate, 1))
    weights = tuple((stiffness(s) for s in gradient))
    remnant = source - reaction * iterate + divergence(tuple((fluxes(s) for s in gradient)))
    levels = build_levels(weights, reaction)
    newton_dir = jnp.zeros_like(iterate)
    precond_out = vcycle(levels, 0, remnant)
    direction = precond_out
    precond_norm = jnp.sum(remnant * precond_out)
    for iter_idx in range(ITERS):
        image_dir = apply_operator(jnp.pad(direction, 1), weights, reaction)
        step_length = precond_norm / jnp.sum(direction * image_dir)
        newton_dir = newton_dir + step_length * direction
        remnant = remnant - step_length * image_dir
        if iter_idx + 1 < ITERS:
            precond_out = vcycle(levels, 0, remnant)
            norm_next = jnp.sum(remnant * precond_out)
            direction = precond_out + norm_next / precond_norm * direction
            precond_norm = norm_next
    layer_cells = NY * NZ
    layers = []
    for trial_idx in range(TRIALS):
        step_scale = jnp.exp2(-trial_powers[trial_idx].astype(jnp.float32))
        trial_field = iterate + step_scale * newton_dir
        trial_slopes = differences(jnp.pad(trial_field, 1))
        energy_x = face_energy(trial_slopes[0])
        layer_sum = lax.optimization_barrier(jnp.sum(energy_x[:-1], axis=(1, 2)))
        layer_sum = layer_sum.at[-1].add(jnp.sum(energy_x[-1]))
        layer_sum = layer_sum + lax.optimization_barrier(jnp.sum(face_energy(trial_slopes[1]), axis=(1, 2))) + lax.optimization_barrier(jnp.sum(face_energy(trial_slopes[2]), axis=(1, 2)))
        layer_sum = layer_sum + lax.optimization_barrier(jnp.sum(0.5 * reaction * trial_field * trial_field - source * trial_field, axis=(1, 2)))
        layers.append(layer_sum / layer_cells)
    layer_energies = jnp.stack(layers)
    energies = lax.optimization_barrier(jnp.sum(layer_energies, axis=1)) / NX
    return (newton_dir, remnant, layer_energies, energies)
```

```python
import functools

import jax
import jax.numpy as jnp
from jax import lax
from jax.experimental import pallas as pl
from jax.experimental.pallas import tpu as pltpu
from jax.sharding import PartitionSpec as P

ITERS = 4
LEVELS = 4
TRIALS = 4
MID = 1.15
HALF = 0.85
SIGMA = MID / HALF
RHO0 = 1.0 / SIGMA
RHO1 = 1.0 / (2.0 * SIGMA - RHO0)
RHO2 = 1.0 / (2.0 * SIGMA - RHO1)
ROUND = 3
KEPT = ROUND
DG, INV, XM, XP, YM, YP, ZM, ZP, YB, ZB = range(10)
MESH = pl.DeviceIdType.MESH


class Grid:
    def __init__(self, Y, Z):
        self.Y, self.Z = Y, Z

    def rows_of(self, x):
        return lax.rem(lax.broadcasted_iota(jnp.int32, (x * self.Y, self.Z), 0), self.Y)

    def lanes_of(self, x):
        return lax.broadcasted_iota(jnp.int32, (x * self.Y, self.Z), 1)

    def pair_x(self, v):
        Y = self.Y
        x = v.shape[0] // Y
        return cat([v[2 * i * Y : (2 * i + 1) * Y] + v[(2 * i + 1) * Y : (2 * i + 2) * Y] for i in range(x // 2)])

    def pick_x(self, v, odd):
        Y = self.Y
        x = v.shape[0] // Y
        return cat([v[(2 * i + odd) * Y : (2 * i + odd + 1) * Y] for i in range(x // 2)])

    def bit(self, v, level, axis):
        at = self.rows_of(v.shape[0] // self.Y) if axis == 0 else self.lanes_of(v.shape[0] // self.Y)
        return lax.rem(at, 2 << level) < (1 << level)

    def pair(self, v, level, axis):
        step = 1 << level
        return v + jnp.where(self.bit(v, level, axis), roll(v, -step, axis), roll(v, step, axis))

    def pick(self, v, level, axis, odd):
        step = 1 << level
        low = self.bit(v, level, axis)
        if odd:
            return jnp.where(low, roll(v, -step, axis), v)
        return jnp.where(low, v, roll(v, step, axis))

    def restrict(self, v, level):
        return self.pair(self.pair(self.pair_x(v), level, 0), level, 1)

    def prolong(self, v):
        Y = self.Y
        x = v.shape[0] // Y
        return cat([v[(i // 2) * Y : (i // 2 + 1) * Y] for i in range(2 * x)])

    def coarsen(self, ws, reaction, level):
        xm, xp, ym, yp, zm, zp = ws
        pair, pick = self.pair, self.pick
        ws = (
            pair(pair(self.pick_x(xm, 0), level, 0), level, 1),
            pair(pair(self.pick_x(xp, 1), level, 0), level, 1),
            pair(pick(self.pair_x(ym), level, 0, 0), level, 1),
            pair(pick(self.pair_x(yp), level, 0, 1), level, 1),
            pick(pair(self.pair_x(zm), level, 0), level, 1, 0),
            pick(pair(self.pair_x(zp), level, 0), level, 1, 1),
        )
        return ws, self.restrict(reaction, level)

    def put(self, w, level, ws, reaction):
        Y, Z = self.Y, self.Z
        xm, xp, ym, yp, zm, zp = ws
        step = 1 << level
        x = xm.shape[0] // Y
        rows, lanes = self.rows_of(x), self.lanes_of(x)
        diagonal = reaction + xm + xp + ym + yp + zm + zp
        zero = jnp.zeros_like(xm)
        w[DG] = diagonal
        w[INV] = 1.0 / diagonal
        w[XM] = xm
        w[XP] = xp
        w[YM] = jnp.where(rows < step, zero, ym)
        w[YP] = jnp.where(rows >= Y - step, zero, yp)
        w[ZM] = jnp.where(lanes < step, zero, zm)
        w[ZP] = jnp.where(lanes >= Z - step, zero, zp)
        if w.shape[0] > YB:
            w[YB] = jnp.where(rows < step, ym, jnp.where(rows >= Y - step, yp, zero))
            w[ZB] = jnp.where(lanes < step, zm, jnp.where(lanes >= Z - step, zp, zero))

    def inner(self, w, v, level):
        step = 1 << level
        acc = w[DG] * v
        acc = acc - w[YM] * roll(v, step, 0) - w[YP] * roll(v, -step, 0)
        acc = acc - w[ZM] * roll(v, step, 1) - w[ZP] * roll(v, -step, 1)
        Y = self.Y
        if v.shape[0] > Y:
            none = jnp.zeros((Y, self.Z), jnp.float32)
            acc = acc - w[XM] * cat([none, v[:-Y]]) - w[XP] * cat([v[Y:], none])
        return acc


def cat(parts):
    return parts[0] if len(parts) == 1 else jnp.concatenate(parts, axis=0)


def roll(v, shift, axis):
    return pltpu.roll(v, shift % v.shape[axis], axis)


def dot(a, b):
    return lax.dot_general(
        a, b, (((1,), (0,)), ((), ())), precision=lax.Precision.HIGHEST, preferred_element_type=jnp.float32
    )


def kernel(
    sizes, counts, tp_ref, it_ref, src_ref, rea_ref, dir_ref, rem_ref, le_ref, en_ref,
    sx, rx, sy, ry, sz, rz, ssem, rsem, lev0, lev1, glev2, glev3, p_ref, q_ref,
    phx, phy, phz, dhx, dhy, dhz, dot_all, en_all, red_ssem, red_rsem,
    picked, gat_pl, gat_x, set_pl, set_x, glob,
):
    X, Y, Z = sizes
    nx, ny, nz = counts
    planes = ny * nz
    levs = (lev0, lev1)
    L = len(levs)
    x_own, y_own, z_own = X >> L, Y >> L, Z >> L
    GY, GZ = ny * y_own, nz * z_own
    here, world = Grid(Y, Z), Grid(GY, GZ)
    rows_of, lanes_of = here.rows_of, here.lanes_of
    ix, iy, iz = lax.axis_index("gx"), lax.axis_index("gy"), lax.axis_index("gz")
    has = (ix > 0, ix < nx - 1, iy > 0, iy < ny - 1, iz > 0, iz < nz - 1)
    devs = (
        (ix - 1, iy, iz), (ix + 1, iy, iz), (ix, iy - 1, iz),
        (ix, iy + 1, iz), (ix, iy, iz - 1), (ix, iy, iz + 1),
    )
    send = (sx, sx, sy, sy, sz, sz)
    recv = (rx, rx, ry, ry, rz, rz)
    lane_y = lax.broadcasted_iota(jnp.int32, (Y, Z), 1)
    lane_1 = lax.broadcasted_iota(jnp.int32, (1, Z), 1)

    for d in range(6):
        @pl.when(jnp.logical_not(has[d]))
        def _():
            recv[d][:, d % 2] = jnp.zeros(recv[d].shape[:1] + recv[d].shape[2:], jnp.float32)

    def outgoing(d, slot):
        side = d % 2
        return pltpu.make_async_remote_copy(
            src_ref=send[d].at[slot, side],
            dst_ref=recv[d].at[slot, 1 - side],
            send_sem=ssem.at[slot, d],
            recv_sem=rsem.at[slot, d + 1 - 2 * side],
            device_id=devs[d],
            device_id_type=MESH,
        )

    def incoming(d, slot):
        side = d % 2
        return pltpu.make_async_remote_copy(
            src_ref=send[d].at[slot, side],
            dst_ref=recv[d].at[slot, side],
            send_sem=ssem.at[slot, d],
            recv_sem=rsem.at[slot, d],
            device_id=devs[d],
            device_id_type=MESH,
        )

    def go(d, slot):
        @pl.when(has[d])
        def _():
            outgoing(d, slot).start()

    def start(v, slot):
        x = v.shape[0] // Y
        sx[slot, 0] = v[:Y]
        sx[slot, 1] = v[-Y:]
        go(0, slot)
        go(1, slot)
        for i in range(x):
            sy[slot, 0, i : i + 1] = v[i * Y : i * Y + 1]
            sy[slot, 1, i : i + 1] = v[i * Y + Y - 1 : i * Y + Y]
        go(2, slot)
        go(3, slot)
        for side, lane in ((0, 0), (1, Z - 1)):
            packed = jnp.broadcast_to(v[:Y, lane : lane + 1], (Y, Z))
            for i in range(1, x):
                part = jnp.broadcast_to(v[i * Y : i * Y + Y, lane : lane + 1], (Y, Z))
                packed = jnp.where(lane_y == i, part, packed)
            sz[slot, side] = packed
        go(4, slot)
        go(5, slot)

    def finish(slot):
        for d in range(6):
            @pl.when(has[d])
            def _():
                copy = incoming(d, slot)
                copy.wait_recv()
                copy.wait_send()

    def wide_y(half, x):
        return cat([jnp.broadcast_to(half[i : i + 1], (Y, Z)) for i in range(x)])

    def wide_z(half, x):
        return cat([jnp.broadcast_to(half[:, i : i + 1], (Y, Z)) for i in range(x)])

    def beyond(w, acc, in_x0, in_x1, in_y, in_z):
        x = acc.shape[0] // Y
        acc = acc - w[YB] * in_y - w[ZB] * in_z
        low = w[XM, :Y] * in_x0
        high = w[XP, (x - 1) * Y :] * in_x1
        if x == 1:
            return acc - low - high
        return cat([acc[:Y] - low] + ([acc[Y:-Y]] if x > 2 else []) + [acc[-Y:] - high])

    def operate(v, level, slot):
        w = levs[level]
        x = X >> level
        start(v, slot)
        acc = here.inner(w, v, level)
        finish(slot)
        in_y = jnp.where(rows_of(x) < Y // 2, wide_y(ry[slot, 0], x), wide_y(ry[slot, 1], x))
        in_z = jnp.where(lanes_of(x) < Z // 2, wide_z(rz[slot, 0], x), wide_z(rz[slot, 1], x))
        return beyond(w, acc, rx[slot, 0], rx[slot, 1], in_y, in_z)

    turn = [0]

    def apply(v, level):
        slot = turn[0] % ROUND
        turn[0] += 1
        return operate(v, level, slot)

    def vcycle(r, level, part):
        w = levs[level]
        u = w[INV] * r * (1.0 / MID)
        total = u
        r = r - apply(u, level)
        u = RHO1 * RHO0 * u + 2.0 * RHO1 / HALF * w[INV] * r
        total = total + u
        r = r - apply(u, level)
        coarse = here.restrict(r, level)
        if level + 1 < L:
            e = here.prolong(vcycle(coarse, level + 1, part))
            r = r - apply(e, level)
        else:
            everywhere = collect(coarse, 1, part, gat_pl, gat_x, 4)
            e, ends = spread(world_cycle(everywhere[0], level + 1))
            r = r - beyond(w, here.inner(w, e, level), *ends)
        total = total + e
        u = w[INV] * r * (1.0 / MID)
        total = total + u
        r = r - apply(u, level)
        u = RHO1 * RHO0 * u + 2.0 * RHO1 / HALF * w[INV] * r
        return total + u

    def world_cycle(r, level):
        w = (glev2, glev3)[level - L]

        def apply(v):
            return world.inner(w, v, level - L)

        u = w[INV] * r * (1.0 / MID)
        total = u
        r = r - apply(u)
        u = RHO1 * RHO0 * u + 2.0 * RHO1 / HALF * w[INV] * r
        total = total + u
        r = r - apply(u)
        if level == LEVELS - 1:
            u = RHO2 * RHO1 * u + 2.0 * RHO2 / HALF * w[INV] * r
            return total + u
        e = world.prolong(world_cycle(world.restrict(r, level - L), level + 1))
        total = total + e
        r = r - apply(e)
        u = w[INV] * r * (1.0 / MID)
        total = total + u
        r = r - apply(u)
        u = RHO1 * RHO0 * u + 2.0 * RHO1 / HALF * w[INV] * r
        return total + u

    def hot(shape, wanted):
        at = lax.broadcasted_iota(jnp.int32, shape, 0)
        return jnp.where(at == wanted, 1.0, 0.0)

    def collect(v, fields, part, pl_ref, x_ref, which):
        count = fields * x_own * y_own
        picked[: fields * x_own * Y] = v
        own = picked[pl.ds(0, count, stride=1 << L), :]
        lane = lax.broadcasted_iota(jnp.int32, (Z, GZ), 1) - iz * z_own
        inside = jnp.logical_and(lane >= 0, lane < z_own)
        put = hot((Z, GZ), jnp.where(inside, lane * (1 << L), -1))
        pl_ref[part, my_plane] = dot(own, put)
        gather(pl_ref, part, planes, my_plane, in_plane, which)
        for j in range(ny):
            rows = pl_ref[part, j * nz]
            for k in range(1, nz):
                rows = rows + pl_ref[part, j * nz + k]
            for i in range(fields * x_own):
                x_ref[part, ix, i * GY + j * y_own : i * GY + (j + 1) * y_own] = rows[i * y_own : (i + 1) * y_own]
        gather(x_ref, part, nx, ix, in_column, which + 1)
        return [
            cat([x_ref[part, d, f * x_own * GY : (f + 1) * x_own * GY] for d in range(nx)]) for f in range(fields)
        ]

    def spread(v):
        lane = lax.broadcasted_iota(jnp.int32, (GZ, Z), 1)
        inside = hot((GZ, Z), iz * z_own + lane // (1 << L))
        outside = hot((GZ, Z), jnp.where(lane < Z // 2, iz * z_own - 1, iz * z_own + z_own))
        glob[0, GY : GY + nx * x_own * GY] = dot(v, inside)
        glob[1, GY : GY + nx * x_own * GY] = dot(v, outside)
        rows = rows_of(1)

        def layer(which, a):
            base = (ix * x_own + 1 + a) * GY + iy * y_own
            out = jnp.broadcast_to(glob[which, pl.ds(base, 1), :], (Y, Z))
            for j in range(1, y_own):
                row = jnp.broadcast_to(glob[which, pl.ds(base + j, 1), :], (Y, Z))
                out = jnp.where(rows < j << L, out, row)
            return out

        def rims(a):
            base = (ix * x_own + 1 + a) * GY + iy * y_own
            low = glob[0, pl.ds(base - 1, 1), :] * has_low
            high = glob[0, pl.ds(base + y_own, 1), :] * has_high
            return jnp.where(rows < Y // 2, jnp.broadcast_to(low, (Y, Z)), jnp.broadcast_to(high, (Y, Z)))

        has_low = jnp.where(iy > 0, 1.0, 0.0)
        has_high = jnp.where(iy < ny - 1, 1.0, 0.0)
        own = range(x_own)
        e = here.prolong(cat([layer(0, a) for a in own]))
        in_y = here.prolong(cat([rims(a) for a in own]))
        in_z = here.prolong(cat([layer(1, a) for a in own]))
        return e, (layer(0, -1), layer(0, x_own), in_y, in_z)

    def gather(ref, part, count, me, device, which):
        for j in range(count):
            @pl.when(me != j)
            def _():
                pltpu.make_async_remote_copy(
                    src_ref=ref.at[part, me],
                    dst_ref=ref.at[part, me],
                    send_sem=red_ssem.at[which, part],
                    recv_sem=red_rsem.at[which, part],
                    device_id=device(j),
                    device_id_type=MESH,
                ).start()
        if count > 1:
            others = ref.at[part, pl.ds(0, count - 1)]
            pltpu.make_async_copy(others, others, red_rsem.at[which, part]).wait()
            pltpu.make_async_copy(others, others, red_ssem.at[which, part]).wait()

    def in_plane(j):
        return (ix, j // nz, j % nz)

    def in_column(j):
        return (j, iy, iz)

    def in_grid(j):
        return (j // planes, j // nz % ny, j % nz)

    my_plane = iy * nz + iz
    me = ix * planes + my_plane

    def reduce_plane(ref, part, value, which):
        ref[part, my_plane] = value
        gather(ref, part, planes, my_plane, in_plane, which)
        return jnp.sum(ref[part], axis=0)

    def reduce_column(ref, part, value, which):
        ref[part, ix] = value
        gather(ref, part, nx, ix, in_column, which)
        return jnp.sum(ref[part], axis=0)

    def total_of(v):
        return jnp.sum(jnp.sum(v, axis=0, keepdims=True), axis=1, keepdims=True)

    def lane_of(row, i):
        return jnp.sum(jnp.where(lane_1 == i, row, 0.0), axis=1, keepdims=True)

    it = it_ref[...].reshape(X * Y, Z)
    reaction = rea_ref[...].reshape(X * Y, Z)
    start(it, KEPT)
    finish(KEPT)
    rows, lanes = rows_of(X), lanes_of(X)
    last_row, last_lane = rows == Y - 1, lanes == Z - 1
    n_xm = cat([rx[KEPT, 0], it[:-Y]])
    n_xp = cat([it[Y:], rx[KEPT, 1]])
    n_ym = jnp.where(rows == 0, wide_y(ry[KEPT, 0], X), roll(it, 1, 0))
    n_yp = jnp.where(last_row, wide_y(ry[KEPT, 1], X), roll(it, -1, 0))
    n_zm = jnp.where(lanes == 0, wide_z(rz[KEPT, 0], X), roll(it, 1, 1))
    n_zp = jnp.where(last_lane, wide_z(rz[KEPT, 1], X), roll(it, -1, 1))
    ws = []
    r = src_ref[...].reshape(X * Y, Z) - reaction * it
    for sign, n in ((-1, n_xm), (1, n_xp), (-1, n_ym), (1, n_yp), (-1, n_zm), (1, n_zp)):
        g = n - it
        square = g * g
        root = jnp.sqrt(1.0 + square)
        ws.append((1.0 + 2.0 * square) / root)
        r = r + g * root
    rem_ref[...] = r.reshape(X, Y, Z)
    here.put(levs[0], 0, ws, reaction)
    for level in range(L):
        ws, reaction = here.coarsen(ws, reaction, level)
        if level + 1 < L:
            here.put(levs[level + 1], level + 1, ws, reaction)
    glob[...] = jnp.zeros_like(glob)
    *ws, reaction = collect(cat(list(ws) + [reaction]), 7, 0, set_pl, set_x, 6)
    world.put(glev2, 0, ws, reaction)
    world.put(glev3, 1, *world.coarsen(ws, reaction, 0))
    for ref in (p_ref, q_ref, phx, phy, phz, dhx, dhy, dhz):
        ref[...] = jnp.zeros_like(ref)
    dir_ref[...] = jnp.zeros_like(dir_ref)

    def body(it_idx, carry):
        rz_old, pq_old = carry
        part = lax.rem(it_idx, 2)
        r = rem_ref[...].reshape(X * Y, Z)
        turn[0] = 0
        z = vcycle(r, 0, part)
        z_slot = turn[0] % ROUND
        az = apply(z, 0)
        q_old = q_ref[...]
        sums = jnp.where(
            lane_1 == 0,
            total_of(rem_ref[...].reshape(X * Y, Z) * z),
            jnp.where(lane_1 == 1, total_of(z * az), total_of(z * q_old)),
        )
        dot_all[part, me] = sums
        gather(dot_all, part, nx * planes, me, in_grid, 0)
        row = jnp.sum(dot_all[part], axis=0)
        rz_new, zaz, zq = lane_of(row, 0), lane_of(row, 1), lane_of(row, 2)
        beta = rz_new / rz_old
        pq = zaz + 2.0 * beta * zq + beta * beta * pq_old
        a = rz_new / pq
        p = z + beta * p_ref[...]
        q = az + beta * q_old
        p_ref[...] = p
        q_ref[...] = q
        dir_ref[...] = dir_ref[...] + (a * p).reshape(X, Y, Z)
        rem_ref[...] = rem_ref[...] - (a * q).reshape(X, Y, Z)
        for got, ph, dh in ((rx, phx, dhx), (ry, phy, dhy), (rz, phz, dhz)):
            for side in range(2):
                edge = got[z_slot, side] + beta * ph[side]
                ph[side] = edge
                dh[side] = dh[side] + a * edge
        return rz_new, pq

    one = jnp.ones((1, 1), jnp.float32)
    lax.fori_loop(0, ITERS, body, (one, jnp.zeros((1, 1), jnp.float32)))

    it = it_ref[...].reshape(X * Y, Z)
    step_dir = dir_ref[...].reshape(X * Y, Z)

    def energy(g):
        square = 1.0 + g * g
        return (square * jnp.sqrt(square) - 1.0) * (1.0 / 3.0)

    ends_y = jnp.where(jnp.logical_and(last_row, iy == ny - 1), 1.0, 0.0)
    ends_z = jnp.where(jnp.logical_and(last_lane, iz == nz - 1), 1.0, 0.0)
    ends_x = jnp.where(ix == nx - 1, 1.0, 0.0)
    across = lax.broadcasted_iota(jnp.int32, (X, Z), 0) == lax.broadcasted_iota(jnp.int32, (X, Z), 1)
    trial_rows = []
    for k in range(TRIALS):
        s = jnp.exp2(-jnp.full((1, Z), tp_ref[k], jnp.int32).astype(jnp.float32))
        v = it + s * step_dir
        low_x = cat([rx[KEPT, 0] + s * dhx[0], v[:-Y]])
        low_y = jnp.where(rows == 0, wide_y(ry[KEPT, 0] + s * dhy[0], X), roll(v, 1, 0))
        low_z = jnp.where(lanes == 0, wide_z(rz[KEPT, 0] + s * dhz[0], X), roll(v, 1, 1))
        at_end = energy(v)
        e = energy(v - low_x) + energy(v - low_y) + energy(v - low_z)
        e = e + at_end * (ends_y + ends_z)
        e = cat([e[:-Y], e[-Y:] + ends_x * at_end[-Y:]]) if X > 1 else e + ends_x * at_end
        e = e + 0.5 * rea_ref[...].reshape(X * Y, Z) * v * v - src_ref[...].reshape(X * Y, Z) * v
        by_layer = jnp.sum(jnp.sum(e.reshape(X, Y, Z), axis=1), axis=1, keepdims=True)
        trial_rows.append(jnp.sum(jnp.where(across, by_layer, 0.0), axis=0, keepdims=True))
    en_all[0, me] = jnp.concatenate(trial_rows, axis=0)
    gather(en_all, 0, nx * planes, me, in_grid, 2)
    layers = jnp.sum(en_all[0, pl.ds(ix * planes, planes)], axis=0)
    layers = layers / (Y * ny * Z * nz)
    le_ref[...] = layers[:, :X]
    overall = jnp.sum(en_all[0], axis=0) / (Y * ny * Z * nz)
    overall = jnp.sum(overall, axis=1, keepdims=True) / (X * nx)
    en_ref[...] = jnp.broadcast_to(overall, (TRIALS, Z))


def on_device(counts, iterate, source, reaction, trial_powers):
    X, Y, Z = iterate.shape
    nx, ny, nz = counts
    f32 = jnp.float32
    slots = ROUND + 1
    vm = pltpu.VMEM
    scratch = [vm((slots, 2, rows, Z), f32) for rows in (Y, Y, X, X, Y, Y)]
    scratch += [pltpu.SemaphoreType.DMA((slots, 6))] * 2
    x_own, y_own = X // 4, Y // 4
    GX, GY, GZ = nx * x_own, ny * y_own, nz * Z // 4
    scratch += [vm((10, (X >> level) * Y, Z), f32) for level in range(2)]
    scratch += [vm((8, (GX >> level) * GY, GZ), f32) for level in range(2)]
    scratch += [vm((X * Y, Z), f32)] * 2
    scratch += [vm((2, rows, Z), f32) for rows in (Y, X, Y)] * 2
    scratch += [
        vm((2, nx * ny * nz, 1, Z), f32),
        vm((1, nx * ny * nz, TRIALS, Z), f32),
        pltpu.SemaphoreType.DMA((8, 2)), pltpu.SemaphoreType.DMA((8, 2)),
        vm((7 * x_own * Y, Z), f32),
        vm((2, ny * nz, x_own * y_own, GZ), f32), vm((2, nx, x_own * GY, GZ), f32),
        vm((1, ny * nz, 7 * x_own * y_own, GZ), f32), vm((1, nx, 7 * x_own * GY, GZ), f32),
        vm((2, (GX + 2) * GY, Z), f32),
    ]
    whole = pl.BlockSpec(memory_space=pltpu.VMEM)
    out = pl.pallas_call(
        functools.partial(kernel, (X, Y, Z), counts),
        out_shape=[
            jax.ShapeDtypeStruct((X, Y, Z), f32),
            jax.ShapeDtypeStruct((X, Y, Z), f32),
            jax.ShapeDtypeStruct((TRIALS, X), f32),
            jax.ShapeDtypeStruct((TRIALS, Z), f32),
        ],
        in_specs=[pl.BlockSpec(memory_space=pltpu.SMEM), whole, whole, whole],
        out_specs=[whole] * 4,
        scratch_shapes=scratch,
        compiler_params=pltpu.CompilerParams(has_side_effects=True, vmem_limit_bytes=48 * 1024 * 1024),
        name="newton_step",
    )(trial_powers, iterate, source, reaction)
    return out[0], out[1], out[2], out[3][:, 0]


LANES = 128
HALO = 8
F_DG, F_XM, F_YM, F_ZM, F_XP, F_YP, F_ZP, F_INV = range(8)
C_ONE = RHO1 * RHO0
C_TWO = 2.0 * RHO1 / HALF
C_THREE = RHO2 * RHO1
C_FOUR = 2.0 * RHO2 / HALF


def slab_fits(counts, shape):
    X, Y, Z = shape
    nx, ny, _ = counts
    return X == 1 << (LEVELS - 1) and X * Y == LANES and nx * ny == X and Z == 2 * HALO * X


def slab_kernel(
    sizes, counts, tp_ref, it_in, src_in, rea_in, dir_out, rem_out, le_ref, en_ref,
    turned, d_it, d_rea, d_src, f_it, f_rea, f_src, w0, w1, w2, w3,
    va, vb, vc, vd, vz, rr, rs, az, sa, ra, sb, rb, s0, r0, sq, rq,
    ua, ub, uc, ud, r1in, r1by, rr1, rs1, sa1, ra1, sb1, rb1, s1, r1, sq1, rq1, e2, cres, cq,
    p_ref, dir_ref, q_ref, r_ref,
    msg, gath, rows_of, wmsg, wgath, hb, sh, emsg, egath, outs, back,
    d_ssem, d_rsem, g_ssem, g_rsem, h_ssem, h_rsem,
):
    X, Y, Z = sizes
    nx, ny, nz = counts
    P = nx * ny
    S = Z // P
    GY = ny * Y
    NS = nz * P
    NZ = nz * Z
    W = S + 2 * HALO
    f32 = jnp.float32
    ix, iy, iz = lax.axis_index("gx"), lax.axis_index("gy"), lax.axis_index("gz")
    odd_z = lax.rem(iz, 2)
    odd_y = lax.rem(iy, 2)
    along = iy * nx + ix + odd_y * (nx - 1 - 2 * ix)
    j = along + odd_z * (P - 1 - 2 * along)
    slab = iz * P + j
    me = (ix * ny + iy) * nz + iz
    own_tile = ix * ny + iy

    def device_at(jj, kz):
        a = jj + lax.rem(kz, 2) * (P - 1 - 2 * jj)
        y = a // nx
        i = lax.rem(a, nx)
        return (i + lax.rem(y, 2) * (nx - 1 - 2 * i), y, kz)

    def device_of(s):
        return device_at(lax.rem(s, P), s // P)

    has_lo, has_hi = slab > 0, slab < NS - 1
    lo_dev, hi_dev = device_of(jnp.maximum(slab - 1, 0)), device_of(jnp.minimum(slab + 1, NS - 1))

    def lane(n):
        return lax.broadcasted_iota(jnp.int32, (n, LANES), 1)

    def row(n):
        return lax.broadcasted_iota(jnp.int32, (n, LANES), 0)

    def low_bit(n, step):
        return lax.rem(lane(n), 2 * step) < step

    def swap(v, step):
        return jnp.where(low_bit(v.shape[0], step), roll(v, -step, 1), roll(v, step, 1))

    def pair(v, step):
        return v + swap(v, step)

    def pick_low(v, step):
        return jnp.where(low_bit(v.shape[0], step), v, roll(v, step, 1))

    def pick_high(v, step):
        return jnp.where(low_bit(v.shape[0], step), roll(v, -step, 1), v)

    def block_transpose(tiles):
        n = tiles[0].shape[0]
        k = P // 2
        while k:
            low = low_bit(n, Y * k)
            new = list(tiles)
            for i in range(P):
                if not i & k:
                    a, b = tiles[i], tiles[i | k]
                    new[i] = jnp.where(low, a, roll(b, Y * k, 1))
                    new[i | k] = jnp.where(low, roll(a, -Y * k, 1), b)
            tiles = new
            k //= 2
        return tiles

    arrays = ((it_in, d_it, f_it, 2 * HALO), (rea_in, d_rea, f_rea, HALO), (src_in, d_src, f_src, HALO))
    LOW, MID_PART, HIGH = range(3)

    def piece(a, kind, src_row, count, dst_row, jd, kz):
        return pltpu.make_async_remote_copy(
            src_ref=turned.at[a, pl.ds(src_row, count)],
            dst_ref=arrays[a][1].at[own_tile, pl.ds(dst_row, count)],
            send_sem=d_ssem.at[a, kind, jd],
            recv_sem=d_rsem.at[a, kind],
            device_id=device_at(jd, kz),
            device_id_type=MESH,
        )

    def pieces(a):
        halo = arrays[a][3]
        for jd in range(P):
            yield j != jd, piece(a, MID_PART, S * jd, S, halo, jd, iz)
            if jd > 0:
                yield j != jd, piece(a, LOW, S * jd - halo, halo, 0, jd, iz)
            else:
                yield iz < nz - 1, piece(a, LOW, Z - halo, halo, 0, jd, iz + 1)
            if jd < P - 1:
                yield j != jd, piece(a, HIGH, S * jd + S, halo, halo + S, jd, iz)
            else:
                yield iz > 0, piece(a, HIGH, 0, halo, halo + S, jd, iz - 1)

    for ref in (va, vb, vc, vd, vz, ua, ub, uc, ud, r1in, r1by, e2, hb, sh, p_ref, dir_ref, q_ref, sq, rq, sq1, rq1, cq, w1):
        ref[...] = jnp.zeros_like(ref)
    w1[F_DG] = jnp.ones(w1.shape[1:], f32)

    for a, (given, landed, _, halo) in enumerate(arrays):
        turned[a] = given[...].reshape(LANES, Z).T
        for wanted, copy in pieces(a):
            @pl.when(wanted)
            def _():
                copy.start()
        landed[own_tile, halo : halo + S] = turned[a, pl.ds(pl.multiple_of(S * j, HALO), S)]

        @pl.when(j > 0)
        def _():
            landed[own_tile, :halo] = turned[a, pl.ds(pl.multiple_of(S * j - halo, HALO), halo)]

        @pl.when(j < P - 1)
        def _():
            landed[own_tile, halo + S :] = turned[a, pl.ds(pl.multiple_of(S * j + S, HALO), halo)]

        @pl.when(slab == 0)
        def _():
            landed[:, :halo] = jnp.zeros((P, halo, LANES), f32)

        @pl.when(slab == NS - 1)
        def _():
            landed[:, halo + S :] = jnp.zeros((P, halo, LANES), f32)

    def landed_wait(a, kind, first, count, tiles):
        view = arrays[a][1].at[pl.ds(0, tiles), pl.ds(first, count)]
        pltpu.make_async_copy(view, view, d_rsem.at[a, kind]).wait()

    for a, (_, landed, flat, halo) in enumerate(arrays):
        landed_wait(a, MID_PART, halo, S, P - 1)
        for kind, first, inner, outer in (
            (LOW, 0, j > 0, jnp.logical_and(j == 0, iz > 0)),
            (HIGH, halo + S, j < P - 1, jnp.logical_and(j == P - 1, iz < nz - 1)),
        ):
            @pl.when(inner)
            def _():
                landed_wait(a, kind, first, halo, P - 1)

            @pl.when(outer)
            def _():
                landed_wait(a, kind, first, halo, P)
        for at in range(0, S + 2 * halo, HALO):
            tiles = block_transpose([landed[i, at : at + HALO] for i in range(P)])
            for i in range(P):
                flat[i, at : at + HALO] = tiles[i]

    lanes = lane(W)
    z_at = slab * S + row(W) - HALO
    inside = jnp.logical_and(z_at >= 0, z_at < NZ)
    z_low = jnp.logical_and(z_at > 0, z_at < NZ)
    z_high = jnp.logical_and(z_at >= 0, z_at < NZ - 1)
    x_first, x_last = lanes < GY, lanes >= LANES - GY
    y_at = lax.rem(lanes, GY)
    y_first, y_last = y_at == 0, y_at == GY - 1

    def face(g):
        square = g * g
        root = jnp.sqrt(1.0 + square)
        return (1.0 + 2.0 * square) / root, g * root

    def window(t):
        return f_it[t, HALO : HALO + W]

    low_w, low_p = face(window(0) - jnp.where(x_first, 0.0, roll(window(X - 1), GY, 1)))
    first_w = low_w
    for t in range(X):
        c = window(t)
        beyond = window(t + 1) if t < X - 1 else jnp.where(x_last, 0.0, roll(window(0), -GY, 1))
        high_w, high_p = face(beyond - c)
        yl_w, yl_p = face(c - jnp.where(y_first, 0.0, roll(c, 1, 1)))
        yh_w, yh_p = face(jnp.where(y_last, 0.0, roll(c, -1, 1)) - c)
        zl_w, zl_p = face(c - f_it[t, HALO - 1 : HALO - 1 + W])
        zh_w, zh_p = face(f_it[t, HALO + 1 : HALO + 1 + W] - c)
        rea = f_rea[t]
        diagonal = rea + low_w + high_w + yl_w + yh_w + zl_w + zh_w
        w0[F_DG, t] = diagonal
        w0[F_INV, t] = 1.0 / diagonal
        w0[F_XM, t] = jnp.where(x_first, 0.0, low_w) if t == 0 else low_w
        w0[F_XP, t] = jnp.where(x_last, 0.0, high_w) if t == X - 1 else high_w
        w0[F_YM, t] = jnp.where(y_first, 0.0, yl_w)
        w0[F_YP, t] = jnp.where(y_last, 0.0, yh_w)
        w0[F_ZM, t] = jnp.where(z_low, zl_w, 0.0)
        w0[F_ZP, t] = jnp.where(z_high, zh_w, 0.0)
        r = f_src[t] - rea * c + (high_p - low_p) + (yh_p - yl_p) + (zh_p - zl_p)
        r = jnp.where(inside, r, 0.0)
        az[t] = r
        r_ref[t] = r
        low_w, low_p = high_w, high_p

    def coarsen(get, step):
        def build(k):
            def both(field, t):
                low, high = get(field, t)
                return low + high
            lo, hi = 2 * k, 2 * k + 1
            xm = pair(both(F_XM, lo), step)
            ym_all = both(F_YM, lo) + both(F_YM, hi)
            zl0, zh0 = get(F_ZM, lo)
            zl1, zh1 = get(F_ZM, hi)
            between = pair(both(F_XM, hi), step) + pick_high(ym_all, step) + pair(zh0 + zh1, step)
            diagonal = pair(both(F_DG, lo) + both(F_DG, hi), step) - 2.0 * between
            return diagonal, xm, pick_low(ym_all, step), pair(zl0 + zl1, step)
        return build

    n1 = W // 2
    S1 = S // 2
    W1 = S1 + 2 * HALO
    T1 = X // 2
    at1 = (W1 - n1) // 2

    def halves0(field, t):
        return w0[field, t, pl.ds(0, n1, stride=2)], w0[field, t, pl.ds(1, n1, stride=2)]

    for k in range(T1):
        for field, value in zip((F_DG, F_XM, F_YM, F_ZM), coarsen(halves0, 1)(k)):
            w1[field, k, at1 : at1 + n1] = value

    def complete1():
        for k in range(T1):
            w1[F_INV, k] = 1.0 / w1[F_DG, k]
            w1[F_XP, k] = w1[F_XM, k + 1] if k < T1 - 1 else roll(w1[F_XM, 0], -GY, 1)
            w1[F_YP, k] = roll(w1[F_YM, k], -2, 1)
            w1[F_ZP, k] = roll(w1[F_ZM, k], -1, 0)

    complete1()

    S2 = S // 4
    T2 = X // 4

    def halves1(field, t):
        return w1[field, t, pl.ds(HALO, S2, stride=2)], w1[field, t, pl.ds(HALO + 1, S2, stride=2)]

    own_chunk = lax.rem(lane(S2), S2) == row(S2)

    def pack(v):
        return jnp.sum(jnp.where(own_chunk, v, 0.0), axis=0, keepdims=True)

    for k in range(T2):
        for field, value in zip((F_DG, F_XM, F_YM, F_ZM), coarsen(halves1, 2)(k)):
            wmsg[field * T2 + k : field * T2 + k + 1] = pack(value)

    def laps(w, vs, t, step):
        T, n = w.shape[1], w.shape[2]
        mid = slice(HALO, HALO + n)
        weights = [w[field, t] for field in range(F_INV)]
        out = []
        for v in vs:
            c = v[t, mid]
            below = v[t - 1, mid] if t > 0 else roll(v[T - 1, mid], GY, 1)
            above = v[t + 1, mid] if t < T - 1 else roll(v[0, mid], -GY, 1)
            acc = weights[F_DG] * c - weights[F_XM] * below - weights[F_XP] * above
            acc = acc - weights[F_YM] * roll(c, step, 1) - weights[F_YP] * roll(c, -step, 1)
            acc = acc - weights[F_ZM] * v[t, HALO - 1 : HALO - 1 + n]
            out.append(acc - weights[F_ZP] * v[t, HALO + 1 : HALO + 1 + n])
        return out

    def lap(w, v, t, step):
        return laps(w, [v], t, step)[0]

    def centre(v, t, n):
        return v[t, HALO : HALO + n]

    def before(w, fields, step):
        T, n = w.shape[1], w.shape[2]
        mid = slice(HALO, HALO + n)
        for t in range(T):
            inverse = w[F_INV, t]
            for r_of, u1, _, _, _, _ in fields:
                u1[t, mid] = inverse * r_of[t] * (1.0 / MID)
        for t in range(T):
            images = laps(w, [f[1] for f in fields], t, step)
            inverse = w[F_INV, t]
            for image, (r_of, u1, u2, rem1, s_out, _) in zip(images, fields):
                r = r_of[t] - image
                first = centre(u1, t, n)
                u = C_ONE * first + C_TWO * inverse * r
                u2[t, mid] = u
                s_out[t] = first + u
                rem1[t] = r
        for t in range(T):
            images = laps(w, [f[2] for f in fields], t, step)
            for image, (_, _, _, rem1, _, r_out) in zip(images, fields):
                r_out[t] = rem1[t] - image

    def after(w, e, u1, rem1, s_in, r_in, put, step):
        T, n = w.shape[1], w.shape[2]
        mid = slice(HALO, HALO + n)
        for t in range(T):
            r = r_in[t] - lap(w, e, t, step)
            rem1[t] = r
            u1[t, mid] = w[F_INV, t] * r * (1.0 / MID)
        for t in range(T):
            r = rem1[t] - lap(w, u1, t, step)
            u = centre(u1, t, n)
            put(t, s_in[t] + centre(e, t, n) + u + (C_ONE * u + C_TWO * w[F_INV, t] * r))

    fine = ((az, va, vb, rr, sa, ra), (r_ref, vc, vd, rs, sb, rb))
    coarse = ((r1in, ua, ub, rr1, sa1, ra1), (r1by, uc, ud, rs1, sb1, rb1))
    C_ROW = (0, T2 + 1)

    def presmooth(par, many):
        before(w0, fine[:many], 1)
        for f in range(many):
            rem = fine[f][-1]
            for k in range(T1):
                total = None
                for t in (2 * k, 2 * k + 1):
                    part = rem[t, pl.ds(0, n1, stride=2)] + rem[t, pl.ds(1, n1, stride=2)]
                    total = part if total is None else total + part
                coarse[f][0][k, at1 : at1 + n1] = pair(total, 1)
        before(w1, coarse[:many], 2)
        for f in range(many):
            rem = coarse[f][-1]
            for k in range(T2):
                total = None
                for t in (2 * k, 2 * k + 1):
                    part = rem[t, pl.ds(HALO, S2, stride=2)] + rem[t, pl.ds(HALO + 1, S2, stride=2)]
                    total = part if total is None else total + part
                msg[par, C_ROW[f] + k : C_ROW[f] + k + 1] = pack(pair(total, 2))

    def all_others(make):
        for other in range(nx * ny * nz):
            @pl.when(me != other)
            def _():
                make((other // (ny * nz), other // nz % ny, other % nz)).start()

    def spread_message(par):
        gath[par, slab] = msg[par]
        all_others(lambda dev: pltpu.make_async_remote_copy(
            src_ref=msg.at[par], dst_ref=gath.at[par, slab],
            send_sem=g_ssem.at[par], recv_sem=g_rsem.at[par],
            device_id=dev, device_id_type=MESH,
        ))

    def wait_message(par):
        others = gath.at[par, pl.ds(0, NS - 1)]
        pltpu.make_async_copy(others, others, g_rsem.at[par]).wait()
        pltpu.make_async_copy(others, others, g_ssem.at[par]).wait()
        for s in range(NS):
            rows_of[s * HALO : s * HALO + 2 * T2 + 1] = gath[par, s]

    def gathered(k):
        return rows_of[pl.ds(k, NS, stride=HALO)]

    per = 2 * (X + T1)
    halo_parts = tuple(
        part for f in range(2) for part in (
            (coarse[f][4], f * per, T1, S1), (coarse[f][5], f * per + T1, T1, S1),
            (fine[f][4], f * per + 2 * T1, X, S), (fine[f][5], f * per + 2 * T1 + X, X, S),
        )
    )

    def halo_send(par, many):
        for side, there, dev in ((0, has_lo, lo_dev), (1, has_hi, hi_dev)):
            @pl.when(there)
            def _():
                for ref, first, count, size in halo_parts[: 4 * many]:
                    start_row = HALO if side == 0 else size
                    pltpu.make_async_remote_copy(
                        src_ref=ref.at[:, pl.ds(start_row, HALO)],
                        dst_ref=hb.at[par, 1 - side, pl.ds(first, count)],
                        send_sem=h_ssem.at[par, side],
                        recv_sem=h_rsem.at[par, 1 - side],
                        device_id=dev,
                        device_id_type=MESH,
                    ).start()

    def halo_wait(par, many):
        for side, there in ((0, has_lo), (1, has_hi)):
            @pl.when(there)
            def _():
                view = hb.at[par, side, pl.ds(0, per * many)]
                pltpu.make_async_copy(view, view, h_rsem.at[par, side]).wait()
                pltpu.make_async_copy(view, view, h_ssem.at[par, side]).wait()

    chunk = lax.rem(lane(NS), S2)

    def down2(v):
        return jnp.where(chunk == 0, roll(roll(v, 1 - S2, 1), 1, 0), roll(v, 1, 1))

    def up2(v):
        return jnp.where(chunk == S2 - 1, roll(roll(v, S2 - 1, 1), -1, 0), roll(v, -1, 1))

    def down3(v):
        return jnp.where(chunk < S2 // 2, roll(roll(v, -(S2 // 2), 1), 1, 0), roll(v, S2 // 2, 1))

    def up3(v):
        return jnp.where(chunk >= S2 // 2, roll(roll(v, S2 // 2, 1), -1, 0), roll(v, -(S2 // 2), 1))

    def lap_all(w, vs, step, down, up):
        T = len(vs)
        out = []
        for t in range(T):
            v = vs[t]
            below = vs[t - 1] if t > 0 else roll(vs[T - 1], GY, 1)
            above = vs[t + 1] if t < T - 1 else roll(vs[0], -GY, 1)
            acc = w[F_DG, t] * v - w[F_XM, t] * below - w[F_XP, t] * above
            acc = acc - w[F_YM, t] * roll(v, step, 1) - w[F_YP, t] * roll(v, -step, 1)
            out.append(acc - w[F_ZM, t] * down(v) - w[F_ZP, t] * up(v))
        return out

    def complete_all(w, step, up):
        T = w.shape[1]
        for t in range(T):
            w[F_INV, t] = 1.0 / w[F_DG, t]
            w[F_XP, t] = w[F_XM, t + 1] if t < T - 1 else roll(w[F_XM, 0], -GY, 1)
            w[F_YP, t] = roll(w[F_YM, t], -step, 1)
            w[F_ZP, t] = up(w[F_ZM, t])

    def world():
        def apply2(v):
            return lap_all(w2, v, S2, down2, up2)

        def apply3(v):
            return lap_all(w3, v, 2 * S2, down3, up3)

        def scaled(w, r):
            return [w[F_INV, t] * r[t] for t in range(len(r))]

        def minus(a, b):
            return [x - y for x, y in zip(a, b)]

        def plus(*many):
            return [sum(vs[1:], vs[0]) for vs in zip(*many)]

        def first(w, r):
            return [d * (1.0 / MID) for d in scaled(w, r)]

        def follow(w, u, r, one, two):
            return [one * a + two * d for a, d in zip(u, scaled(w, r))]

        r = [cres[k] for k in range(T2)]
        u = first(w2, r)
        r = minus(r, apply2(u))
        u2 = follow(w2, u, r, C_ONE, C_TWO)
        total = plus(u, u2)
        r = minus(r, apply2(u2))
        rc = [pair(pair(r[0] + r[1], S2), 1)]
        u = first(w3, rc)
        rc = minus(rc, apply3(u))
        v = follow(w3, u, rc, C_ONE, C_TWO)
        e = plus(u, v)
        rc = minus(rc, apply3(v))
        e = plus(e, follow(w3, v, rc, C_THREE, C_FOUR))
        e = [e[0]] * T2
        total = plus(total, e)
        r = minus(r, apply2(e))
        u = first(w2, r)
        r = minus(r, apply2(u))
        total = plus(total, u, follow(w2, u, r, C_ONE, C_TWO))
        for k in range(T2):
            e2[k, HALO : HALO + NS] = total[k]

    def precondition():
        world()
        for d in range(3):
            for k in range(T2):
                line = e2[k, pl.ds(slab + HALO - 1 + d, 1)]
                v = jnp.where(own_chunk, jnp.broadcast_to(line, (S2, LANES)), 0.0)
                v = pair(pair(v, 1), 2)
                for t in (2 * k, 2 * k + 1):
                    for half in range(2):
                        ua[t, pl.ds(HALO + 2 * S2 * d + half, S2, stride=2)] = v

        def put1(k, v):
            for t in (2 * k, 2 * k + 1):
                for half in range(2):
                    va[t, pl.ds(half, W1, stride=2)] = v

        after(w1, ua, ub, rr1, s1, r1, put1, 2)

        def put0(t, v):
            vz[t, HALO : HALO + W] = v

        after(w0, va, vb, rr, s0, r0, put0, 1)

    def total_of(v):
        return jnp.sum(jnp.sum(v, axis=0, keepdims=True), axis=1, keepdims=True)

    lane_1 = lane(1)

    def image_and_dots(par):
        rz = zaz = zq = None
        own = slice(HALO, HALO + S)
        for t in range(X):
            image = lap(w0, vz, t, 1)
            az[t] = image
            z = vz[t, 2 * HALO : 2 * HALO + S]
            parts = (r_ref[t, own] * z, z * image[own], z * q_ref[t, own])
            if t == 0:
                rz, zaz, zq = parts
            else:
                rz, zaz, zq = rz + parts[0], zaz + parts[1], zq + parts[2]
        msg[par, T2 : T2 + 1] = jnp.where(
            lane_1 == 0, total_of(rz), jnp.where(lane_1 == 1, total_of(zaz), total_of(zq))
        )

    def lane_of(v, i):
        return jnp.sum(jnp.where(lane_1 == i, v, 0.0), axis=1, keepdims=True)

    def scalars(rz_old, pq_old):
        sums = jnp.sum(gathered(T2), axis=0, keepdims=True)
        rz, zaz, zq = lane_of(sums, 0), lane_of(sums, 1), lane_of(sums, 2)
        beta = rz / rz_old
        pq = zaz + 2.0 * beta * zq + beta * beta * pq_old
        return rz, pq, rz / pq, beta

    def advance(a, beta):
        for t in range(X):
            p = vz[t, HALO : HALO + HALO + S] + beta * p_ref[t]
            p_ref[t] = p
            dir_ref[t] = dir_ref[t] + a * p
            q = az[t] + beta * q_ref[t]
            q_ref[t] = q
            r_ref[t] = r_ref[t] - a * q

    def coarse_advance(a, beta):
        for k in range(T2):
            v = gathered(C_ROW[0] + k) + beta * cq[k]
            cq[k] = v
            cres[k] = gathered(C_ROW[1] + k) - a * v

    def kept_advance(par, a, beta):
        for i, (keep, slope) in enumerate(((s1, sq1), (r1, rq1), (s0, sq), (r0, rq))):
            moved, first, count, size = halo_parts[i]
            base, other, _, _ = halo_parts[4 + i]
            for t in range(count):
                for rows, got in (
                    (slice(0, HALO), lambda ref, at: hb[par, 0, at + t]),
                    (slice(HALO, HALO + size), lambda ref, at: ref[t, HALO : HALO + size]),
                    (slice(HALO + size, 2 * HALO + size), lambda ref, at: hb[par, 1, at + t]),
                ):
                    if a is None:
                        keep[t, rows] = got(moved, first)
                    else:
                        v = got(moved, first) + beta * slope[t, rows]
                        slope[t, rows] = v
                        keep[t, rows] = got(base, other) - a * v

    all_others(lambda dev: pltpu.make_async_remote_copy(
        src_ref=wmsg, dst_ref=wgath.at[pl.ds(pl.multiple_of(slab * HALO, HALO), HALO)],
        send_sem=g_ssem.at[2], recv_sem=g_rsem.at[2], device_id=dev, device_id_type=MESH,
    ))
    wgath[pl.ds(pl.multiple_of(slab * HALO, HALO), HALO)] = wmsg[...]
    for side, there, dev in ((0, has_lo, lo_dev), (1, has_hi, hi_dev)):
        @pl.when(there)
        def _():
            pltpu.make_async_remote_copy(
                src_ref=w1.at[pl.ds(0, 4), :, pl.ds(HALO, HALO)], dst_ref=sh.at[1 - side],
                send_sem=h_ssem.at[2, side], recv_sem=h_rsem.at[2, 1 - side],
                device_id=dev, device_id_type=MESH,
            ).start()
    presmooth(0, 1)
    msg[0, T2:] = jnp.zeros((T2 + 1, LANES), f32)
    spread_message(0)
    halo_send(0, 1)

    for a in range(len(arrays)):
        for wanted, copy in pieces(a):
            @pl.when(wanted)
            def _():
                copy.wait_send()

    others = wgath.at[pl.ds(0, (NS - 1) * HALO)]
    pltpu.make_async_copy(others, others, g_rsem.at[2]).wait()
    pltpu.make_async_copy(others, others, g_ssem.at[2]).wait()
    for field in range(4):
        for k in range(T2):
            w2[field, k] = wgath[pl.ds(field * T2 + k, NS, stride=HALO)]
    complete_all(w2, S2, up2)
    dg, xm, ym, zm = F_DG, F_XM, F_YM, F_ZM
    ym_all = w2[ym, 0] + w2[ym, 1]
    ym_all = pair(ym_all, 1)
    zm_all = pair(w2[zm, 0] + w2[zm, 1], S2)
    between = pair(pair(w2[xm, 1], S2), 1) + pick_high(ym_all, S2) + pick_high(zm_all, 1)
    w3[dg, 0] = pair(pair(w2[dg, 0] + w2[dg, 1], S2), 1) - 2.0 * between
    w3[xm, 0] = pair(pair(w2[xm, 0], S2), 1)
    w3[ym, 0] = pick_low(ym_all, S2)
    w3[zm, 0] = pick_low(zm_all, 1)
    complete_all(w3, 2 * S2, up3)
    for side, there in ((0, has_lo), (1, has_hi)):
        @pl.when(there)
        def _():
            view = sh.at[side]
            pltpu.make_async_copy(view, view, h_rsem.at[2, side]).wait()
            pltpu.make_async_copy(view, view, h_ssem.at[2, side]).wait()
            first = 0 if side == 0 else HALO + S1
            for field in range(4):
                w1[field, :, first : first + HALO] = sh[side, field]
    complete1()
    wait_message(0)
    for k in range(T2):
        cres[k] = gathered(k)
    halo_wait(0, 1)
    kept_advance(0, None, None)

    def body(it_idx, carry):
        par = lax.rem(it_idx + 1, 2)
        precondition()
        image_and_dots(par)
        presmooth(par, 2)
        spread_message(par)
        halo_send(par, 2)
        wait_message(par)
        rz, pq, a, beta = scalars(*carry)
        coarse_advance(a, beta)
        advance(a, beta)
        halo_wait(par, 2)
        kept_advance(par, a, beta)
        return rz, pq

    one = jnp.ones((1, 1), f32)
    carry = lax.fori_loop(0, ITERS - 1, body, (one, jnp.zeros((1, 1), f32)))
    last = ITERS % 2
    precondition()
    image_and_dots(last)
    spread_message(last)
    wait_message(last)
    _, _, a, beta = scalars(*carry)
    advance(a, beta)

    def back_copy(which, jd):
        dev = device_at(jd, iz)
        return pltpu.make_async_remote_copy(
            src_ref=outs.at[which, dev[0] * ny + dev[1]],
            dst_ref=back.at[which, pl.ds(pl.multiple_of(S * j, HALO), S)],
            send_sem=d_ssem.at[which, MID_PART, jd],
            recv_sem=d_rsem.at[which, MID_PART],
            device_id=dev,
            device_id_type=MESH,
        )

    for which in range(2):
        for at in range(0, S, HALO):
            if which == 0:
                tiles = [dir_ref[t, HALO + at : 2 * HALO + at] for t in range(X)]
            else:
                tiles = [r_ref[t, HALO + at : 2 * HALO + at] for t in range(X)]
            tiles = block_transpose(tiles)
            for t in range(X):
                outs[which, t, at : at + HALO] = tiles[t]
        for jd in range(P):
            @pl.when(j != jd)
            def _():
                back_copy(which, jd).start()
        back[which, pl.ds(pl.multiple_of(S * j, HALO), S)] = outs[which, own_tile]

    def energy(g):
        square = 1.0 + g * g
        return (square * jnp.sqrt(square) - 1.0) * (1.0 / 3.0)

    lanes = lane(S)
    y_at = lax.rem(lanes, GY)
    x_first, x_last, y_first = lanes < GY, lanes >= LANES - GY, y_at == 0
    ends = jnp.where(y_at == GY - 1, 1.0, 0.0) + jnp.where(slab * S + row(S) == NZ - 1, 1.0, 0.0)
    ends_x = ends + jnp.where(x_last, 1.0, 0.0)
    fetch = lax.rem(lane_1, GY)
    packed = jnp.zeros((1, LANES), f32)
    for k in range(TRIALS):
        s = jnp.exp2(-jnp.full((1, LANES), tp_ref[k], jnp.int32).astype(f32))

        def trial(t, shift):
            first = 2 * HALO - shift
            return f_it[t, first : first + S] + s * dir_ref[t, HALO - shift : HALO - shift + S]

        below = jnp.where(x_first, 0.0, roll(trial(X - 1, 0), GY, 1))
        for t in range(X):
            v = trial(t, 0)
            e = energy(v - below) + energy(v - trial(t, 1))
            e = e + energy(v - jnp.where(y_first, 0.0, roll(v, 1, 1)))
            e = e + energy(v) * (ends_x if t == X - 1 else ends)
            e = e + (0.5 * f_rea[t, HALO : HALO + S] * v - f_src[t, HALO : HALO + S]) * v
            column = jnp.sum(e, axis=0, keepdims=True)
            step = 1
            while step < GY:
                column = pair(column, step)
                step *= 2
            packed = packed + jnp.where(fetch == k * X + t, column, 0.0)
            below = v
    emsg[...] = packed
    egath[slab] = packed
    all_others(lambda dev: pltpu.make_async_remote_copy(
        src_ref=emsg, dst_ref=egath.at[slab],
        send_sem=g_ssem.at[3], recv_sem=g_rsem.at[3], device_id=dev, device_id_type=MESH,
    ))
    for which, out in ((0, dir_out), (1, rem_out)):
        view = back.at[which, pl.ds(0, S * (P - 1))]
        pltpu.make_async_copy(view, view, d_rsem.at[which, MID_PART]).wait()
        out[...] = back[which].T.reshape(X, Y, Z)
        for jd in range(P):
            @pl.when(j != jd)
            def _():
                back_copy(which, jd).wait_send()
    others = egath.at[pl.ds(0, NS - 1)]
    pltpu.make_async_copy(others, others, g_rsem.at[3]).wait()
    pltpu.make_async_copy(others, others, g_ssem.at[3]).wait()
    layers = jnp.sum(egath[...], axis=0) / (GY * NZ)
    here = jnp.where(lane_1 // GY == ix, layers, 0.0)
    at_k = lax.broadcasted_iota(jnp.int32, (TRIALS * X, LANES), 0)
    mine = jnp.sum(jnp.where(lax.rem(lane(TRIALS * X), GY) == at_k, here, 0.0), axis=1, keepdims=True)
    mine = jnp.where(lane(TRIALS * X) == lax.rem(at_k, X), mine, 0.0)
    for k in range(TRIALS):
        le_ref[k : k + 1] = jnp.sum(mine[k * X : k * X + X], axis=0, keepdims=True)[:, :X]
        total = jnp.sum(jnp.where(fetch // X == k, layers, 0.0), axis=1, keepdims=True) / (X * nx)
        en_ref[k : k + 1] = jnp.broadcast_to(total, (1, LANES))


def slab_on_device(counts, iterate, source, reaction, trial_powers):
    X, Y, Z = iterate.shape
    nx, ny, nz = counts
    P = nx * ny
    S = Z // P
    NS = nz * P
    W, W1 = S + 2 * HALO, S // 2 + 2 * HALO
    T1, T2, T3 = X // 2, X // 4, X // 8
    f32 = jnp.float32

    def vm(*shape):
        return pltpu.VMEM(shape, f32)

    def sem(*shape):
        return pltpu.SemaphoreType.DMA(shape)

    full, padded = (X, W, LANES), (X, W + 2 * HALO, LANES)
    full1, padded1 = (T1, W1, LANES), (T1, W1 + 2 * HALO, LANES)
    scratch = [vm(3, Z, LANES), vm(P, S + 4 * HALO, LANES), vm(P, W, LANES), vm(P, W, LANES)]
    scratch += [vm(*padded), vm(*full), vm(*full)]
    scratch += [vm(8, *full), vm(8, *full1), vm(8, T2, NS, LANES), vm(8, T3, NS, LANES)]
    scratch += [vm(*padded)] * 5 + [vm(*full)] * 11
    scratch += [vm(*padded1)] * 4 + [vm(*full1)] * 12
    scratch += [vm(T2, NS + 2 * HALO, LANES), vm(T2, NS, LANES), vm(T2, NS, LANES)]
    scratch += [vm(X, S + HALO, LANES)] * 2 + [vm(*full)] * 2
    scratch += [vm(2, 2 * T2 + 1, LANES), vm(2, NS, 2 * T2 + 1, LANES), vm(NS * HALO, LANES)]
    scratch += [vm(HALO, LANES), vm(NS * HALO, LANES)]
    scratch += [vm(2, 2, 4 * (X + T1), HALO, LANES), vm(2, 4, T1, HALO, LANES)]
    scratch += [vm(1, LANES), vm(NS, 1, LANES), vm(2, P, S, LANES), vm(2, Z, LANES)]
    scratch += [sem(3, 3, P), sem(3, 3), sem(4), sem(4), sem(3, 2), sem(3, 2)]
    whole = pl.BlockSpec(memory_space=pltpu.VMEM)
    out = pl.pallas_call(
        functools.partial(slab_kernel, (X, Y, Z), counts),
        out_shape=[
            jax.ShapeDtypeStruct((X, Y, Z), f32),
            jax.ShapeDtypeStruct((X, Y, Z), f32),
            jax.ShapeDtypeStruct((TRIALS, X), f32),
            jax.ShapeDtypeStruct((TRIALS, LANES), f32),
        ],
        in_specs=[pl.BlockSpec(memory_space=pltpu.SMEM), whole, whole, whole],
        out_specs=[whole] * 4,
        scratch_shapes=scratch,
        compiler_params=pltpu.CompilerParams(has_side_effects=True, vmem_limit_bytes=48 * 1024 * 1024),
        name="newton_step",
    )(trial_powers, iterate, source, reaction)
    return out[0], out[1], out[2], out[3][:, 0]


def solution(mesh):
    counts = tuple(mesh.shape[axis] for axis in ("gx", "gy", "gz"))
    grid = P("gx", "gy", "gz")

    def on_each(iterate, source, reaction, trial_powers):
        form = slab_on_device if slab_fits(counts, iterate.shape) else on_device
        return form(counts, iterate, source, reaction, trial_powers)

    return jax.shard_map(
        on_each,
        mesh=mesh,
        in_specs=(grid, grid, grid, P()),
        out_specs=(grid, grid, P(None, "gx"), P()),
        check_vma=False,
    )
```

```python
import functools

import jax
import jax.numpy as jnp
from jax import lax
from jax.experimental import pallas as pl
from jax.experimental.pallas import tpu as pltpu
from jax.sharding import PartitionSpec as P

ITERS = 4
LEVELS = 4
TRIALS = 4
MID = 1.15
HALF = 0.85
SIGMA = MID / HALF
RHO0 = 1.0 / SIGMA
RHO1 = 1.0 / (2.0 * SIGMA - RHO0)
RHO2 = 1.0 / (2.0 * SIGMA - RHO1)
ROUND = 3
KEPT = ROUND
DG, INV, XM, XP, YM, YP, ZM, ZP, YB, ZB = range(10)
MESH = pl.DeviceIdType.MESH


class Grid:
    def __init__(self, Y, Z):
        self.Y, self.Z = Y, Z

    def rows_of(self, x):
        return lax.rem(lax.broadcasted_iota(jnp.int32, (x * self.Y, self.Z), 0), self.Y)

    def lanes_of(self, x):
        return lax.broadcasted_iota(jnp.int32, (x * self.Y, self.Z), 1)

    def pair_x(self, v):
        Y = self.Y
        x = v.shape[0] // Y
        return cat([v[2 * i * Y : (2 * i + 1) * Y] + v[(2 * i + 1) * Y : (2 * i + 2) * Y] for i in range(x // 2)])

    def pick_x(self, v, odd):
        Y = self.Y
        x = v.shape[0] // Y
        return cat([v[(2 * i + odd) * Y : (2 * i + odd + 1) * Y] for i in range(x // 2)])

    def bit(self, v, level, axis):
        at = self.rows_of(v.shape[0] // self.Y) if axis == 0 else self.lanes_of(v.shape[0] // self.Y)
        return lax.rem(at, 2 << level) < (1 << level)

    def pair(self, v, level, axis):
        step = 1 << level
        return v + jnp.where(self.bit(v, level, axis), roll(v, -step, axis), roll(v, step, axis))

    def pick(self, v, level, axis, odd):
        step = 1 << level
        low = self.bit(v, level, axis)
        if odd:
            return jnp.where(low, roll(v, -step, axis), v)
        return jnp.where(low, v, roll(v, step, axis))

    def restrict(self, v, level):
        return self.pair(self.pair(self.pair_x(v), level, 0), level, 1)

    def prolong(self, v):
        Y = self.Y
        x = v.shape[0] // Y
        return cat([v[(i // 2) * Y : (i // 2 + 1) * Y] for i in range(2 * x)])

    def coarsen(self, ws, reaction, level):
        xm, xp, ym, yp, zm, zp = ws
        pair, pick = self.pair, self.pick
        ws = (
            pair(pair(self.pick_x(xm, 0), level, 0), level, 1),
            pair(pair(self.pick_x(xp, 1), level, 0), level, 1),
            pair(pick(self.pair_x(ym), level, 0, 0), level, 1),
            pair(pick(self.pair_x(yp), level, 0, 1), level, 1),
            pick(pair(self.pair_x(zm), level, 0), level, 1, 0),
            pick(pair(self.pair_x(zp), level, 0), level, 1, 1),
        )
        return ws, self.restrict(reaction, level)

    def put(self, w, level, ws, reaction):
        Y, Z = self.Y, self.Z
        xm, xp, ym, yp, zm, zp = ws
        step = 1 << level
        x = xm.shape[0] // Y
        rows, lanes = self.rows_of(x), self.lanes_of(x)
        diagonal = reaction + xm + xp + ym + yp + zm + zp
        zero = jnp.zeros_like(xm)
        w[DG] = diagonal
        w[INV] = 1.0 / diagonal
        w[XM] = xm
        w[XP] = xp
        w[YM] = jnp.where(rows < step, zero, ym)
        w[YP] = jnp.where(rows >= Y - step, zero, yp)
        w[ZM] = jnp.where(lanes < step, zero, zm)
        w[ZP] = jnp.where(lanes >= Z - step, zero, zp)
        if w.shape[0] > YB:
            w[YB] = jnp.where(rows < step, ym, jnp.where(rows >= Y - step, yp, zero))
            w[ZB] = jnp.where(lanes < step, zm, jnp.where(lanes >= Z - step, zp, zero))

    def inner(self, w, v, level):
        step = 1 << level
        acc = w[DG] * v
        acc = acc - w[YM] * roll(v, step, 0) - w[YP] * roll(v, -step, 0)
        acc = acc - w[ZM] * roll(v, step, 1) - w[ZP] * roll(v, -step, 1)
        Y = self.Y
        if v.shape[0] > Y:
            none = jnp.zeros((Y, self.Z), jnp.float32)
            acc = acc - w[XM] * cat([none, v[:-Y]]) - w[XP] * cat([v[Y:], none])
        return acc


def cat(parts):
    return parts[0] if len(parts) == 1 else jnp.concatenate(parts, axis=0)


def roll(v, shift, axis):
    return pltpu.roll(v, shift % v.shape[axis], axis)


def dot(a, b):
    return lax.dot_general(
        a, b, (((1,), (0,)), ((), ())), precision=lax.Precision.HIGHEST, preferred_element_type=jnp.float32
    )


def kernel(
    sizes, counts, tp_ref, it_ref, src_ref, rea_ref, dir_ref, rem_ref, le_ref, en_ref,
    sx, rx, sy, ry, sz, rz, ssem, rsem, lev0, lev1, glev2, glev3, p_ref, q_ref,
    phx, phy, phz, dhx, dhy, dhz, dot_all, en_all, red_ssem, red_rsem,
    picked, gat_pl, gat_x, set_pl, set_x, glob,
):
    X, Y, Z = sizes
    nx, ny, nz = counts
    planes = ny * nz
    levs = (lev0, lev1)
    L = len(levs)
    x_own, y_own, z_own = X >> L, Y >> L, Z >> L
    GY, GZ = ny * y_own, nz * z_own
    here, world = Grid(Y, Z), Grid(GY, GZ)
    rows_of, lanes_of = here.rows_of, here.lanes_of
    ix, iy, iz = lax.axis_index("gx"), lax.axis_index("gy"), lax.axis_index("gz")
    has = (ix > 0, ix < nx - 1, iy > 0, iy < ny - 1, iz > 0, iz < nz - 1)
    devs = (
        (ix - 1, iy, iz), (ix + 1, iy, iz), (ix, iy - 1, iz),
        (ix, iy + 1, iz), (ix, iy, iz - 1), (ix, iy, iz + 1),
    )
    send = (sx, sx, sy, sy, sz, sz)
    recv = (rx, rx, ry, ry, rz, rz)
    lane_y = lax.broadcasted_iota(jnp.int32, (Y, Z), 1)
    lane_1 = lax.broadcasted_iota(jnp.int32, (1, Z), 1)

    for d in range(6):
        @pl.when(jnp.logical_not(has[d]))
        def _():
            recv[d][:, d % 2] = jnp.zeros(recv[d].shape[:1] + recv[d].shape[2:], jnp.float32)

    def outgoing(d, slot):
        side = d % 2
        return pltpu.make_async_remote_copy(
            src_ref=send[d].at[slot, side],
            dst_ref=recv[d].at[slot, 1 - side],
            send_sem=ssem.at[slot, d],
            recv_sem=rsem.at[slot, d + 1 - 2 * side],
            device_id=devs[d],
            device_id_type=MESH,
        )

    def incoming(d, slot):
        side = d % 2
        return pltpu.make_async_remote_copy(
            src_ref=send[d].at[slot, side],
            dst_ref=recv[d].at[slot, side],
            send_sem=ssem.at[slot, d],
            recv_sem=rsem.at[slot, d],
            device_id=devs[d],
            device_id_type=MESH,
        )

    def go(d, slot):
        @pl.when(has[d])
        def _():
            outgoing(d, slot).start()

    def start(v, slot):
        x = v.shape[0] // Y
        sx[slot, 0] = v[:Y]
        sx[slot, 1] = v[-Y:]
        go(0, slot)
        go(1, slot)
        for i in range(x):
            sy[slot, 0, i : i + 1] = v[i * Y : i * Y + 1]
            sy[slot, 1, i : i + 1] = v[i * Y + Y - 1 : i * Y + Y]
        go(2, slot)
        go(3, slot)
        for side, lane in ((0, 0), (1, Z - 1)):
            packed = jnp.broadcast_to(v[:Y, lane : lane + 1], (Y, Z))
            for i in range(1, x):
                part = jnp.broadcast_to(v[i * Y : i * Y + Y, lane : lane + 1], (Y, Z))
                packed = jnp.where(lane_y == i, part, packed)
            sz[slot, side] = packed
        go(4, slot)
        go(5, slot)

    def finish(slot):
        for d in range(6):
            @pl.when(has[d])
            def _():
                copy = incoming(d, slot)
                copy.wait_recv()
                copy.wait_send()

    def wide_y(half, x):
        return cat([jnp.broadcast_to(half[i : i + 1], (Y, Z)) for i in range(x)])

    def wide_z(half, x):
        return cat([jnp.broadcast_to(half[:, i : i + 1], (Y, Z)) for i in range(x)])

    def beyond(w, acc, in_x0, in_x1, in_y, in_z):
        x = acc.shape[0] // Y
        acc = acc - w[YB] * in_y - w[ZB] * in_z
        low = w[XM, :Y] * in_x0
        high = w[XP, (x - 1) * Y :] * in_x1
        if x == 1:
            return acc - low - high
        return cat([acc[:Y] - low] + ([acc[Y:-Y]] if x > 2 else []) + [acc[-Y:] - high])

    def operate(v, level, slot):
        w = levs[level]
        x = X >> level
        start(v, slot)
        acc = here.inner(w, v, level)
        finish(slot)
        in_y = jnp.where(rows_of(x) < Y // 2, wide_y(ry[slot, 0], x), wide_y(ry[slot, 1], x))
        in_z = jnp.where(lanes_of(x) < Z // 2, wide_z(rz[slot, 0], x), wide_z(rz[slot, 1], x))
        return beyond(w, acc, rx[slot, 0], rx[slot, 1], in_y, in_z)

    turn = [0]

    def apply(v, level):
        slot = turn[0] % ROUND
        turn[0] += 1
        return operate(v, level, slot)

    def vcycle(r, level, part):
        w = levs[level]
        u = w[INV] * r * (1.0 / MID)
        total = u
        r = r - apply(u, level)
        u = RHO1 * RHO0 * u + 2.0 * RHO1 / HALF * w[INV] * r
        total = total + u
        r = r - apply(u, level)
        coarse = here.restrict(r, level)
        if level + 1 < L:
            e = here.prolong(vcycle(coarse, level + 1, part))
            r = r - apply(e, level)
        else:
            everywhere = collect(coarse, 1, part, gat_pl, gat_x, 4)
            e, ends = spread(world_cycle(everywhere[0], level + 1))
            r = r - beyond(w, here.inner(w, e, level), *ends)
        total = total + e
        u = w[INV] * r * (1.0 / MID)
        total = total + u
        r = r - apply(u, level)
        u = RHO1 * RHO0 * u + 2.0 * RHO1 / HALF * w[INV] * r
        return total + u

    def world_cycle(r, level):
        w = (glev2, glev3)[level - L]

        def apply(v):
            return world.inner(w, v, level - L)

        u = w[INV] * r * (1.0 / MID)
        total = u
        r = r - apply(u)
        u = RHO1 * RHO0 * u + 2.0 * RHO1 / HALF * w[INV] * r
        total = total + u
        r = r - apply(u)
        if level == LEVELS - 1:
            u = RHO2 * RHO1 * u + 2.0 * RHO2 / HALF * w[INV] * r
            return total + u
        e = world.prolong(world_cycle(world.restrict(r, level - L), level + 1))
        total = total + e
        r = r - apply(e)
        u = w[INV] * r * (1.0 / MID)
        total = total + u
        r = r - apply(u)
        u = RHO1 * RHO0 * u + 2.0 * RHO1 / HALF * w[INV] * r
        return total + u

    def hot(shape, wanted):
        at = lax.broadcasted_iota(jnp.int32, shape, 0)
        return jnp.where(at == wanted, 1.0, 0.0)

    def collect(v, fields, part, pl_ref, x_ref, which):
        count = fields * x_own * y_own
        picked[: fields * x_own * Y] = v
        own = picked[pl.ds(0, count, stride=1 << L), :]
        lane = lax.broadcasted_iota(jnp.int32, (Z, GZ), 1) - iz * z_own
        inside = jnp.logical_and(lane >= 0, lane < z_own)
        put = hot((Z, GZ), jnp.where(inside, lane * (1 << L), -1))
        pl_ref[part, my_plane] = dot(own, put)
        gather(pl_ref, part, planes, my_plane, in_plane, which)
        for j in range(ny):
            rows = pl_ref[part, j * nz]
            for k in range(1, nz):
                rows = rows + pl_ref[part, j * nz + k]
            for i in range(fields * x_own):
                x_ref[part, ix, i * GY + j * y_own : i * GY + (j + 1) * y_own] = rows[i * y_own : (i + 1) * y_own]
        gather(x_ref, part, nx, ix, in_column, which + 1)
        return [
            cat([x_ref[part, d, f * x_own * GY : (f + 1) * x_own * GY] for d in range(nx)]) for f in range(fields)
        ]

    def spread(v):
        lane = lax.broadcasted_iota(jnp.int32, (GZ, Z), 1)
        inside = hot((GZ, Z), iz * z_own + lane // (1 << L))
        outside = hot((GZ, Z), jnp.where(lane < Z // 2, iz * z_own - 1, iz * z_own + z_own))
        glob[0, GY : GY + nx * x_own * GY] = dot(v, inside)
        glob[1, GY : GY + nx * x_own * GY] = dot(v, outside)
        rows = rows_of(1)

        def layer(which, a):
            base = (ix * x_own + 1 + a) * GY + iy * y_own
            out = jnp.broadcast_to(glob[which, pl.ds(base, 1), :], (Y, Z))
            for j in range(1, y_own):
                row = jnp.broadcast_to(glob[which, pl.ds(base + j, 1), :], (Y, Z))
                out = jnp.where(rows < j << L, out, row)
            return out

        def rims(a):
            base = (ix * x_own + 1 + a) * GY + iy * y_own
            low = glob[0, pl.ds(base - 1, 1), :] * has_low
            high = glob[0, pl.ds(base + y_own, 1), :] * has_high
            return jnp.where(rows < Y // 2, jnp.broadcast_to(low, (Y, Z)), jnp.broadcast_to(high, (Y, Z)))

        has_low = jnp.where(iy > 0, 1.0, 0.0)
        has_high = jnp.where(iy < ny - 1, 1.0, 0.0)
        own = range(x_own)
        e = here.prolong(cat([layer(0, a) for a in own]))
        in_y = here.prolong(cat([rims(a) for a in own]))
        in_z = here.prolong(cat([layer(1, a) for a in own]))
        return e, (layer(0, -1), layer(0, x_own), in_y, in_z)

    def gather(ref, part, count, me, device, which):
        for j in range(count):
            @pl.when(me != j)
            def _():
                pltpu.make_async_remote_copy(
                    src_ref=ref.at[part, me],
                    dst_ref=ref.at[part, me],
                    send_sem=red_ssem.at[which, part],
                    recv_sem=red_rsem.at[which, part],
                    device_id=device(j),
                    device_id_type=MESH,
                ).start()
        if count > 1:
            others = ref.at[part, pl.ds(0, count - 1)]
            pltpu.make_async_copy(others, others, red_rsem.at[which, part]).wait()
            pltpu.make_async_copy(others, others, red_ssem.at[which, part]).wait()

    def in_plane(j):
        return (ix, j // nz, j % nz)

    def in_column(j):
        return (j, iy, iz)

    def in_grid(j):
        return (j // planes, j // nz % ny, j % nz)

    my_plane = iy * nz + iz
    me = ix * planes + my_plane

    def reduce_plane(ref, part, value, which):
        ref[part, my_plane] = value
        gather(ref, part, planes, my_plane, in_plane, which)
        return jnp.sum(ref[part], axis=0)

    def reduce_column(ref, part, value, which):
        ref[part, ix] = value
        gather(ref, part, nx, ix, in_column, which)
        return jnp.sum(ref[part], axis=0)

    def total_of(v):
        return jnp.sum(jnp.sum(v, axis=0, keepdims=True), axis=1, keepdims=True)

    def lane_of(row, i):
        return jnp.sum(jnp.where(lane_1 == i, row, 0.0), axis=1, keepdims=True)

    it = it_ref[...].reshape(X * Y, Z)
    reaction = rea_ref[...].reshape(X * Y, Z)
    start(it, KEPT)
    finish(KEPT)
    rows, lanes = rows_of(X), lanes_of(X)
    last_row, last_lane = rows == Y - 1, lanes == Z - 1
    n_xm = cat([rx[KEPT, 0], it[:-Y]])
    n_xp = cat([it[Y:], rx[KEPT, 1]])
    n_ym = jnp.where(rows == 0, wide_y(ry[KEPT, 0], X), roll(it, 1, 0))
    n_yp = jnp.where(last_row, wide_y(ry[KEPT, 1], X), roll(it, -1, 0))
    n_zm = jnp.where(lanes == 0, wide_z(rz[KEPT, 0], X), roll(it, 1, 1))
    n_zp = jnp.where(last_lane, wide_z(rz[KEPT, 1], X), roll(it, -1, 1))
    ws = []
    r = src_ref[...].reshape(X * Y, Z) - reaction * it
    for sign, n in ((-1, n_xm), (1, n_xp), (-1, n_ym), (1, n_yp), (-1, n_zm), (1, n_zp)):
        g = n - it
        square = g * g
        root = jnp.sqrt(1.0 + square)
        ws.append((1.0 + 2.0 * square) / root)
        r = r + g * root
    rem_ref[...] = r.reshape(X, Y, Z)
    here.put(levs[0], 0, ws, reaction)
    for level in range(L):
        ws, reaction = here.coarsen(ws, reaction, level)
        if level + 1 < L:
            here.put(levs[level + 1], level + 1, ws, reaction)
    glob[...] = jnp.zeros_like(glob)
    *ws, reaction = collect(cat(list(ws) + [reaction]), 7, 0, set_pl, set_x, 6)
    world.put(glev2, 0, ws, reaction)
    world.put(glev3, 1, *world.coarsen(ws, reaction, 0))
    for ref in (p_ref, q_ref, phx, phy, phz, dhx, dhy, dhz):
        ref[...] = jnp.zeros_like(ref)
    dir_ref[...] = jnp.zeros_like(dir_ref)

    def body(it_idx, carry):
        rz_old, pq_old = carry
        part = lax.rem(it_idx, 2)
        r = rem_ref[...].reshape(X * Y, Z)
        turn[0] = 0
        z = vcycle(r, 0, part)
        z_slot = turn[0] % ROUND
        az = apply(z, 0)
        q_old = q_ref[...]
        sums = jnp.where(
            lane_1 == 0,
            total_of(rem_ref[...].reshape(X * Y, Z) * z),
            jnp.where(lane_1 == 1, total_of(z * az), total_of(z * q_old)),
        )
        dot_all[part, me] = sums
        gather(dot_all, part, nx * planes, me, in_grid, 0)
        row = jnp.sum(dot_all[part], axis=0)
        rz_new, zaz, zq = lane_of(row, 0), lane_of(row, 1), lane_of(row, 2)
        beta = rz_new / rz_old
        pq = zaz + 2.0 * beta * zq + beta * beta * pq_old
        a = rz_new / pq
        p = z + beta * p_ref[...]
        q = az + beta * q_old
        p_ref[...] = p
        q_ref[...] = q
        dir_ref[...] = dir_ref[...] + (a * p).reshape(X, Y, Z)
        rem_ref[...] = rem_ref[...] - (a * q).reshape(X, Y, Z)
        for got, ph, dh in ((rx, phx, dhx), (ry, phy, dhy), (rz, phz, dhz)):
            for side in range(2):
                edge = got[z_slot, side] + beta * ph[side]
                ph[side] = edge
                dh[side] = dh[side] + a * edge
        return rz_new, pq

    one = jnp.ones((1, 1), jnp.float32)
    lax.fori_loop(0, ITERS, body, (one, jnp.zeros((1, 1), jnp.float32)))

    it = it_ref[...].reshape(X * Y, Z)
    step_dir = dir_ref[...].reshape(X * Y, Z)

    def energy(g):
        square = 1.0 + g * g
        return (square * jnp.sqrt(square) - 1.0) * (1.0 / 3.0)

    ends_y = jnp.where(jnp.logical_and(last_row, iy == ny - 1), 1.0, 0.0)
    ends_z = jnp.where(jnp.logical_and(last_lane, iz == nz - 1), 1.0, 0.0)
    ends_x = jnp.where(ix == nx - 1, 1.0, 0.0)
    across = lax.broadcasted_iota(jnp.int32, (X, Z), 0) == lax.broadcasted_iota(jnp.int32, (X, Z), 1)
    trial_rows = []
    for k in range(TRIALS):
        s = jnp.exp2(-jnp.full((1, Z), tp_ref[k], jnp.int32).astype(jnp.float32))
        v = it + s * step_dir
        low_x = cat([rx[KEPT, 0] + s * dhx[0], v[:-Y]])
        low_y = jnp.where(rows == 0, wide_y(ry[KEPT, 0] + s * dhy[0], X), roll(v, 1, 0))
        low_z = jnp.where(lanes == 0, wide_z(rz[KEPT, 0] + s * dhz[0], X), roll(v, 1, 1))
        at_end = energy(v)
        e = energy(v - low_x) + energy(v - low_y) + energy(v - low_z)
        e = e + at_end * (ends_y + ends_z)
        e = cat([e[:-Y], e[-Y:] + ends_x * at_end[-Y:]]) if X > 1 else e + ends_x * at_end
        e = e + 0.5 * rea_ref[...].reshape(X * Y, Z) * v * v - src_ref[...].reshape(X * Y, Z) * v
        by_layer = jnp.sum(jnp.sum(e.reshape(X, Y, Z), axis=1), axis=1, keepdims=True)
        trial_rows.append(jnp.sum(jnp.where(across, by_layer, 0.0), axis=0, keepdims=True))
    en_all[0, me] = jnp.concatenate(trial_rows, axis=0)
    gather(en_all, 0, nx * planes, me, in_grid, 2)
    layers = jnp.sum(en_all[0, pl.ds(ix * planes, planes)], axis=0)
    layers = layers / (Y * ny * Z * nz)
    le_ref[...] = layers[:, :X]
    overall = jnp.sum(en_all[0], axis=0) / (Y * ny * Z * nz)
    overall = jnp.sum(overall, axis=1, keepdims=True) / (X * nx)
    en_ref[...] = jnp.broadcast_to(overall, (TRIALS, Z))


def on_device(counts, iterate, source, reaction, trial_powers):
    X, Y, Z = iterate.shape
    nx, ny, nz = counts
    f32 = jnp.float32
    slots = ROUND + 1
    vm = pltpu.VMEM
    scratch = [vm((slots, 2, rows, Z), f32) for rows in (Y, Y, X, X, Y, Y)]
    scratch += [pltpu.SemaphoreType.DMA((slots, 6))] * 2
    x_own, y_own = X // 4, Y // 4
    GX, GY, GZ = nx * x_own, ny * y_own, nz * Z // 4
    scratch += [vm((10, (X >> level) * Y, Z), f32) for level in range(2)]
    scratch += [vm((8, (GX >> level) * GY, GZ), f32) for level in range(2)]
    scratch += [vm((X * Y, Z), f32)] * 2
    scratch += [vm((2, rows, Z), f32) for rows in (Y, X, Y)] * 2
    scratch += [
        vm((2, nx * ny * nz, 1, Z), f32),
        vm((1, nx * ny * nz, TRIALS, Z), f32),
        pltpu.SemaphoreType.DMA((8, 2)), pltpu.SemaphoreType.DMA((8, 2)),
        vm((7 * x_own * Y, Z), f32),
        vm((2, ny * nz, x_own * y_own, GZ), f32), vm((2, nx, x_own * GY, GZ), f32),
        vm((1, ny * nz, 7 * x_own * y_own, GZ), f32), vm((1, nx, 7 * x_own * GY, GZ), f32),
        vm((2, (GX + 2) * GY, Z), f32),
    ]
    whole = pl.BlockSpec(memory_space=pltpu.VMEM)
    out = pl.pallas_call(
        functools.partial(kernel, (X, Y, Z), counts),
        out_shape=[
            jax.ShapeDtypeStruct((X, Y, Z), f32),
            jax.ShapeDtypeStruct((X, Y, Z), f32),
            jax.ShapeDtypeStruct((TRIALS, X), f32),
            jax.ShapeDtypeStruct((TRIALS, Z), f32),
        ],
        in_specs=[pl.BlockSpec(memory_space=pltpu.SMEM), whole, whole, whole],
        out_specs=[whole] * 4,
        scratch_shapes=scratch,
        compiler_params=pltpu.CompilerParams(has_side_effects=True, vmem_limit_bytes=48 * 1024 * 1024),
        name="newton_step",
    )(trial_powers, iterate, source, reaction)
    return out[0], out[1], out[2], out[3][:, 0]


LANES = 128
HALO = 8
PLANES = 2
PAIR = 2
CHUNK = 4
F_DG, F_XM, F_YM, F_ZM, F_XP, F_YP, F_ZP, F_INV = range(8)
C_ONE = RHO1 * RHO0
C_TWO = 2.0 * RHO1 / HALF
C_THREE = RHO2 * RHO1
C_FOUR = 2.0 * RHO2 / HALF


def slab_fits(counts, shape):
    X, Y, Z = shape
    nx, ny, nz = counts
    per = PLANES * ny * PAIR
    rows = PAIR * Z // per
    return (
        X == 1 << (LEVELS - 1) and X * Y == LANES and nx * ny == X and nx >= PLANES and nz % PAIR == 0
        and rows * per == PAIR * Z and rows % (2 * HALO) == 0 and Z % rows == 0
    )


def slab_kernel(
    sizes, counts, tp_ref, it_in, src_in, rea_in, dir_out, rem_out, le_ref, en_ref,
    turned, d_it, d_rs, f_it, f_rea, f_src, w0, w1, w2, w3,
    va, vb, vz, rr, az, sa, ra, sb, rb, s0, r0, sq, rq,
    ua, ub, r1in, rr1, sa1, ra1, sb1, rb1, s1, r1, sq1, rq1, e2, cres, cq, cnew,
    p_ref, dir_ref, q_ref, r_ref,
    msg, gath, early, egath, wmsg, wgath, hb, he, sh, enmsg, engath, outs, back,
    d_ssem, d_rsem, g_ssem, g_rsem, h_ssem, h_rsem, b_ssem, b_rsem, e_ssem,
):
    X, Y, Z = sizes
    nx, ny, nz = counts
    P = nx * ny
    GY = ny * Y
    NZ = nz * Z
    PER = PLANES * ny
    NS = PER * nz
    S = NZ // NS
    BLOCK = Z // S
    W = S + 2 * HALO
    f32 = jnp.float32
    ix, iy, iz = lax.axis_index("gx"), lax.axis_index("gy"), lax.axis_index("gz")
    me = (ix * ny + iy) * nz + iz
    own_tile = ix * ny + iy
    base = (nx - PLANES) // 2

    def fold(value, turn, size):
        return value + lax.rem(turn, 2) * (size - 1 - 2 * value)

    def device_of(s):
        c = s // PAIR
        plane = c // PER
        q = fold(lax.rem(c, PER), plane, PER)
        y = q // PLANES
        return (base + fold(lax.rem(q, PLANES), y, PLANES), y, plane * PAIR + lax.rem(s, PAIR))

    works = jnp.logical_and(ix >= base, ix < base + PLANES)
    plane = iz // PAIR
    slab = fold(iy * PLANES + fold(ix - base, iy, PLANES), plane, PER)
    slab = (plane * PER + slab) * PAIR + lax.rem(iz, PAIR)
    slab = jnp.where(works, slab, -BLOCK - 1)
    block = slab // BLOCK
    j = lax.rem(slab, BLOCK)

    has_lo, has_hi = slab > 0, slab < NS - 1
    lo_dev, hi_dev = device_of(jnp.maximum(slab - 1, 0)), device_of(jnp.clip(slab + 1, 0, NS - 1))

    def lane(n):
        return lax.broadcasted_iota(jnp.int32, (n, LANES), 1)

    def row(n):
        return lax.broadcasted_iota(jnp.int32, (n, LANES), 0)

    def low_bit(n, step):
        return lax.rem(lane(n), 2 * step) < step

    def swap(v, step):
        return jnp.where(low_bit(v.shape[0], step), roll(v, -step, 1), roll(v, step, 1))

    def pair(v, step):
        return v + swap(v, step)

    def pick_low(v, step):
        return jnp.where(low_bit(v.shape[0], step), v, roll(v, step, 1))

    def pick_high(v, step):
        return jnp.where(low_bit(v.shape[0], step), roll(v, -step, 1), v)

    def block_transpose(tiles):
        n = tiles[0].shape[0]
        k = P // 2
        while k:
            low = low_bit(n, Y * k)
            new = list(tiles)
            for i in range(P):
                if not i & k:
                    a, b = tiles[i], tiles[i | k]
                    new[i] = jnp.where(low, a, roll(b, Y * k, 1))
                    new[i | k] = jnp.where(low, roll(a, -Y * k, 1), b)
            tiles = new
            k //= 2
        return tiles

    parts = ((pl.ds(0, 1), d_it, 2 * HALO), (pl.ds(1, 2), d_rs, HALO))

    def pieces(a):
        halo = parts[a][2]
        for jd in range(BLOCK):
            first = S * jd - (halo if jd > 0 else 0)
            last = S * jd + S + (halo if jd < BLOCK - 1 else 0)
            yield BLOCK * iz + jd, None, first, last - first, 0 if jd > 0 else halo, jd
        yield BLOCK * iz + BLOCK, iz < nz - 1, Z - halo, halo, 0, BLOCK
        yield BLOCK * iz - 1, iz > 0, 0, halo, halo + S, BLOCK + 1

    def piece(a, to, first, count, there, number):
        which, landed, _ = parts[a]
        return pltpu.make_async_remote_copy(
            src_ref=turned.at[which, pl.ds(first, count)],
            dst_ref=landed.at[:, own_tile, pl.ds(there, count)],
            send_sem=d_ssem.at[a, number],
            recv_sem=d_rsem.at[a, max(number - BLOCK + 1, 0)],
            device_id=device_of(jnp.clip(to, 0, NS - 1)),
            device_id_type=MESH,
        )

    def both(a, b):
        return b if a is None else jnp.logical_and(a, b)

    @pl.when(works)
    def _():
        for ref in (va, vb, vz, ua, ub, r1in, e2, p_ref, dir_ref, q_ref, sq, rq, sq1, rq1, cq, w1):
            ref[...] = jnp.zeros_like(ref)
        w1[F_DG] = jnp.ones(w1.shape[1:], f32)
        for side, at in ((0, 0), (1, NS - 1)):
            @pl.when(slab == at)
            def _():
                for ref in (hb, he):
                    ref[:, side] = jnp.zeros(ref.shape[:1] + ref.shape[2:], f32)

    for a, (which, landed, halo) in enumerate(parts):
        for i, given in ((0, it_in),) if a == 0 else ((1, rea_in), (2, src_in)):
            turned[i] = given[...].reshape(LANES, Z).T
        for to, exists, first, count, there, number in pieces(a):
            @pl.when(both(exists, to != slab))
            def _():
                piece(a, to, first, count, there, number).start()

            @pl.when(both(exists, to == slab))
            def _():
                landed[:, own_tile, there : there + count] = turned[which, first : first + count]

    def wait_sent():
        for a in range(2):
            for to, exists, first, count, there, number in pieces(a):
                @pl.when(both(exists, to != slab))
                def _():
                    piece(a, to, first, count, there, number).wait_send()

    def wait_landed(a, wanted, kind, first, count, source):
        mine = jnp.where(source == iz, 1, 0)
        for own in range(2):
            @pl.when(jnp.logical_and(wanted, mine == own))
            def _():
                view = parts[a][1].at[:, pl.ds(0, P - own), pl.ds(first, count)]
                pltpu.make_async_copy(view, view, d_rsem.at[a, kind]).wait()

    def gather_block():
        for a, (_, landed, halo) in enumerate(parts):
            @pl.when(slab == 0)
            def _():
                landed[:, :, :halo] = jnp.zeros((landed.shape[0], P, halo, LANES), f32)

            @pl.when(slab == NS - 1)
            def _():
                landed[:, :, halo + S :] = jnp.zeros((landed.shape[0], P, halo, LANES), f32)

            for jd in range(BLOCK):
                count = S + (halo if jd > 0 else 0) + (halo if jd < BLOCK - 1 else 0)
                wait_landed(a, j == jd, 0, 0 if jd > 0 else halo, count, block)
            wait_landed(a, jnp.logical_and(j == 0, has_lo), 1, 0, halo, block - 1)
            wait_landed(a, jnp.logical_and(j == BLOCK - 1, has_hi), 2, halo + S, halo, block + 1)
            for i, flat in ((0, f_it),) if a == 0 else ((0, f_rea), (1, f_src)):
                for at in range(0, S + 2 * halo, HALO):
                    tiles = block_transpose([landed[i, t, at : at + HALO] for t in range(P)])
                    for t in range(P):
                        flat[t, at : at + HALO] = tiles[t]

    def back_copy(which, t):
        return pltpu.make_async_remote_copy(
            src_ref=outs.at[which, t],
            dst_ref=back.at[which, pl.ds(pl.multiple_of(S * j, HALO), S)],
            send_sem=b_ssem.at[which, t],
            recv_sem=b_rsem.at[which],
            device_id=(t // ny, t % ny, block),
            device_id_type=MESH,
        )

    def back_here(which):
        @pl.when(block == iz)
        def _():
            back[which, pl.ds(pl.multiple_of(S * j, HALO), S)] = outs[which, own_tile]

    def energy_copy(dev):
        return pltpu.make_async_remote_copy(
            src_ref=enmsg, dst_ref=engath.at[slab],
            send_sem=e_ssem.at[(dev[0] * ny + dev[1]) * nz + dev[2]], recv_sem=g_rsem.at[5],
            device_id=dev, device_id_type=MESH,
        )

    WROWS = 4 * (X // 4) * (S // (4 * CHUNK))

    @pl.when(works)
    def _():
        gather_block()

        lanes = lane(W)
        z_at = slab * S + row(W) - HALO
        inside = jnp.logical_and(z_at >= 0, z_at < NZ)
        z_low = jnp.logical_and(z_at > 0, z_at < NZ)
        z_high = jnp.logical_and(z_at >= 0, z_at < NZ - 1)
        x_first, x_last = lanes < GY, lanes >= LANES - GY
        y_at = lax.rem(lanes, GY)
        y_first, y_last = y_at == 0, y_at == GY - 1

        def face(g):
            square = g * g
            root = jnp.sqrt(1.0 + square)
            return (1.0 + 2.0 * square) / root, g * root

        def window(t):
            return f_it[t, HALO : HALO + W]

        low_w, low_p = face(window(0) - jnp.where(x_first, 0.0, roll(window(X - 1), GY, 1)))
        first_w = low_w
        for t in range(X):
            c = window(t)
            beyond = window(t + 1) if t < X - 1 else jnp.where(x_last, 0.0, roll(window(0), -GY, 1))
            high_w, high_p = face(beyond - c)
            yl_w, yl_p = face(c - jnp.where(y_first, 0.0, roll(c, 1, 1)))
            yh_w, yh_p = face(jnp.where(y_last, 0.0, roll(c, -1, 1)) - c)
            zl_w, zl_p = face(c - f_it[t, HALO - 1 : HALO - 1 + W])
            zh_w, zh_p = face(f_it[t, HALO + 1 : HALO + 1 + W] - c)
            rea = f_rea[t]
            diagonal = rea + low_w + high_w + yl_w + yh_w + zl_w + zh_w
            w0[F_DG, t] = diagonal
            w0[F_INV, t] = 1.0 / diagonal
            w0[F_XM, t] = jnp.where(x_first, 0.0, low_w) if t == 0 else low_w
            w0[F_XP, t] = jnp.where(x_last, 0.0, high_w) if t == X - 1 else high_w
            w0[F_YM, t] = jnp.where(y_first, 0.0, yl_w)
            w0[F_YP, t] = jnp.where(y_last, 0.0, yh_w)
            w0[F_ZM, t] = jnp.where(z_low, zl_w, 0.0)
            w0[F_ZP, t] = jnp.where(z_high, zh_w, 0.0)
            r = f_src[t] - rea * c + (high_p - low_p) + (yh_p - yl_p) + (zh_p - zl_p)
            r = jnp.where(inside, r, 0.0)
            az[t] = r
            r_ref[t] = r
            low_w, low_p = high_w, high_p

        def coarsen(get, step):
            def build(k):
                def both(field, t):
                    low, high = get(field, t)
                    return low + high
                lo, hi = 2 * k, 2 * k + 1
                xm = pair(both(F_XM, lo), step)
                ym_all = both(F_YM, lo) + both(F_YM, hi)
                zl0, zh0 = get(F_ZM, lo)
                zl1, zh1 = get(F_ZM, hi)
                between = pair(both(F_XM, hi), step) + pick_high(ym_all, step) + pair(zh0 + zh1, step)
                diagonal = pair(both(F_DG, lo) + both(F_DG, hi), step) - 2.0 * between
                return diagonal, xm, pick_low(ym_all, step), pair(zl0 + zl1, step)
            return build

        n1 = W // 2
        S1 = S // 2
        W1 = S1 + 2 * HALO
        T1 = X // 2
        at1 = (W1 - n1) // 2

        def halves0(field, t):
            return w0[field, t, pl.ds(0, n1, stride=2)], w0[field, t, pl.ds(1, n1, stride=2)]

        for k in range(T1):
            for field, value in zip((F_DG, F_XM, F_YM, F_ZM), coarsen(halves0, 1)(k)):
                w1[field, k, at1 : at1 + n1] = value

        def complete1():
            for k in range(T1):
                w1[F_INV, k] = 1.0 / w1[F_DG, k]
                w1[F_XP, k] = w1[F_XM, k + 1] if k < T1 - 1 else roll(w1[F_XM, 0], -GY, 1)
                w1[F_YP, k] = roll(w1[F_YM, k], -2, 1)
                w1[F_ZP, k] = roll(w1[F_ZM, k], -1, 0)

        complete1()

        S2 = S // 4
        T2 = X // 4
        LINES = S2 // CHUNK

        def halves1(field, t):
            return w1[field, t, pl.ds(HALO, S2, stride=2)], w1[field, t, pl.ds(HALO + 1, S2, stride=2)]

        own_chunk = lax.rem(lane(S2), CHUNK) == lax.rem(row(S2), CHUNK)

        def pack(ref, first, v):
            v = jnp.where(own_chunk, v, 0.0)
            for h in range(LINES):
                ref[first + h : first + h + 1] = jnp.sum(jnp.where(row(S2) // CHUNK == h, v, 0.0), axis=0, keepdims=True)

        for k in range(T2):
            for field, value in zip((F_DG, F_XM, F_YM, F_ZM), coarsen(halves1, 2)(k)):
                pack(wmsg, (field * T2 + k) * LINES, value)

        def laps(w, vs, t, step):
            T, n = w.shape[1], w.shape[2]
            mid = slice(HALO, HALO + n)
            weights = [w[field, t] for field in range(F_INV)]
            out = []
            for v in vs:
                c = v[t, mid]
                below = v[t - 1, mid] if t > 0 else roll(v[T - 1, mid], GY, 1)
                above = v[t + 1, mid] if t < T - 1 else roll(v[0, mid], -GY, 1)
                acc = weights[F_DG] * c - weights[F_XM] * below - weights[F_XP] * above
                acc = acc - weights[F_YM] * roll(c, step, 1) - weights[F_YP] * roll(c, -step, 1)
                acc = acc - weights[F_ZM] * v[t, HALO - 1 : HALO - 1 + n]
                out.append(acc - weights[F_ZP] * v[t, HALO + 1 : HALO + 1 + n])
            return out

        def lap(w, v, t, step):
            return laps(w, [v], t, step)[0]

        def centre(v, t, n):
            return v[t, HALO : HALO + n]

        def before(w, r_of, u1, u2, rem1, s_out, r_out, step):
            T, n = w.shape[1], w.shape[2]
            mid = slice(HALO, HALO + n)
            for t in range(T):
                u1[t, mid] = w[F_INV, t] * r_of[t] * (1.0 / MID)
            for t in range(T):
                r = r_of[t] - lap(w, u1, t, step)
                first = centre(u1, t, n)
                u = C_ONE * first + C_TWO * w[F_INV, t] * r
                u2[t, mid] = u
                s_out[t] = first + u
                rem1[t] = r
            for t in range(T):
                r_out[t] = rem1[t] - lap(w, u2, t, step)

        def after(w, e, u1, rem1, s_in, r_in, put, step):
            T, n = w.shape[1], w.shape[2]
            mid = slice(HALO, HALO + n)
            for t in range(T):
                r = r_in[t] - lap(w, e, t, step)
                rem1[t] = r
                u1[t, mid] = w[F_INV, t] * r * (1.0 / MID)
            for t in range(T):
                r = rem1[t] - lap(w, u1, t, step)
                u = centre(u1, t, n)
                put(t, s_in[t] + centre(e, t, n) + u + (C_ONE * u + C_TWO * w[F_INV, t] * r))

        kept = ((az, sa, ra, sa1, ra1), (r_ref, sb, rb, sb1, rb1))

        def presmooth(f, ref, par):
            r_of, s_out, r_out, s1_out, r1_out = kept[f]
            before(w0, r_of, va, vb, rr, s_out, r_out, 1)
            for k in range(T1):
                total = None
                for t in (2 * k, 2 * k + 1):
                    part = r_out[t, pl.ds(0, n1, stride=2)] + r_out[t, pl.ds(1, n1, stride=2)]
                    total = part if total is None else total + part
                r1in[k, at1 : at1 + n1] = pair(total, 1)
            before(w1, r1in, ua, ub, rr1, s1_out, r1_out, 2)
            for k in range(T2):
                total = None
                for t in (2 * k, 2 * k + 1):
                    part = r1_out[t, pl.ds(HALO, S2, stride=2)] + r1_out[t, pl.ds(HALO + 1, S2, stride=2)]
                    total = part if total is None else total + part
                pack(ref.at[par], k * LINES, pair(total, 2))

        def to_workers(ref, out, sem):
            for s in range(NS):
                @pl.when(slab != s)
                def _():
                    pltpu.make_async_remote_copy(
                        src_ref=ref, dst_ref=out.at[slab], send_sem=g_ssem.at[sem], recv_sem=g_rsem.at[sem],
                        device_id=device_of(s), device_id_type=MESH,
                    ).start()
            out[slab] = ref[...]

        def from_workers(out, sem):
            others = out.at[pl.ds(0, NS - 1)]
            pltpu.make_async_copy(others, others, g_rsem.at[sem]).wait()
            pltpu.make_async_copy(others, others, g_ssem.at[sem]).wait()

        def unpack(out, packed):
            for k in range(T2):
                for s in range(NS):
                    out[k, s * LINES : (s + 1) * LINES] = packed[s, k * LINES : (k + 1) * LINES]

        per = 2 * (X + T1)
        halo_parts = tuple(
            ((of[3], 0, T1, S1), (of[4], T1, T1, S1), (of[1], 2 * T1, X, S), (of[2], 2 * T1 + X, X, S)) for of in kept
        )
        halo_at = (hb, he)

        def halo_send(f, par):
            for side, there, dev in ((0, has_lo, lo_dev), (1, has_hi, hi_dev)):
                @pl.when(there)
                def _():
                    for ref, first, count, size in halo_parts[f]:
                        start_row = HALO if side == 0 else size
                        pltpu.make_async_remote_copy(
                            src_ref=ref.at[:, pl.ds(start_row, HALO)],
                            dst_ref=halo_at[f].at[par, 1 - side, pl.ds(first, count)],
                            send_sem=h_ssem.at[2 * f + par, side],
                            recv_sem=h_rsem.at[2 * f + par, 1 - side],
                            device_id=dev,
                            device_id_type=MESH,
                        ).start()

        def halo_wait(view_of, sem):
            for side, there in ((0, has_lo), (1, has_hi)):
                @pl.when(there)
                def _():
                    view = view_of(side)
                    pltpu.make_async_copy(view, view, h_rsem.at[sem, side]).wait()
                    pltpu.make_async_copy(view, view, h_ssem.at[sem, side]).wait()

        chunk = lax.rem(lane(NS * LINES), CHUNK)

        def down2(v):
            return jnp.where(chunk == 0, roll(roll(v, 1 - CHUNK, 1), 1, 0), roll(v, 1, 1))

        def up2(v):
            return jnp.where(chunk == CHUNK - 1, roll(roll(v, CHUNK - 1, 1), -1, 0), roll(v, -1, 1))

        def down3(v):
            return jnp.where(chunk < CHUNK // 2, roll(roll(v, -(CHUNK // 2), 1), 1, 0), roll(v, CHUNK // 2, 1))

        def up3(v):
            return jnp.where(chunk >= CHUNK // 2, roll(roll(v, CHUNK // 2, 1), -1, 0), roll(v, -(CHUNK // 2), 1))

        def lap_all(w, vs, step, down, up):
            T = len(vs)
            out = []
            for t in range(T):
                v = vs[t]
                below = vs[t - 1] if t > 0 else roll(vs[T - 1], GY, 1)
                above = vs[t + 1] if t < T - 1 else roll(vs[0], -GY, 1)
                acc = w[F_DG, t] * v - w[F_XM, t] * below - w[F_XP, t] * above
                acc = acc - w[F_YM, t] * roll(v, step, 1) - w[F_YP, t] * roll(v, -step, 1)
                out.append(acc - w[F_ZM, t] * down(v) - w[F_ZP, t] * up(v))
            return out

        def complete_all(w, step, up):
            T = w.shape[1]
            for t in range(T):
                w[F_INV, t] = 1.0 / w[F_DG, t]
                w[F_XP, t] = w[F_XM, t + 1] if t < T - 1 else roll(w[F_XM, 0], -GY, 1)
                w[F_YP, t] = roll(w[F_YM, t], -step, 1)
                w[F_ZP, t] = up(w[F_ZM, t])

        def world():
            def apply2(v):
                return lap_all(w2, v, CHUNK, down2, up2)

            def apply3(v):
                return lap_all(w3, v, 2 * CHUNK, down3, up3)

            def scaled(w, r):
                return [w[F_INV, t] * r[t] for t in range(len(r))]

            def minus(a, b):
                return [x - y for x, y in zip(a, b)]

            def plus(*many):
                return [sum(vs[1:], vs[0]) for vs in zip(*many)]

            def first(w, r):
                return [d * (1.0 / MID) for d in scaled(w, r)]

            def follow(w, u, r, one, two):
                return [one * a + two * d for a, d in zip(u, scaled(w, r))]

            r = [cres[k] for k in range(T2)]
            u = first(w2, r)
            r = minus(r, apply2(u))
            u2 = follow(w2, u, r, C_ONE, C_TWO)
            total = plus(u, u2)
            r = minus(r, apply2(u2))
            rc = [pair(pair(r[0] + r[1], CHUNK), 1)]
            u = first(w3, rc)
            rc = minus(rc, apply3(u))
            v = follow(w3, u, rc, C_ONE, C_TWO)
            e = plus(u, v)
            rc = minus(rc, apply3(v))
            e = plus(e, follow(w3, v, rc, C_THREE, C_FOUR))
            e = [e[0]] * T2
            total = plus(total, e)
            r = minus(r, apply2(e))
            u = first(w2, r)
            r = minus(r, apply2(u))
            total = plus(total, u, follow(w2, u, r, C_ONE, C_TWO))
            for k in range(T2):
                e2[k, HALO : HALO + NS * LINES] = total[k]

        def precondition():
            world()
            own = lax.rem(lane(CHUNK), CHUNK) == row(CHUNK)
            for d in range(LINES + 2):
                for k in range(T2):
                    line = e2[k, pl.ds(slab * LINES + HALO - 1 + d, 1)]
                    v = jnp.where(own, jnp.broadcast_to(line, (CHUNK, LANES)), 0.0)
                    v = pair(pair(v, 1), 2)
                    for t in (2 * k, 2 * k + 1):
                        for half in range(2):
                            ua[t, pl.ds(HALO + 2 * CHUNK * d + half, CHUNK, stride=2)] = v

            def put1(k, v):
                for t in (2 * k, 2 * k + 1):
                    for half in range(2):
                        va[t, pl.ds(half, W1, stride=2)] = v

            after(w1, ua, ub, rr1, s1, r1, put1, 2)

            def put0(t, v):
                vz[t, HALO : HALO + W] = v

            after(w0, va, vb, rr, s0, r0, put0, 1)

        def total_of(v):
            return jnp.sum(jnp.sum(v, axis=0, keepdims=True), axis=1, keepdims=True)

        lane_1 = lane(1)

        def image_and_dots(par):
            rz = zaz = zq = None
            own = slice(HALO, HALO + S)
            for t in range(X):
                image = lap(w0, vz, t, 1)
                az[t] = image
                z = vz[t, 2 * HALO : 2 * HALO + S]
                parts = (r_ref[t, own] * z, z * image[own], z * q_ref[t, own])
                if t == 0:
                    rz, zaz, zq = parts
                else:
                    rz, zaz, zq = rz + parts[0], zaz + parts[1], zq + parts[2]
            msg[par, T2 * LINES :] = jnp.where(
                lane_1 == 0, total_of(rz), jnp.where(lane_1 == 1, total_of(zaz), total_of(zq))
            )

        def lane_of(v, i):
            return jnp.sum(jnp.where(lane_1 == i, v, 0.0), axis=1, keepdims=True)

        def scalars(par, rz_old, pq_old):
            sums = gath[par, 0, T2 * LINES :]
            for s in range(1, NS):
                sums = sums + gath[par, s, T2 * LINES :]
            rz, zaz, zq = lane_of(sums, 0), lane_of(sums, 1), lane_of(sums, 2)
            beta = rz / rz_old
            pq = zaz + 2.0 * beta * zq + beta * beta * pq_old
            return rz, pq, rz / pq, beta

        def advance(a, beta):
            for t in range(X):
                p = vz[t, HALO : HALO + HALO + S] + beta * p_ref[t]
                p_ref[t] = p
                dir_ref[t] = dir_ref[t] + a * p
                q = az[t] + beta * q_ref[t]
                q_ref[t] = q
                r_ref[t] = r_ref[t] - a * q

        def coarse_advance(par, a, beta, fresh):
            unpack(cnew, gath.at[par])
            if fresh:
                unpack(cres, egath.at[par])
            for k in range(T2):
                v = cnew[k] + beta * cq[k]
                cq[k] = v
                cres[k] = cres[k] - a * v

        def kept_advance(par, a, beta, fresh):
            for i, (keep, slope) in enumerate(((s1, sq1), (r1, rq1), (s0, sq), (r0, rq))):
                moved, first, count, size = halo_parts[0][i]
                true = halo_parts[1][i][0]
                for t in range(count):
                    for side, rows in ((0, slice(0, HALO)), (None, slice(HALO, HALO + size)), (1, slice(HALO + size, 2 * HALO + size))):
                        got = moved[t, rows] if side is None else hb[par, side, first + t]
                        if a is None:
                            keep[t, rows] = got
                            continue
                        v = got + beta * slope[t, rows]
                        slope[t, rows] = v
                        if not fresh:
                            start = keep[t, rows]
                        else:
                            start = true[t, rows] if side is None else he[par, side, first + t]
                        keep[t, rows] = start - a * v

        for s in range(NS):
            @pl.when(slab != s)
            def _():
                pltpu.make_async_remote_copy(
                    src_ref=wmsg, dst_ref=wgath.at[pl.ds(pl.multiple_of(slab * WROWS, HALO), WROWS)],
                    send_sem=g_ssem.at[4], recv_sem=g_rsem.at[4], device_id=device_of(s), device_id_type=MESH,
                ).start()
        wgath[pl.ds(pl.multiple_of(slab * WROWS, HALO), WROWS)] = wmsg[...]
        for side, there, dev in ((0, has_lo, lo_dev), (1, has_hi, hi_dev)):
            @pl.when(there)
            def _():
                pltpu.make_async_remote_copy(
                    src_ref=w1.at[pl.ds(0, 4), :, pl.ds(HALO if side == 0 else S1, HALO)], dst_ref=sh.at[1 - side],
                    send_sem=h_ssem.at[4, side], recv_sem=h_rsem.at[4, 1 - side],
                    device_id=dev, device_id_type=MESH,
                ).start()
        presmooth(0, msg, 0)
        msg[0, T2 * LINES :] = jnp.zeros((1, LANES), f32)
        to_workers(msg.at[0], gath.at[0], 0)
        halo_send(0, 0)
        wait_sent()

        others = wgath.at[pl.ds(0, (NS - 1) * WROWS)]
        pltpu.make_async_copy(others, others, g_rsem.at[4]).wait()
        pltpu.make_async_copy(others, others, g_ssem.at[4]).wait()
        for field in range(4):
            for k in range(T2):
                for h in range(LINES):
                    line = (field * T2 + k) * LINES + h
                    w2[field, k, pl.ds(h, NS, stride=LINES)] = wgath[pl.ds(line, NS, stride=WROWS)]
        complete_all(w2, CHUNK, up2)
        dg, xm, ym, zm = F_DG, F_XM, F_YM, F_ZM
        ym_all = pair(w2[ym, 0] + w2[ym, 1], 1)
        zm_all = pair(w2[zm, 0] + w2[zm, 1], CHUNK)
        between = pair(pair(w2[xm, 1], CHUNK), 1) + pick_high(ym_all, CHUNK) + pick_high(zm_all, 1)
        w3[dg, 0] = pair(pair(w2[dg, 0] + w2[dg, 1], CHUNK), 1) - 2.0 * between
        w3[xm, 0] = pair(pair(w2[xm, 0], CHUNK), 1)
        w3[ym, 0] = pick_low(ym_all, CHUNK)
        w3[zm, 0] = pick_low(zm_all, 1)
        complete_all(w3, 2 * CHUNK, up3)
        halo_wait(lambda side: sh.at[side], 4)
        for side, there in ((0, has_lo), (1, has_hi)):
            @pl.when(there)
            def _():
                first = 0 if side == 0 else HALO + S1
                for field in range(4):
                    w1[field, :, first : first + HALO] = sh[side, field]
        complete1()
        from_workers(gath.at[0], 0)
        unpack(cres, gath.at[0])
        halo_wait(lambda side: hb.at[0, side], 0)
        kept_advance(0, None, None, False)

        def step(par, fresh, carry):
            if fresh:
                presmooth(1, early, par)
                to_workers(early.at[par], egath.at[par], 2 + par)
                halo_send(1, par)
            precondition()
            image_and_dots(par)
            presmooth(0, msg, par)
            to_workers(msg.at[par], gath.at[par], par)
            halo_send(0, par)
            from_workers(gath.at[par], par)
            rz, pq, a, beta = scalars(par, *carry)
            if fresh:
                from_workers(egath.at[par], 2 + par)
            coarse_advance(par, a, beta, fresh)
            advance(a, beta)
            halo_wait(lambda side: hb.at[par, side], par)
            if fresh:
                halo_wait(lambda side: he.at[par, side], 2 + par)
            kept_advance(par, a, beta, fresh)
            return rz, pq

        carry = step(1, False, (jnp.ones((1, 1), f32), jnp.zeros((1, 1), f32)))
        carry = lax.fori_loop(1, ITERS - 1, lambda i, c: step(lax.rem(i + 1, 2), True, c), carry)
        last = ITERS % 2
        precondition()
        image_and_dots(last)
        to_workers(msg.at[last], gath.at[last], last)
        from_workers(gath.at[last], last)
        _, _, a, beta = scalars(last, *carry)
        advance(a, beta)

        for which in range(2):
            for at in range(0, S, HALO):
                ref = r_ref if which else dir_ref
                tiles = block_transpose([ref[t, HALO + at : 2 * HALO + at] for t in range(X)])
                for t in range(X):
                    outs[which, t, at : at + HALO] = tiles[t]
            for t in range(P):
                remote = jnp.logical_or(block != iz, own_tile != t)

                @pl.when(remote)
                def _():
                    back_copy(which, t).start()
            back_here(which)

        def energy(g):
            square = 1.0 + g * g
            return (square * jnp.sqrt(square) - 1.0) * (1.0 / 3.0)

        lanes = lane(S)
        y_at = lax.rem(lanes, GY)
        x_first, x_last, y_first = lanes < GY, lanes >= LANES - GY, y_at == 0
        ends = jnp.where(y_at == GY - 1, 1.0, 0.0) + jnp.where(slab * S + row(S) == NZ - 1, 1.0, 0.0)
        ends_x = ends + jnp.where(x_last, 1.0, 0.0)
        fetch = lax.rem(lane_1, GY)
        packed = jnp.zeros((1, LANES), f32)
        for k in range(TRIALS):
            s = jnp.exp2(-jnp.full((1, LANES), tp_ref[k], jnp.int32).astype(f32))

            def trial(t, shift):
                first = 2 * HALO - shift
                return f_it[t, first : first + S] + s * dir_ref[t, HALO - shift : HALO - shift + S]

            below = jnp.where(x_first, 0.0, roll(trial(X - 1, 0), GY, 1))
            for t in range(X):
                v = trial(t, 0)
                e = energy(v - below) + energy(v - trial(t, 1))
                e = e + energy(v - jnp.where(y_first, 0.0, roll(v, 1, 1)))
                e = e + energy(v) * (ends_x if t == X - 1 else ends)
                e = e + (0.5 * f_rea[t, HALO : HALO + S] * v - f_src[t, HALO : HALO + S]) * v
                column = jnp.sum(e, axis=0, keepdims=True)
                step = 1
                while step < GY:
                    column = pair(column, step)
                    step *= 2
                packed = packed + jnp.where(fetch == k * X + t, column, 0.0)
                below = v
        enmsg[...] = packed
        engath[slab] = packed
        for other in range(nx * ny * nz):
            @pl.when(me != other)
            def _():
                energy_copy((other // (ny * nz), other // nz % ny, other % nz)).start()
        for which in range(2):
            for t in range(P):
                @pl.when(jnp.logical_or(block != iz, own_tile != t))
                def _():
                    back_copy(which, t).wait_send()

    @pl.when(jnp.logical_not(works))
    def _():
        wait_sent()

    for which, out in ((0, dir_out), (1, rem_out)):
        for own in range(2):
            @pl.when(jnp.where(block == iz, 1, 0) == own)
            def _():
                view = back.at[which, pl.ds(0, Z - own * S)]
                pltpu.make_async_copy(view, view, b_rsem.at[which]).wait()
        out[...] = back[which].T.reshape(X, Y, Z)
    @pl.when(works)
    def _():
        others = engath.at[pl.ds(0, NS - 1)]
        pltpu.make_async_copy(others, others, g_rsem.at[5]).wait()
        for other in range(nx * ny * nz):
            @pl.when(me != other)
            def _():
                energy_copy((other // (ny * nz), other // nz % ny, other % nz)).wait_send()

    @pl.when(jnp.logical_not(works))
    def _():
        pltpu.make_async_copy(engath, engath, g_rsem.at[5]).wait()

    lane_1 = lane(1)
    fetch = lax.rem(lane_1, GY)
    layers = jnp.sum(engath[...], axis=0) / (GY * NZ)
    here = jnp.where(lane_1 // GY == ix, layers, 0.0)
    at_k = lax.broadcasted_iota(jnp.int32, (TRIALS * X, LANES), 0)
    mine = jnp.sum(jnp.where(lax.rem(lane(TRIALS * X), GY) == at_k, here, 0.0), axis=1, keepdims=True)
    mine = jnp.where(lane(TRIALS * X) == lax.rem(at_k, X), mine, 0.0)
    for k in range(TRIALS):
        le_ref[k : k + 1] = jnp.sum(mine[k * X : k * X + X], axis=0, keepdims=True)[:, :X]
        total = jnp.sum(jnp.where(fetch // X == k, layers, 0.0), axis=1, keepdims=True) / (X * nx)
        en_ref[k : k + 1] = jnp.broadcast_to(total, (1, LANES))


def slab_on_device(counts, iterate, source, reaction, trial_powers):
    X, Y, Z = iterate.shape
    nx, ny, nz = counts
    P = nx * ny
    NS = PLANES * ny * nz
    S = nz * Z // NS
    BLOCK = Z // S
    W, W1 = S + 2 * HALO, S // 2 + 2 * HALO
    T1, T2, T3 = X // 2, X // 4, X // 8
    LINES = S // (4 * CHUNK)
    C_ROWS, ROWS = T2 * LINES, NS * LINES
    f32 = jnp.float32

    def vm(*shape):
        return pltpu.VMEM(shape, f32)

    def sem(*shape):
        return pltpu.SemaphoreType.DMA(shape)

    full, padded = (X, W, LANES), (X, W + 2 * HALO, LANES)
    full1, padded1 = (T1, W1, LANES), (T1, W1 + 2 * HALO, LANES)
    scratch = [vm(3, Z, LANES), vm(1, P, W + 2 * HALO, LANES), vm(2, P, W, LANES)]
    scratch += [vm(*padded), vm(*full), vm(*full)]
    scratch += [vm(8, *full), vm(8, *full1), vm(8, T2, ROWS, LANES), vm(8, T3, ROWS, LANES)]
    scratch += [vm(*padded)] * 3 + [vm(*full)] * 10
    scratch += [vm(*padded1)] * 2 + [vm(*full1)] * 10
    scratch += [vm(T2, ROWS + 2 * HALO, LANES)] + [vm(T2, ROWS, LANES)] * 3
    scratch += [vm(X, S + HALO, LANES)] * 2 + [vm(*full)] * 2
    scratch += [vm(2, C_ROWS + 1, LANES), vm(2, NS, C_ROWS + 1, LANES), vm(2, C_ROWS, LANES), vm(2, NS, C_ROWS, LANES)]
    scratch += [vm(4 * C_ROWS, LANES), vm(NS * 4 * C_ROWS, LANES)]
    scratch += [vm(2, 2, 2 * (X + T1), HALO, LANES)] * 2 + [vm(2, 4, T1, HALO, LANES)]
    scratch += [vm(1, LANES), vm(NS, 1, LANES), vm(2, P, S, LANES), vm(2, Z, LANES)]
    scratch += [sem(2, BLOCK + 2), sem(2, 3), sem(6), sem(6), sem(5, 2), sem(5, 2), sem(2, P), sem(2), sem(nx * ny * nz)]
    whole = pl.BlockSpec(memory_space=pltpu.VMEM)
    out = pl.pallas_call(
        functools.partial(slab_kernel, (X, Y, Z), counts),
        out_shape=[
            jax.ShapeDtypeStruct((X, Y, Z), f32),
            jax.ShapeDtypeStruct((X, Y, Z), f32),
            jax.ShapeDtypeStruct((TRIALS, X), f32),
            jax.ShapeDtypeStruct((TRIALS, LANES), f32),
        ],
        in_specs=[pl.BlockSpec(memory_space=pltpu.SMEM), whole, whole, whole],
        out_specs=[whole] * 4,
        scratch_shapes=scratch,
        compiler_params=pltpu.CompilerParams(has_side_effects=True, vmem_limit_bytes=48 * 1024 * 1024),
        name="newton_step",
    )(trial_powers, iterate, source, reaction)
    return out[0], out[1], out[2], out[3][:, 0]


def solution(mesh):
    counts = tuple(mesh.shape[axis] for axis in ("gx", "gy", "gz"))
    grid = P("gx", "gy", "gz")

    def on_each(iterate, source, reaction, trial_powers):
        form = slab_on_device if slab_fits(counts, iterate.shape) else on_device
        return form(counts, iterate, source, reaction, trial_powers)

    return jax.shard_map(
        on_each,
        mesh=mesh,
        in_specs=(grid, grid, grid, P()),
        out_specs=(grid, grid, P(None, "gx"), P()),
        check_vma=False,
    )
```

```python
import functools

import jax
import jax.numpy as jnp
from jax import lax
from jax.experimental import pallas as pl
from jax.experimental.pallas import tpu as pltpu
from jax.sharding import PartitionSpec as P

ITERS = 4
LEVELS = 4
TRIALS = 4
MID = 1.15
HALF = 0.85
SIGMA = MID / HALF
RHO0 = 1.0 / SIGMA
RHO1 = 1.0 / (2.0 * SIGMA - RHO0)
RHO2 = 1.0 / (2.0 * SIGMA - RHO1)
ROUND = 3
KEPT = ROUND
DG, INV, XM, XP, YM, YP, ZM, ZP, YB, ZB = range(10)
MESH = pl.DeviceIdType.MESH


class Grid:
    def __init__(self, Y, Z):
        self.Y, self.Z = Y, Z

    def rows_of(self, x):
        return lax.rem(lax.broadcasted_iota(jnp.int32, (x * self.Y, self.Z), 0), self.Y)

    def lanes_of(self, x):
        return lax.broadcasted_iota(jnp.int32, (x * self.Y, self.Z), 1)

    def pair_x(self, v):
        Y = self.Y
        x = v.shape[0] // Y
        return cat([v[2 * i * Y : (2 * i + 1) * Y] + v[(2 * i + 1) * Y : (2 * i + 2) * Y] for i in range(x // 2)])

    def pick_x(self, v, odd):
        Y = self.Y
        x = v.shape[0] // Y
        return cat([v[(2 * i + odd) * Y : (2 * i + odd + 1) * Y] for i in range(x // 2)])

    def bit(self, v, level, axis):
        at = self.rows_of(v.shape[0] // self.Y) if axis == 0 else self.lanes_of(v.shape[0] // self.Y)
        return lax.rem(at, 2 << level) < (1 << level)

    def pair(self, v, level, axis):
        step = 1 << level
        return v + jnp.where(self.bit(v, level, axis), roll(v, -step, axis), roll(v, step, axis))

    def pick(self, v, level, axis, odd):
        step = 1 << level
        low = self.bit(v, level, axis)
        if odd:
            return jnp.where(low, roll(v, -step, axis), v)
        return jnp.where(low, v, roll(v, step, axis))

    def restrict(self, v, level):
        return self.pair(self.pair(self.pair_x(v), level, 0), level, 1)

    def prolong(self, v):
        Y = self.Y
        x = v.shape[0] // Y
        return cat([v[(i // 2) * Y : (i // 2 + 1) * Y] for i in range(2 * x)])

    def coarsen(self, ws, reaction, level):
        xm, xp, ym, yp, zm, zp = ws
        pair, pick = self.pair, self.pick
        ws = (
            pair(pair(self.pick_x(xm, 0), level, 0), level, 1),
            pair(pair(self.pick_x(xp, 1), level, 0), level, 1),
            pair(pick(self.pair_x(ym), level, 0, 0), level, 1),
            pair(pick(self.pair_x(yp), level, 0, 1), level, 1),
            pick(pair(self.pair_x(zm), level, 0), level, 1, 0),
            pick(pair(self.pair_x(zp), level, 0), level, 1, 1),
        )
        return ws, self.restrict(reaction, level)

    def put(self, w, level, ws, reaction):
        Y, Z = self.Y, self.Z
        xm, xp, ym, yp, zm, zp = ws
        step = 1 << level
        x = xm.shape[0] // Y
        rows, lanes = self.rows_of(x), self.lanes_of(x)
        diagonal = reaction + xm + xp + ym + yp + zm + zp
        zero = jnp.zeros_like(xm)
        w[DG] = diagonal
        w[INV] = 1.0 / diagonal
        w[XM] = xm
        w[XP] = xp
        w[YM] = jnp.where(rows < step, zero, ym)
        w[YP] = jnp.where(rows >= Y - step, zero, yp)
        w[ZM] = jnp.where(lanes < step, zero, zm)
        w[ZP] = jnp.where(lanes >= Z - step, zero, zp)
        if w.shape[0] > YB:
            w[YB] = jnp.where(rows < step, ym, jnp.where(rows >= Y - step, yp, zero))
            w[ZB] = jnp.where(lanes < step, zm, jnp.where(lanes >= Z - step, zp, zero))

    def inner(self, w, v, level):
        step = 1 << level
        acc = w[DG] * v
        acc = acc - w[YM] * roll(v, step, 0) - w[YP] * roll(v, -step, 0)
        acc = acc - w[ZM] * roll(v, step, 1) - w[ZP] * roll(v, -step, 1)
        Y = self.Y
        if v.shape[0] > Y:
            none = jnp.zeros((Y, self.Z), jnp.float32)
            acc = acc - w[XM] * cat([none, v[:-Y]]) - w[XP] * cat([v[Y:], none])
        return acc


def cat(parts):
    return parts[0] if len(parts) == 1 else jnp.concatenate(parts, axis=0)


def roll(v, shift, axis):
    return pltpu.roll(v, shift % v.shape[axis], axis)


def dot(a, b):
    return lax.dot_general(
        a, b, (((1,), (0,)), ((), ())), precision=lax.Precision.HIGHEST, preferred_element_type=jnp.float32
    )


def kernel(
    sizes, counts, tp_ref, it_ref, src_ref, rea_ref, dir_ref, rem_ref, le_ref, en_ref,
    sx, rx, sy, ry, sz, rz, ssem, rsem, lev0, lev1, glev2, glev3, p_ref, q_ref,
    phx, phy, phz, dhx, dhy, dhz, dot_all, en_all, red_ssem, red_rsem,
    picked, gat_pl, gat_x, set_pl, set_x, glob,
):
    X, Y, Z = sizes
    nx, ny, nz = counts
    planes = ny * nz
    levs = (lev0, lev1)
    L = len(levs)
    x_own, y_own, z_own = X >> L, Y >> L, Z >> L
    GY, GZ = ny * y_own, nz * z_own
    here, world = Grid(Y, Z), Grid(GY, GZ)
    rows_of, lanes_of = here.rows_of, here.lanes_of
    ix, iy, iz = lax.axis_index("gx"), lax.axis_index("gy"), lax.axis_index("gz")
    has = (ix > 0, ix < nx - 1, iy > 0, iy < ny - 1, iz > 0, iz < nz - 1)
    devs = (
        (ix - 1, iy, iz), (ix + 1, iy, iz), (ix, iy - 1, iz),
        (ix, iy + 1, iz), (ix, iy, iz - 1), (ix, iy, iz + 1),
    )
    send = (sx, sx, sy, sy, sz, sz)
    recv = (rx, rx, ry, ry, rz, rz)
    lane_y = lax.broadcasted_iota(jnp.int32, (Y, Z), 1)
    lane_1 = lax.broadcasted_iota(jnp.int32, (1, Z), 1)

    for d in range(6):
        @pl.when(jnp.logical_not(has[d]))
        def _():
            recv[d][:, d % 2] = jnp.zeros(recv[d].shape[:1] + recv[d].shape[2:], jnp.float32)

    def outgoing(d, slot):
        side = d % 2
        return pltpu.make_async_remote_copy(
            src_ref=send[d].at[slot, side],
            dst_ref=recv[d].at[slot, 1 - side],
            send_sem=ssem.at[slot, d],
            recv_sem=rsem.at[slot, d + 1 - 2 * side],
            device_id=devs[d],
            device_id_type=MESH,
        )

    def incoming(d, slot):
        side = d % 2
        return pltpu.make_async_remote_copy(
            src_ref=send[d].at[slot, side],
            dst_ref=recv[d].at[slot, side],
            send_sem=ssem.at[slot, d],
            recv_sem=rsem.at[slot, d],
            device_id=devs[d],
            device_id_type=MESH,
        )

    def go(d, slot):
        @pl.when(has[d])
        def _():
            outgoing(d, slot).start()

    def start(v, slot):
        x = v.shape[0] // Y
        sx[slot, 0] = v[:Y]
        sx[slot, 1] = v[-Y:]
        go(0, slot)
        go(1, slot)
        for i in range(x):
            sy[slot, 0, i : i + 1] = v[i * Y : i * Y + 1]
            sy[slot, 1, i : i + 1] = v[i * Y + Y - 1 : i * Y + Y]
        go(2, slot)
        go(3, slot)
        for side, lane in ((0, 0), (1, Z - 1)):
            packed = jnp.broadcast_to(v[:Y, lane : lane + 1], (Y, Z))
            for i in range(1, x):
                part = jnp.broadcast_to(v[i * Y : i * Y + Y, lane : lane + 1], (Y, Z))
                packed = jnp.where(lane_y == i, part, packed)
            sz[slot, side] = packed
        go(4, slot)
        go(5, slot)

    def finish(slot):
        for d in range(6):
            @pl.when(has[d])
            def _():
                copy = incoming(d, slot)
                copy.wait_recv()
                copy.wait_send()

    def wide_y(half, x):
        return cat([jnp.broadcast_to(half[i : i + 1], (Y, Z)) for i in range(x)])

    def wide_z(half, x):
        return cat([jnp.broadcast_to(half[:, i : i + 1], (Y, Z)) for i in range(x)])

    def beyond(w, acc, in_x0, in_x1, in_y, in_z):
        x = acc.shape[0] // Y
        acc = acc - w[YB] * in_y - w[ZB] * in_z
        low = w[XM, :Y] * in_x0
        high = w[XP, (x - 1) * Y :] * in_x1
        if x == 1:
            return acc - low - high
        return cat([acc[:Y] - low] + ([acc[Y:-Y]] if x > 2 else []) + [acc[-Y:] - high])

    def operate(v, level, slot):
        w = levs[level]
        x = X >> level
        start(v, slot)
        acc = here.inner(w, v, level)
        finish(slot)
        in_y = jnp.where(rows_of(x) < Y // 2, wide_y(ry[slot, 0], x), wide_y(ry[slot, 1], x))
        in_z = jnp.where(lanes_of(x) < Z // 2, wide_z(rz[slot, 0], x), wide_z(rz[slot, 1], x))
        return beyond(w, acc, rx[slot, 0], rx[slot, 1], in_y, in_z)

    turn = [0]

    def apply(v, level):
        slot = turn[0] % ROUND
        turn[0] += 1
        return operate(v, level, slot)

    def vcycle(r, level, part):
        w = levs[level]
        u = w[INV] * r * (1.0 / MID)
        total = u
        r = r - apply(u, level)
        u = RHO1 * RHO0 * u + 2.0 * RHO1 / HALF * w[INV] * r
        total = total + u
        r = r - apply(u, level)
        coarse = here.restrict(r, level)
        if level + 1 < L:
            e = here.prolong(vcycle(coarse, level + 1, part))
            r = r - apply(e, level)
        else:
            everywhere = collect(coarse, 1, part, gat_pl, gat_x, 4)
            e, ends = spread(world_cycle(everywhere[0], level + 1))
            r = r - beyond(w, here.inner(w, e, level), *ends)
        total = total + e
        u = w[INV] * r * (1.0 / MID)
        total = total + u
        r = r - apply(u, level)
        u = RHO1 * RHO0 * u + 2.0 * RHO1 / HALF * w[INV] * r
        return total + u

    def world_cycle(r, level):
        w = (glev2, glev3)[level - L]

        def apply(v):
            return world.inner(w, v, level - L)

        u = w[INV] * r * (1.0 / MID)
        total = u
        r = r - apply(u)
        u = RHO1 * RHO0 * u + 2.0 * RHO1 / HALF * w[INV] * r
        total = total + u
        r = r - apply(u)
        if level == LEVELS - 1:
            u = RHO2 * RHO1 * u + 2.0 * RHO2 / HALF * w[INV] * r
            return total + u
        e = world.prolong(world_cycle(world.restrict(r, level - L), level + 1))
        total = total + e
        r = r - apply(e)
        u = w[INV] * r * (1.0 / MID)
        total = total + u
        r = r - apply(u)
        u = RHO1 * RHO0 * u + 2.0 * RHO1 / HALF * w[INV] * r
        return total + u

    def hot(shape, wanted):
        at = lax.broadcasted_iota(jnp.int32, shape, 0)
        return jnp.where(at == wanted, 1.0, 0.0)

    def collect(v, fields, part, pl_ref, x_ref, which):
        count = fields * x_own * y_own
        picked[: fields * x_own * Y] = v
        own = picked[pl.ds(0, count, stride=1 << L), :]
        lane = lax.broadcasted_iota(jnp.int32, (Z, GZ), 1) - iz * z_own
        inside = jnp.logical_and(lane >= 0, lane < z_own)
        put = hot((Z, GZ), jnp.where(inside, lane * (1 << L), -1))
        pl_ref[part, my_plane] = dot(own, put)
        gather(pl_ref, part, planes, my_plane, in_plane, which)
        for j in range(ny):
            rows = pl_ref[part, j * nz]
            for k in range(1, nz):
                rows = rows + pl_ref[part, j * nz + k]
            for i in range(fields * x_own):
                x_ref[part, ix, i * GY + j * y_own : i * GY + (j + 1) * y_own] = rows[i * y_own : (i + 1) * y_own]
        gather(x_ref, part, nx, ix, in_column, which + 1)
        return [
            cat([x_ref[part, d, f * x_own * GY : (f + 1) * x_own * GY] for d in range(nx)]) for f in range(fields)
        ]

    def spread(v):
        lane = lax.broadcasted_iota(jnp.int32, (GZ, Z), 1)
        inside = hot((GZ, Z), iz * z_own + lane // (1 << L))
        outside = hot((GZ, Z), jnp.where(lane < Z // 2, iz * z_own - 1, iz * z_own + z_own))
        glob[0, GY : GY + nx * x_own * GY] = dot(v, inside)
        glob[1, GY : GY + nx * x_own * GY] = dot(v, outside)
        rows = rows_of(1)

        def layer(which, a):
            base = (ix * x_own + 1 + a) * GY + iy * y_own
            out = jnp.broadcast_to(glob[which, pl.ds(base, 1), :], (Y, Z))
            for j in range(1, y_own):
                row = jnp.broadcast_to(glob[which, pl.ds(base + j, 1), :], (Y, Z))
                out = jnp.where(rows < j << L, out, row)
            return out

        def rims(a):
            base = (ix * x_own + 1 + a) * GY + iy * y_own
            low = glob[0, pl.ds(base - 1, 1), :] * has_low
            high = glob[0, pl.ds(base + y_own, 1), :] * has_high
            return jnp.where(rows < Y // 2, jnp.broadcast_to(low, (Y, Z)), jnp.broadcast_to(high, (Y, Z)))

        has_low = jnp.where(iy > 0, 1.0, 0.0)
        has_high = jnp.where(iy < ny - 1, 1.0, 0.0)
        own = range(x_own)
        e = here.prolong(cat([layer(0, a) for a in own]))
        in_y = here.prolong(cat([rims(a) for a in own]))
        in_z = here.prolong(cat([layer(1, a) for a in own]))
        return e, (layer(0, -1), layer(0, x_own), in_y, in_z)

    def gather(ref, part, count, me, device, which):
        for j in range(count):
            @pl.when(me != j)
            def _():
                pltpu.make_async_remote_copy(
                    src_ref=ref.at[part, me],
                    dst_ref=ref.at[part, me],
                    send_sem=red_ssem.at[which, part],
                    recv_sem=red_rsem.at[which, part],
                    device_id=device(j),
                    device_id_type=MESH,
                ).start()
        if count > 1:
            others = ref.at[part, pl.ds(0, count - 1)]
            pltpu.make_async_copy(others, others, red_rsem.at[which, part]).wait()
            pltpu.make_async_copy(others, others, red_ssem.at[which, part]).wait()

    def in_plane(j):
        return (ix, j // nz, j % nz)

    def in_column(j):
        return (j, iy, iz)

    def in_grid(j):
        return (j // planes, j // nz % ny, j % nz)

    my_plane = iy * nz + iz
    me = ix * planes + my_plane

    def reduce_plane(ref, part, value, which):
        ref[part, my_plane] = value
        gather(ref, part, planes, my_plane, in_plane, which)
        return jnp.sum(ref[part], axis=0)

    def reduce_column(ref, part, value, which):
        ref[part, ix] = value
        gather(ref, part, nx, ix, in_column, which)
        return jnp.sum(ref[part], axis=0)

    def total_of(v):
        return jnp.sum(jnp.sum(v, axis=0, keepdims=True), axis=1, keepdims=True)

    def lane_of(row, i):
        return jnp.sum(jnp.where(lane_1 == i, row, 0.0), axis=1, keepdims=True)

    it = it_ref[...].reshape(X * Y, Z)
    reaction = rea_ref[...].reshape(X * Y, Z)
    start(it, KEPT)
    finish(KEPT)
    rows, lanes = rows_of(X), lanes_of(X)
    last_row, last_lane = rows == Y - 1, lanes == Z - 1
    n_xm = cat([rx[KEPT, 0], it[:-Y]])
    n_xp = cat([it[Y:], rx[KEPT, 1]])
    n_ym = jnp.where(rows == 0, wide_y(ry[KEPT, 0], X), roll(it, 1, 0))
    n_yp = jnp.where(last_row, wide_y(ry[KEPT, 1], X), roll(it, -1, 0))
    n_zm = jnp.where(lanes == 0, wide_z(rz[KEPT, 0], X), roll(it, 1, 1))
    n_zp = jnp.where(last_lane, wide_z(rz[KEPT, 1], X), roll(it, -1, 1))
    ws = []
    r = src_ref[...].reshape(X * Y, Z) - reaction * it
    for sign, n in ((-1, n_xm), (1, n_xp), (-1, n_ym), (1, n_yp), (-1, n_zm), (1, n_zp)):
        g = n - it
        square = g * g
        root = jnp.sqrt(1.0 + square)
        ws.append((1.0 + 2.0 * square) / root)
        r = r + g * root
    rem_ref[...] = r.reshape(X, Y, Z)
    here.put(levs[0], 0, ws, reaction)
    for level in range(L):
        ws, reaction = here.coarsen(ws, reaction, level)
        if level + 1 < L:
            here.put(levs[level + 1], level + 1, ws, reaction)
    glob[...] = jnp.zeros_like(glob)
    *ws, reaction = collect(cat(list(ws) + [reaction]), 7, 0, set_pl, set_x, 6)
    world.put(glev2, 0, ws, reaction)
    world.put(glev3, 1, *world.coarsen(ws, reaction, 0))
    for ref in (p_ref, q_ref, phx, phy, phz, dhx, dhy, dhz):
        ref[...] = jnp.zeros_like(ref)
    dir_ref[...] = jnp.zeros_like(dir_ref)

    def body(it_idx, carry):
        rz_old, pq_old = carry
        part = lax.rem(it_idx, 2)
        r = rem_ref[...].reshape(X * Y, Z)
        turn[0] = 0
        z = vcycle(r, 0, part)
        z_slot = turn[0] % ROUND
        az = apply(z, 0)
        q_old = q_ref[...]
        sums = jnp.where(
            lane_1 == 0,
            total_of(rem_ref[...].reshape(X * Y, Z) * z),
            jnp.where(lane_1 == 1, total_of(z * az), total_of(z * q_old)),
        )
        dot_all[part, me] = sums
        gather(dot_all, part, nx * planes, me, in_grid, 0)
        row = jnp.sum(dot_all[part], axis=0)
        rz_new, zaz, zq = lane_of(row, 0), lane_of(row, 1), lane_of(row, 2)
        beta = rz_new / rz_old
        pq = zaz + 2.0 * beta * zq + beta * beta * pq_old
        a = rz_new / pq
        p = z + beta * p_ref[...]
        q = az + beta * q_old
        p_ref[...] = p
        q_ref[...] = q
        dir_ref[...] = dir_ref[...] + (a * p).reshape(X, Y, Z)
        rem_ref[...] = rem_ref[...] - (a * q).reshape(X, Y, Z)
        for got, ph, dh in ((rx, phx, dhx), (ry, phy, dhy), (rz, phz, dhz)):
            for side in range(2):
                edge = got[z_slot, side] + beta * ph[side]
                ph[side] = edge
                dh[side] = dh[side] + a * edge
        return rz_new, pq

    one = jnp.ones((1, 1), jnp.float32)
    lax.fori_loop(0, ITERS, body, (one, jnp.zeros((1, 1), jnp.float32)))

    it = it_ref[...].reshape(X * Y, Z)
    step_dir = dir_ref[...].reshape(X * Y, Z)

    def energy(g):
        square = 1.0 + g * g
        return (square * jnp.sqrt(square) - 1.0) * (1.0 / 3.0)

    ends_y = jnp.where(jnp.logical_and(last_row, iy == ny - 1), 1.0, 0.0)
    ends_z = jnp.where(jnp.logical_and(last_lane, iz == nz - 1), 1.0, 0.0)
    ends_x = jnp.where(ix == nx - 1, 1.0, 0.0)
    across = lax.broadcasted_iota(jnp.int32, (X, Z), 0) == lax.broadcasted_iota(jnp.int32, (X, Z), 1)
    trial_rows = []
    for k in range(TRIALS):
        s = jnp.exp2(-jnp.full((1, Z), tp_ref[k], jnp.int32).astype(jnp.float32))
        v = it + s * step_dir
        low_x = cat([rx[KEPT, 0] + s * dhx[0], v[:-Y]])
        low_y = jnp.where(rows == 0, wide_y(ry[KEPT, 0] + s * dhy[0], X), roll(v, 1, 0))
        low_z = jnp.where(lanes == 0, wide_z(rz[KEPT, 0] + s * dhz[0], X), roll(v, 1, 1))
        at_end = energy(v)
        e = energy(v - low_x) + energy(v - low_y) + energy(v - low_z)
        e = e + at_end * (ends_y + ends_z)
        e = cat([e[:-Y], e[-Y:] + ends_x * at_end[-Y:]]) if X > 1 else e + ends_x * at_end
        e = e + 0.5 * rea_ref[...].reshape(X * Y, Z) * v * v - src_ref[...].reshape(X * Y, Z) * v
        by_layer = jnp.sum(jnp.sum(e.reshape(X, Y, Z), axis=1), axis=1, keepdims=True)
        trial_rows.append(jnp.sum(jnp.where(across, by_layer, 0.0), axis=0, keepdims=True))
    en_all[0, me] = jnp.concatenate(trial_rows, axis=0)
    gather(en_all, 0, nx * planes, me, in_grid, 2)
    layers = jnp.sum(en_all[0, pl.ds(ix * planes, planes)], axis=0)
    layers = layers / (Y * ny * Z * nz)
    le_ref[...] = layers[:, :X]
    overall = jnp.sum(en_all[0], axis=0) / (Y * ny * Z * nz)
    overall = jnp.sum(overall, axis=1, keepdims=True) / (X * nx)
    en_ref[...] = jnp.broadcast_to(overall, (TRIALS, Z))


def on_device(counts, iterate, source, reaction, trial_powers):
    X, Y, Z = iterate.shape
    nx, ny, nz = counts
    f32 = jnp.float32
    slots = ROUND + 1
    vm = pltpu.VMEM
    scratch = [vm((slots, 2, rows, Z), f32) for rows in (Y, Y, X, X, Y, Y)]
    scratch += [pltpu.SemaphoreType.DMA((slots, 6))] * 2
    x_own, y_own = X // 4, Y // 4
    GX, GY, GZ = nx * x_own, ny * y_own, nz * Z // 4
    scratch += [vm((10, (X >> level) * Y, Z), f32) for level in range(2)]
    scratch += [vm((8, (GX >> level) * GY, GZ), f32) for level in range(2)]
    scratch += [vm((X * Y, Z), f32)] * 2
    scratch += [vm((2, rows, Z), f32) for rows in (Y, X, Y)] * 2
    scratch += [
        vm((2, nx * ny * nz, 1, Z), f32),
        vm((1, nx * ny * nz, TRIALS, Z), f32),
        pltpu.SemaphoreType.DMA((8, 2)), pltpu.SemaphoreType.DMA((8, 2)),
        vm((7 * x_own * Y, Z), f32),
        vm((2, ny * nz, x_own * y_own, GZ), f32), vm((2, nx, x_own * GY, GZ), f32),
        vm((1, ny * nz, 7 * x_own * y_own, GZ), f32), vm((1, nx, 7 * x_own * GY, GZ), f32),
        vm((2, (GX + 2) * GY, Z), f32),
    ]
    whole = pl.BlockSpec(memory_space=pltpu.VMEM)
    out = pl.pallas_call(
        functools.partial(kernel, (X, Y, Z), counts),
        out_shape=[
            jax.ShapeDtypeStruct((X, Y, Z), f32),
            jax.ShapeDtypeStruct((X, Y, Z), f32),
            jax.ShapeDtypeStruct((TRIALS, X), f32),
            jax.ShapeDtypeStruct((TRIALS, Z), f32),
        ],
        in_specs=[pl.BlockSpec(memory_space=pltpu.SMEM), whole, whole, whole],
        out_specs=[whole] * 4,
        scratch_shapes=scratch,
        compiler_params=pltpu.CompilerParams(has_side_effects=True, vmem_limit_bytes=48 * 1024 * 1024),
        name="newton_step",
    )(trial_powers, iterate, source, reaction)
    return out[0], out[1], out[2], out[3][:, 0]


LANES = 128
HALO = 8
PLANES = 2
PAIR = 2
CHUNK = 4
F_DG, F_XM, F_YM, F_ZM, F_XP, F_YP, F_ZP, F_INV = range(8)
C_ONE = RHO1 * RHO0
C_TWO = 2.0 * RHO1 / HALF
C_THREE = RHO2 * RHO1
C_FOUR = 2.0 * RHO2 / HALF


def slab_fits(counts, shape):
    X, Y, Z = shape
    nx, ny, nz = counts
    per = PLANES * ny * PAIR
    rows = PAIR * Z // per
    return (
        X == 1 << (LEVELS - 1) and X * Y == LANES and nx * ny == X and nx >= PLANES and nz % PAIR == 0
        and rows * per == PAIR * Z and rows % (2 * HALO) == 0 and Z % rows == 0
    )


def slab_kernel(
    sizes, counts, tp_ref, given, fields_out, sums_out,
    turned, d_it, d_rs, f_it, f_rea, f_src, w0, w1, w2, w3,
    va, vb, vz, rr, az, sa, ra, sb, rb, s0, r0, sq, rq,
    ua, ub, r1in, rr1, sa1, ra1, sb1, rb1, s1, r1, sq1, rq1, e2, cres, cq, cnew,
    p_ref, dir_ref, q_ref, r_ref,
    msg, gath, early, egath, wmsg, wgath, hb, he, sh, enmsg, engath, outs, back,
    d_ssem, d_rsem, g_ssem, g_rsem, h_ssem, h_rsem, b_ssem, b_rsem, e_ssem,
):
    X, Y, Z = sizes
    nx, ny, nz = counts
    P = nx * ny
    GY = ny * Y
    NZ = nz * Z
    PER = PLANES * ny
    NS = PER * nz
    S = NZ // NS
    BLOCK = Z // S
    W = S + 2 * HALO
    f32 = jnp.float32
    ix, iy, iz = lax.axis_index("gx"), lax.axis_index("gy"), lax.axis_index("gz")
    me = (ix * ny + iy) * nz + iz
    own_tile = ix * ny + iy
    base = (nx - PLANES) // 2

    def fold(value, turn, size):
        return value + lax.rem(turn, 2) * (size - 1 - 2 * value)

    def device_of(s):
        c = s // PAIR
        plane = c // PER
        q = fold(lax.rem(c, PER), plane, PER)
        y = q // PLANES
        return (base + fold(lax.rem(q, PLANES), y, PLANES), y, plane * PAIR + lax.rem(s, PAIR))

    works = jnp.logical_and(ix >= base, ix < base + PLANES)
    plane = iz // PAIR
    slab = fold(iy * PLANES + fold(ix - base, iy, PLANES), plane, PER)
    slab = (plane * PER + slab) * PAIR + lax.rem(iz, PAIR)
    slab = jnp.where(works, slab, -BLOCK - 1)
    block = slab // BLOCK
    j = lax.rem(slab, BLOCK)

    has_lo, has_hi = slab > 0, slab < NS - 1
    lo_dev, hi_dev = device_of(jnp.maximum(slab - 1, 0)), device_of(jnp.clip(slab + 1, 0, NS - 1))

    def lane(n):
        return lax.broadcasted_iota(jnp.int32, (n, LANES), 1)

    def row(n):
        return lax.broadcasted_iota(jnp.int32, (n, LANES), 0)

    def low_bit(n, step):
        return lax.rem(lane(n), 2 * step) < step

    def swap(v, step):
        return jnp.where(low_bit(v.shape[0], step), roll(v, -step, 1), roll(v, step, 1))

    def pair(v, step):
        return v + swap(v, step)

    def pick_low(v, step):
        return jnp.where(low_bit(v.shape[0], step), v, roll(v, step, 1))

    def pick_high(v, step):
        return jnp.where(low_bit(v.shape[0], step), roll(v, -step, 1), v)

    def block_transpose(tiles):
        n = tiles[0].shape[0]
        k = P // 2
        while k:
            low = low_bit(n, Y * k)
            new = list(tiles)
            for i in range(P):
                if not i & k:
                    a, b = tiles[i], tiles[i | k]
                    new[i] = jnp.where(low, a, roll(b, Y * k, 1))
                    new[i | k] = jnp.where(low, roll(a, -Y * k, 1), b)
            tiles = new
            k //= 2
        return tiles

    parts = ((pl.ds(0, 1), d_it, 2 * HALO), (pl.ds(1, 2), d_rs, HALO))

    def pieces(a):
        halo = parts[a][2]
        for jd in range(BLOCK):
            first = S * jd - (halo if jd > 0 else 0)
            last = S * jd + S + (halo if jd < BLOCK - 1 else 0)
            yield BLOCK * iz + jd, None, first, last - first, 0 if jd > 0 else halo, jd
        yield BLOCK * iz + BLOCK, iz < nz - 1, Z - halo, halo, 0, BLOCK
        yield BLOCK * iz - 1, iz > 0, 0, halo, halo + S, BLOCK + 1

    def piece(a, to, first, count, there, number):
        which, landed, _ = parts[a]
        return pltpu.make_async_remote_copy(
            src_ref=turned.at[which, pl.ds(first, count)],
            dst_ref=landed.at[:, own_tile, pl.ds(there, count)],
            send_sem=d_ssem.at[a, number],
            recv_sem=d_rsem.at[a, max(number - BLOCK + 1, 0)],
            device_id=device_of(jnp.clip(to, 0, NS - 1)),
            device_id_type=MESH,
        )

    def both(a, b):
        return b if a is None else jnp.logical_and(a, b)

    barrier = pltpu.get_barrier_semaphore()
    for other in range(nx * ny * nz):
        @pl.when(me != other)
        def _():
            pl.semaphore_signal(
                barrier, inc=1, device_id=(other // (ny * nz), other // nz % ny, other % nz), device_id_type=MESH
            )

    for a, (which, landed, halo) in enumerate(parts):
        for i in (0,) if a == 0 else (1, 2):
            turned[i] = given[i * LANES : (i + 1) * LANES].T
        if a == 0:
            pl.semaphore_wait(barrier, nx * ny * nz - 1)
        for to, exists, first, count, there, number in pieces(a):
            @pl.when(both(exists, to != slab))
            def _():
                piece(a, to, first, count, there, number).start()

            @pl.when(both(exists, to == slab))
            def _():
                landed[:, own_tile, there : there + count] = turned[which, first : first + count]

    @pl.when(works)
    def _():
        for ref in (va, vb, vz, ua, ub, r1in, e2, p_ref, dir_ref, q_ref, sq, rq, sq1, rq1, cq, w1):
            ref[...] = jnp.zeros_like(ref)
        w1[F_DG] = jnp.ones(w1.shape[1:], f32)
        for side, at in ((0, 0), (1, NS - 1)):
            @pl.when(slab == at)
            def _():
                for ref in (hb, he):
                    ref[:, side] = jnp.zeros(ref.shape[:1] + ref.shape[2:], f32)

    def wait_sent():
        for a in range(2):
            for to, exists, first, count, there, number in pieces(a):
                @pl.when(both(exists, to != slab))
                def _():
                    piece(a, to, first, count, there, number).wait_send()

    def wait_landed(a, wanted, kind, first, count, source):
        mine = jnp.where(source == iz, 1, 0)
        for own in range(2):
            @pl.when(jnp.logical_and(wanted, mine == own))
            def _():
                view = parts[a][1].at[:, pl.ds(0, P - own), pl.ds(first, count)]
                pltpu.make_async_copy(view, view, d_rsem.at[a, kind]).wait()

    def gather_block(a):
        for _, landed, halo in parts[a : a + 1]:
            @pl.when(slab == 0)
            def _():
                landed[:, :, :halo] = jnp.zeros((landed.shape[0], P, halo, LANES), f32)

            @pl.when(slab == NS - 1)
            def _():
                landed[:, :, halo + S :] = jnp.zeros((landed.shape[0], P, halo, LANES), f32)

            for jd in range(BLOCK):
                count = S + (halo if jd > 0 else 0) + (halo if jd < BLOCK - 1 else 0)
                wait_landed(a, j == jd, 0, 0 if jd > 0 else halo, count, block)
            wait_landed(a, jnp.logical_and(j == 0, has_lo), 1, 0, halo, block - 1)
            wait_landed(a, jnp.logical_and(j == BLOCK - 1, has_hi), 2, halo + S, halo, block + 1)
            for i, flat in ((0, f_it),) if a == 0 else ((0, f_rea), (1, f_src)):
                for at in range(0, S + 2 * halo, HALO):
                    tiles = block_transpose([landed[i, t, at : at + HALO] for t in range(P)])
                    for t in range(P):
                        flat[t, at : at + HALO] = tiles[t]

    def back_copy(which, t):
        return pltpu.make_async_remote_copy(
            src_ref=outs.at[which, t],
            dst_ref=back.at[which, pl.ds(pl.multiple_of(S * j, HALO), S)],
            send_sem=b_ssem.at[which, t],
            recv_sem=b_rsem.at[which],
            device_id=(t // ny, t % ny, block),
            device_id_type=MESH,
        )

    def back_here(which):
        @pl.when(block == iz)
        def _():
            back[which, pl.ds(pl.multiple_of(S * j, HALO), S)] = outs[which, own_tile]

    def energy_copy(dev):
        return pltpu.make_async_remote_copy(
            src_ref=enmsg, dst_ref=engath.at[slab],
            send_sem=e_ssem.at[(dev[0] * ny + dev[1]) * nz + dev[2]], recv_sem=g_rsem.at[5],
            device_id=dev, device_id_type=MESH,
        )

    WROWS = 4 * (X // 4) * (S // (4 * CHUNK))

    @pl.when(works)
    def _():
        gather_block(0)

        lanes = lane(W)
        z_at = slab * S + row(W) - HALO
        inside = jnp.logical_and(z_at >= 0, z_at < NZ)
        z_low = jnp.logical_and(z_at > 0, z_at < NZ)
        z_high = jnp.logical_and(z_at >= 0, z_at < NZ - 1)
        x_first, x_last = lanes < GY, lanes >= LANES - GY
        y_at = lax.rem(lanes, GY)
        y_first, y_last = y_at == 0, y_at == GY - 1

        def face(g):
            square = g * g
            one = 1.0 + square
            inverse = lax.rsqrt(one)
            return (one + square) * inverse, g * (one * inverse)

        def window(t):
            return f_it[t, HALO : HALO + W]

        low_w, low_p = face(window(0) - jnp.where(x_first, 0.0, roll(window(X - 1), GY, 1)))
        for t in range(X):
            c = window(t)
            beyond = window(t + 1) if t < X - 1 else jnp.where(x_last, 0.0, roll(window(0), -GY, 1))
            high_w, high_p = face(beyond - c)
            yl_w, yl_p = face(c - jnp.where(y_first, 0.0, roll(c, 1, 1)))
            yh_w, yh_p = face(jnp.where(y_last, 0.0, roll(c, -1, 1)) - c)
            zl_w, zl_p = face(c - f_it[t, HALO - 1 : HALO - 1 + W])
            zh_w, zh_p = face(f_it[t, HALO + 1 : HALO + 1 + W] - c)
            w0[F_DG, t] = low_w + high_w + yl_w + yh_w + zl_w + zh_w
            w0[F_XM, t] = jnp.where(x_first, 0.0, low_w) if t == 0 else low_w
            w0[F_XP, t] = jnp.where(x_last, 0.0, high_w) if t == X - 1 else high_w
            w0[F_YM, t] = jnp.where(y_first, 0.0, yl_w)
            w0[F_YP, t] = jnp.where(y_last, 0.0, yh_w)
            w0[F_ZM, t] = jnp.where(z_low, zl_w, 0.0)
            w0[F_ZP, t] = jnp.where(z_high, zh_w, 0.0)
            az[t] = (high_p - low_p) + (yh_p - yl_p) + (zh_p - zl_p)
            low_w, low_p = high_w, high_p

        gather_block(1)
        for t in range(X):
            rea = f_rea[t]
            diagonal = w0[F_DG, t] + rea
            w0[F_DG, t] = diagonal
            w0[F_INV, t] = 1.0 / diagonal
            r = jnp.where(inside, f_src[t] - rea * window(t) + az[t], 0.0)
            az[t] = r
            r_ref[t] = r

        def coarsen(get, step):
            def build(k):
                def both(field, t):
                    low, high = get(field, t)
                    return low + high
                lo, hi = 2 * k, 2 * k + 1
                xm = pair(both(F_XM, lo), step)
                ym_all = both(F_YM, lo) + both(F_YM, hi)
                zl0, zh0 = get(F_ZM, lo)
                zl1, zh1 = get(F_ZM, hi)
                between = pair(both(F_XM, hi), step) + pick_high(ym_all, step) + pair(zh0 + zh1, step)
                diagonal = pair(both(F_DG, lo) + both(F_DG, hi), step) - 2.0 * between
                return diagonal, xm, pick_low(ym_all, step), pair(zl0 + zl1, step)
            return build

        n1 = W // 2
        S1 = S // 2
        W1 = S1 + 2 * HALO
        T1 = X // 2
        at1 = (W1 - n1) // 2

        def halves0(field, t):
            return w0[field, t, pl.ds(0, n1, stride=2)], w0[field, t, pl.ds(1, n1, stride=2)]

        for k in range(T1):
            for field, value in zip((F_DG, F_XM, F_YM, F_ZM), coarsen(halves0, 1)(k)):
                w1[field, k, at1 : at1 + n1] = value

        def complete1():
            for k in range(T1):
                w1[F_INV, k] = 1.0 / w1[F_DG, k]
                w1[F_XP, k] = w1[F_XM, k + 1] if k < T1 - 1 else roll(w1[F_XM, 0], -GY, 1)
                w1[F_YP, k] = roll(w1[F_YM, k], -2, 1)
                w1[F_ZP, k] = roll(w1[F_ZM, k], -1, 0)

        complete1()

        S2 = S // 4
        T2 = X // 4
        LINES = S2 // CHUNK

        def halves1(field, t):
            return w1[field, t, pl.ds(HALO, S2, stride=2)], w1[field, t, pl.ds(HALO + 1, S2, stride=2)]

        own_chunk = lax.rem(lane(S2), CHUNK) == lax.rem(row(S2), CHUNK)

        def pack(ref, first, v):
            v = jnp.where(own_chunk, v, 0.0)
            for h in range(LINES):
                ref[first + h : first + h + 1] = jnp.sum(jnp.where(row(S2) // CHUNK == h, v, 0.0), axis=0, keepdims=True)

        for k in range(T2):
            for field, value in zip((F_DG, F_XM, F_YM, F_ZM), coarsen(halves1, 2)(k)):
                pack(wmsg, (field * T2 + k) * LINES, value)

        def laps(w, vs, t, step):
            T, n = w.shape[1], w.shape[2]
            mid = slice(HALO, HALO + n)
            weights = [w[field, t] for field in range(F_INV)]
            out = []
            for v in vs:
                c = v[t, mid]
                below = v[t - 1, mid] if t > 0 else roll(v[T - 1, mid], GY, 1)
                above = v[t + 1, mid] if t < T - 1 else roll(v[0, mid], -GY, 1)
                acc = weights[F_DG] * c - weights[F_XM] * below - weights[F_XP] * above
                acc = acc - weights[F_YM] * roll(c, step, 1) - weights[F_YP] * roll(c, -step, 1)
                acc = acc - weights[F_ZM] * v[t, HALO - 1 : HALO - 1 + n]
                out.append(acc - weights[F_ZP] * v[t, HALO + 1 : HALO + 1 + n])
            return out

        def lap(w, v, t, step):
            return laps(w, [v], t, step)[0]

        def centre(v, t, n):
            return v[t, HALO : HALO + n]

        def before(w, r_of, u1, u2, rem1, s_out, r_out, step):
            T, n = w.shape[1], w.shape[2]
            mid = slice(HALO, HALO + n)
            for t in range(T):
                u1[t, mid] = w[F_INV, t] * r_of[t] * (1.0 / MID)
            for t in range(T):
                r = r_of[t] - lap(w, u1, t, step)
                first = centre(u1, t, n)
                u = C_ONE * first + C_TWO * w[F_INV, t] * r
                u2[t, mid] = u
                s_out[t] = first + u
                rem1[t] = r
            for t in range(T):
                r_out[t] = rem1[t] - lap(w, u2, t, step)

        def after(w, e, u1, rem1, s_in, r_in, put, step):
            T, n = w.shape[1], w.shape[2]
            mid = slice(HALO, HALO + n)
            for t in range(T):
                r = r_in[t] - lap(w, e, t, step)
                rem1[t] = r
                u1[t, mid] = w[F_INV, t] * r * (1.0 / MID)
            for t in range(T):
                r = rem1[t] - lap(w, u1, t, step)
                u = centre(u1, t, n)
                put(t, s_in[t] + centre(e, t, n) + u + (C_ONE * u + C_TWO * w[F_INV, t] * r))

        kept = ((az, sa, ra, sa1, ra1), (r_ref, sb, rb, sb1, rb1))

        def presmooth(f, ref, par):
            r_of, s_out, r_out, s1_out, r1_out = kept[f]
            before(w0, r_of, va, vb, rr, s_out, r_out, 1)
            for k in range(T1):
                total = None
                for t in (2 * k, 2 * k + 1):
                    part = r_out[t, pl.ds(0, n1, stride=2)] + r_out[t, pl.ds(1, n1, stride=2)]
                    total = part if total is None else total + part
                r1in[k, at1 : at1 + n1] = pair(total, 1)
            before(w1, r1in, ua, ub, rr1, s1_out, r1_out, 2)
            for k in range(T2):
                total = None
                for t in (2 * k, 2 * k + 1):
                    part = r1_out[t, pl.ds(HALO, S2, stride=2)] + r1_out[t, pl.ds(HALO + 1, S2, stride=2)]
                    total = part if total is None else total + part
                pack(ref.at[par], k * LINES, pair(total, 2))

        def to_workers(ref, out, sem):
            for s in range(NS):
                @pl.when(slab != s)
                def _():
                    pltpu.make_async_remote_copy(
                        src_ref=ref, dst_ref=out.at[slab], send_sem=g_ssem.at[sem], recv_sem=g_rsem.at[sem],
                        device_id=device_of(s), device_id_type=MESH,
                    ).start()
            out[slab] = ref[...]

        def from_workers(out, sem):
            others = out.at[pl.ds(0, NS - 1)]
            pltpu.make_async_copy(others, others, g_rsem.at[sem]).wait()
            pltpu.make_async_copy(others, others, g_ssem.at[sem]).wait()

        def unpack(out, packed):
            for k in range(T2):
                for s in range(NS):
                    out[k, s * LINES : (s + 1) * LINES] = packed[s, k * LINES : (k + 1) * LINES]

        per = 2 * (X + T1)
        halo_parts = tuple(
            ((of[3], 0, T1, S1), (of[4], T1, T1, S1), (of[1], 2 * T1, X, S), (of[2], 2 * T1 + X, X, S)) for of in kept
        )
        halo_at = (hb, he)

        def halo_send(f, par):
            for side, there, dev in ((0, has_lo, lo_dev), (1, has_hi, hi_dev)):
                @pl.when(there)
                def _():
                    for ref, first, count, size in halo_parts[f]:
                        start_row = HALO if side == 0 else size
                        pltpu.make_async_remote_copy(
                            src_ref=ref.at[:, pl.ds(start_row, HALO)],
                            dst_ref=halo_at[f].at[par, 1 - side, pl.ds(first, count)],
                            send_sem=h_ssem.at[2 * f + par, side],
                            recv_sem=h_rsem.at[2 * f + par, 1 - side],
                            device_id=dev,
                            device_id_type=MESH,
                        ).start()

        def halo_wait(view_of, sem):
            for side, there in ((0, has_lo), (1, has_hi)):
                @pl.when(there)
                def _():
                    view = view_of(side)
                    pltpu.make_async_copy(view, view, h_rsem.at[sem, side]).wait()
                    pltpu.make_async_copy(view, view, h_ssem.at[sem, side]).wait()

        chunk = lax.rem(lane(NS * LINES), CHUNK)

        def down2(v):
            return jnp.where(chunk == 0, roll(roll(v, 1 - CHUNK, 1), 1, 0), roll(v, 1, 1))

        def up2(v):
            return jnp.where(chunk == CHUNK - 1, roll(roll(v, CHUNK - 1, 1), -1, 0), roll(v, -1, 1))

        def down3(v):
            return jnp.where(chunk < CHUNK // 2, roll(roll(v, -(CHUNK // 2), 1), 1, 0), roll(v, CHUNK // 2, 1))

        def up3(v):
            return jnp.where(chunk >= CHUNK // 2, roll(roll(v, CHUNK // 2, 1), -1, 0), roll(v, -(CHUNK // 2), 1))

        def lap_all(w, vs, step, down, up):
            T = len(vs)
            out = []
            for t in range(T):
                v = vs[t]
                below = vs[t - 1] if t > 0 else roll(vs[T - 1], GY, 1)
                above = vs[t + 1] if t < T - 1 else roll(vs[0], -GY, 1)
                acc = w[F_DG, t] * v - w[F_XM, t] * below - w[F_XP, t] * above
                acc = acc - w[F_YM, t] * roll(v, step, 1) - w[F_YP, t] * roll(v, -step, 1)
                out.append(acc - w[F_ZM, t] * down(v) - w[F_ZP, t] * up(v))
            return out

        def complete_all(w, step, up):
            T = w.shape[1]
            for t in range(T):
                w[F_INV, t] = 1.0 / w[F_DG, t]
                w[F_XP, t] = w[F_XM, t + 1] if t < T - 1 else roll(w[F_XM, 0], -GY, 1)
                w[F_YP, t] = roll(w[F_YM, t], -step, 1)
                w[F_ZP, t] = up(w[F_ZM, t])

        def world():
            def apply2(v):
                return lap_all(w2, v, CHUNK, down2, up2)

            def apply3(v):
                return lap_all(w3, v, 2 * CHUNK, down3, up3)

            def scaled(w, r):
                return [w[F_INV, t] * r[t] for t in range(len(r))]

            def minus(a, b):
                return [x - y for x, y in zip(a, b)]

            def plus(*many):
                return [sum(vs[1:], vs[0]) for vs in zip(*many)]

            def first(w, r):
                return [d * (1.0 / MID) for d in scaled(w, r)]

            def follow(w, u, r, one, two):
                return [one * a + two * d for a, d in zip(u, scaled(w, r))]

            r = [cres[k] for k in range(T2)]
            u = first(w2, r)
            r = minus(r, apply2(u))
            u2 = follow(w2, u, r, C_ONE, C_TWO)
            total = plus(u, u2)
            r = minus(r, apply2(u2))
            rc = [pair(pair(r[0] + r[1], CHUNK), 1)]
            u = first(w3, rc)
            rc = minus(rc, apply3(u))
            v = follow(w3, u, rc, C_ONE, C_TWO)
            e = plus(u, v)
            rc = minus(rc, apply3(v))
            e = plus(e, follow(w3, v, rc, C_THREE, C_FOUR))
            e = [e[0]] * T2
            total = plus(total, e)
            r = minus(r, apply2(e))
            u = first(w2, r)
            r = minus(r, apply2(u))
            total = plus(total, u, follow(w2, u, r, C_ONE, C_TWO))
            for k in range(T2):
                e2[k, HALO : HALO + NS * LINES] = total[k]

        def precondition():
            world()
            own = lax.rem(lane(CHUNK), CHUNK) == row(CHUNK)
            for d in range(LINES + 2):
                for k in range(T2):
                    line = e2[k, pl.ds(slab * LINES + HALO - 1 + d, 1)]
                    v = jnp.where(own, jnp.broadcast_to(line, (CHUNK, LANES)), 0.0)
                    v = pair(pair(v, 1), 2)
                    for t in (2 * k, 2 * k + 1):
                        for half in range(2):
                            ua[t, pl.ds(HALO + 2 * CHUNK * d + half, CHUNK, stride=2)] = v

            def put1(k, v):
                for t in (2 * k, 2 * k + 1):
                    for half in range(2):
                        va[t, pl.ds(half, W1, stride=2)] = v

            after(w1, ua, ub, rr1, s1, r1, put1, 2)

            def put0(t, v):
                vz[t, HALO : HALO + W] = v

            after(w0, va, vb, rr, s0, r0, put0, 1)

        def total_of(v):
            return jnp.sum(jnp.sum(v, axis=0, keepdims=True), axis=1, keepdims=True)

        lane_1 = lane(1)

        def image_and_dots(par):
            rz = zaz = zq = None
            own = slice(HALO, HALO + S)
            for t in range(X):
                image = lap(w0, vz, t, 1)
                az[t] = image
                z = vz[t, 2 * HALO : 2 * HALO + S]
                parts = (r_ref[t, own] * z, z * image[own], z * q_ref[t, own])
                if t == 0:
                    rz, zaz, zq = parts
                else:
                    rz, zaz, zq = rz + parts[0], zaz + parts[1], zq + parts[2]
            msg[par, T2 * LINES :] = jnp.where(
                lane_1 == 0, total_of(rz), jnp.where(lane_1 == 1, total_of(zaz), total_of(zq))
            )

        def lane_of(v, i):
            return jnp.sum(jnp.where(lane_1 == i, v, 0.0), axis=1, keepdims=True)

        def scalars(par, rz_old, pq_old):
            sums = gath[par, 0, T2 * LINES :]
            for s in range(1, NS):
                sums = sums + gath[par, s, T2 * LINES :]
            rz, zaz, zq = lane_of(sums, 0), lane_of(sums, 1), lane_of(sums, 2)
            beta = rz / rz_old
            pq = zaz + 2.0 * beta * zq + beta * beta * pq_old
            return rz, pq, rz / pq, beta

        def advance(a, beta):
            for t in range(X):
                p = vz[t, HALO : HALO + HALO + S] + beta * p_ref[t]
                p_ref[t] = p
                dir_ref[t] = dir_ref[t] + a * p
                q = az[t] + beta * q_ref[t]
                q_ref[t] = q
                r_ref[t] = r_ref[t] - a * q

        def coarse_advance(par, a, beta, fresh):
            unpack(cnew, gath.at[par])
            if fresh:
                unpack(cres, egath.at[par])
            for k in range(T2):
                v = cnew[k] + beta * cq[k]
                cq[k] = v
                cres[k] = cres[k] - a * v

        def kept_advance(par, a, beta, fresh):
            for i, (keep, slope) in enumerate(((s1, sq1), (r1, rq1), (s0, sq), (r0, rq))):
                moved, first, count, size = halo_parts[0][i]
                true = halo_parts[1][i][0]
                for t in range(count):
                    for side, rows in ((0, slice(0, HALO)), (None, slice(HALO, HALO + size)), (1, slice(HALO + size, 2 * HALO + size))):
                        got = moved[t, rows] if side is None else hb[par, side, first + t]
                        if a is None:
                            keep[t, rows] = got
                            continue
                        v = got + beta * slope[t, rows]
                        slope[t, rows] = v
                        if not fresh:
                            start = keep[t, rows]
                        else:
                            start = true[t, rows] if side is None else he[par, side, first + t]
                        keep[t, rows] = start - a * v

        for s in range(NS):
            @pl.when(slab != s)
            def _():
                pltpu.make_async_remote_copy(
                    src_ref=wmsg, dst_ref=wgath.at[pl.ds(pl.multiple_of(slab * WROWS, HALO), WROWS)],
                    send_sem=g_ssem.at[4], recv_sem=g_rsem.at[4], device_id=device_of(s), device_id_type=MESH,
                ).start()
        wgath[pl.ds(pl.multiple_of(slab * WROWS, HALO), WROWS)] = wmsg[...]
        for side, there, dev in ((0, has_lo, lo_dev), (1, has_hi, hi_dev)):
            @pl.when(there)
            def _():
                pltpu.make_async_remote_copy(
                    src_ref=w1.at[pl.ds(0, 4), :, pl.ds(HALO if side == 0 else S1, HALO)], dst_ref=sh.at[1 - side],
                    send_sem=h_ssem.at[4, side], recv_sem=h_rsem.at[4, 1 - side],
                    device_id=dev, device_id_type=MESH,
                ).start()
        presmooth(0, msg, 0)
        msg[0, T2 * LINES :] = jnp.zeros((1, LANES), f32)
        to_workers(msg.at[0], gath.at[0], 0)
        halo_send(0, 0)
        wait_sent()

        others = wgath.at[pl.ds(0, (NS - 1) * WROWS)]
        pltpu.make_async_copy(others, others, g_rsem.at[4]).wait()
        pltpu.make_async_copy(others, others, g_ssem.at[4]).wait()
        for field in range(4):
            for k in range(T2):
                for h in range(LINES):
                    line = (field * T2 + k) * LINES + h
                    w2[field, k, pl.ds(h, NS, stride=LINES)] = wgath[pl.ds(line, NS, stride=WROWS)]
        complete_all(w2, CHUNK, up2)
        dg, xm, ym, zm = F_DG, F_XM, F_YM, F_ZM
        ym_all = pair(w2[ym, 0] + w2[ym, 1], 1)
        zm_all = pair(w2[zm, 0] + w2[zm, 1], CHUNK)
        between = pair(pair(w2[xm, 1], CHUNK), 1) + pick_high(ym_all, CHUNK) + pick_high(zm_all, 1)
        w3[dg, 0] = pair(pair(w2[dg, 0] + w2[dg, 1], CHUNK), 1) - 2.0 * between
        w3[xm, 0] = pair(pair(w2[xm, 0], CHUNK), 1)
        w3[ym, 0] = pick_low(ym_all, CHUNK)
        w3[zm, 0] = pick_low(zm_all, 1)
        complete_all(w3, 2 * CHUNK, up3)
        halo_wait(lambda side: sh.at[side], 4)
        for side, there in ((0, has_lo), (1, has_hi)):
            @pl.when(there)
            def _():
                first = 0 if side == 0 else HALO + S1
                for field in range(4):
                    w1[field, :, first : first + HALO] = sh[side, field]
        complete1()
        from_workers(gath.at[0], 0)
        unpack(cres, gath.at[0])
        halo_wait(lambda side: hb.at[0, side], 0)
        kept_advance(0, None, None, False)

        def step(par, fresh, carry):
            if fresh:
                presmooth(1, early, par)
                to_workers(early.at[par], egath.at[par], 2 + par)
                halo_send(1, par)
            precondition()
            image_and_dots(par)
            presmooth(0, msg, par)
            to_workers(msg.at[par], gath.at[par], par)
            halo_send(0, par)
            from_workers(gath.at[par], par)
            rz, pq, a, beta = scalars(par, *carry)
            if fresh:
                from_workers(egath.at[par], 2 + par)
            coarse_advance(par, a, beta, fresh)
            advance(a, beta)
            halo_wait(lambda side: hb.at[par, side], par)
            if fresh:
                halo_wait(lambda side: he.at[par, side], 2 + par)
            kept_advance(par, a, beta, fresh)
            return rz, pq

        carry = step(1, False, (jnp.ones((1, 1), f32), jnp.zeros((1, 1), f32)))
        carry = lax.fori_loop(1, ITERS - 1, lambda i, c: step(lax.rem(i + 1, 2), True, c), carry)
        last = ITERS % 2
        precondition()
        image_and_dots(last)
        to_workers(msg.at[last], gath.at[last], last)
        from_workers(gath.at[last], last)
        _, _, a, beta = scalars(last, *carry)
        advance(a, beta)

        for which in range(2):
            for at in range(0, S, HALO):
                ref = r_ref if which else dir_ref
                tiles = block_transpose([ref[t, HALO + at : 2 * HALO + at] for t in range(X)])
                for t in range(X):
                    outs[which, t, at : at + HALO] = tiles[t]
            for t in range(P):
                remote = jnp.logical_or(block != iz, own_tile != t)

                @pl.when(remote)
                def _():
                    back_copy(which, t).start()
            back_here(which)

        def energy(g):
            square = 1.0 + g * g
            return (square * (square * lax.rsqrt(square)) - 1.0) * (1.0 / 3.0)

        lanes = lane(S)
        y_at = lax.rem(lanes, GY)
        x_first, x_last, y_first = lanes < GY, lanes >= LANES - GY, y_at == 0
        ends = jnp.where(y_at == GY - 1, 1.0, 0.0) + jnp.where(slab * S + row(S) == NZ - 1, 1.0, 0.0)
        ends_x = ends + jnp.where(x_last, 1.0, 0.0)
        fetch = lax.rem(lane_1, GY)
        packed = jnp.zeros((1, LANES), f32)
        for k in range(TRIALS):
            s = jnp.exp2(-jnp.full((1, LANES), tp_ref[k], jnp.int32).astype(f32))

            def trial(t, shift):
                first = 2 * HALO - shift
                return f_it[t, first : first + S] + s * dir_ref[t, HALO - shift : HALO - shift + S]

            below = jnp.where(x_first, 0.0, roll(trial(X - 1, 0), GY, 1))
            for t in range(X):
                v = trial(t, 0)
                e = energy(v - below) + energy(v - trial(t, 1))
                e = e + energy(v - jnp.where(y_first, 0.0, roll(v, 1, 1)))
                e = e + energy(v) * (ends_x if t == X - 1 else ends)
                e = e + (0.5 * f_rea[t, HALO : HALO + S] * v - f_src[t, HALO : HALO + S]) * v
                column = jnp.sum(e, axis=0, keepdims=True)
                step = 1
                while step < GY:
                    column = pair(column, step)
                    step *= 2
                packed = packed + jnp.where(fetch == k * X + t, column, 0.0)
                below = v
        enmsg[...] = packed
        engath[slab] = packed
        for other in range(nx * ny * nz):
            @pl.when(me != other)
            def _():
                energy_copy((other // (ny * nz), other // nz % ny, other % nz)).start()
        for which in range(2):
            for t in range(P):
                @pl.when(jnp.logical_or(block != iz, own_tile != t))
                def _():
                    back_copy(which, t).wait_send()

    @pl.when(jnp.logical_not(works))
    def _():
        wait_sent()

    for which in range(2):
        for own in range(2):
            @pl.when(jnp.where(block == iz, 1, 0) == own)
            def _():
                view = back.at[which, pl.ds(0, Z - own * S)]
                pltpu.make_async_copy(view, view, b_rsem.at[which]).wait()
        fields_out[which] = back[which].T.reshape(X, Y, Z)
    @pl.when(works)
    def _():
        others = engath.at[pl.ds(0, NS - 1)]
        pltpu.make_async_copy(others, others, g_rsem.at[5]).wait()
        for other in range(nx * ny * nz):
            @pl.when(me != other)
            def _():
                energy_copy((other // (ny * nz), other // nz % ny, other % nz)).wait_send()

    @pl.when(jnp.logical_not(works))
    def _():
        pltpu.make_async_copy(engath, engath, g_rsem.at[5]).wait()

    lane_1 = lane(1)
    fetch = lax.rem(lane_1, GY)
    layers = jnp.sum(engath[...], axis=0) / (GY * NZ)
    here = jnp.where(lane_1 // GY == ix, layers, 0.0)
    at_k = lax.broadcasted_iota(jnp.int32, (TRIALS * X, LANES), 0)
    mine = jnp.sum(jnp.where(lax.rem(lane(TRIALS * X), GY) == at_k, here, 0.0), axis=1, keepdims=True)
    mine = jnp.where(lane(TRIALS * X) == lax.rem(at_k, X), mine, 0.0)
    for k in range(TRIALS):
        sums_out[k : k + 1] = jnp.sum(mine[k * X : k * X + X], axis=0, keepdims=True)
        total = jnp.sum(jnp.where(fetch // X == k, layers, 0.0), axis=1, keepdims=True) / (X * nx)
        sums_out[TRIALS + k : TRIALS + k + 1] = jnp.broadcast_to(total, (1, LANES))


def hand_out(fields, sums, dir_out, rem_out, le_out, en_out, le, en, sem):
    copies = [pltpu.make_async_copy(fields.at[i], out, sem.at[i]) for i, out in ((0, dir_out), (1, rem_out))]
    for copy in copies:
        copy.start()
    le[...] = sums[:TRIALS, : le.shape[1]]
    for k in range(TRIALS):
        en[k] = jnp.max(sums[TRIALS + k : TRIALS + k + 1])
    copies += [pltpu.make_async_copy(le, le_out, sem.at[2]), pltpu.make_async_copy(en, en_out, sem.at[3])]
    for copy in copies[2:]:
        copy.start()
    for copy in copies:
        copy.wait()


def slab_on_device(counts, iterate, source, reaction, trial_powers):
    X, Y, Z = iterate.shape
    nx, ny, nz = counts
    P = nx * ny
    NS = PLANES * ny * nz
    S = nz * Z // NS
    BLOCK = Z // S
    W, W1 = S + 2 * HALO, S // 2 + 2 * HALO
    T1, T2, T3 = X // 2, X // 4, X // 8
    LINES = S // (4 * CHUNK)
    C_ROWS, ROWS = T2 * LINES, NS * LINES
    f32 = jnp.float32

    def vm(*shape):
        return pltpu.VMEM(shape, f32)

    def sem(*shape):
        return pltpu.SemaphoreType.DMA(shape)

    full, padded = (X, W, LANES), (X, W + 2 * HALO, LANES)
    full1, padded1 = (T1, W1, LANES), (T1, W1 + 2 * HALO, LANES)
    scratch = [vm(3, Z, LANES), vm(1, P, W + 2 * HALO, LANES), vm(2, P, W, LANES)]
    scratch += [vm(*padded), vm(*full), vm(*full)]
    scratch += [vm(8, *full), vm(8, *full1), vm(8, T2, ROWS, LANES), vm(8, T3, ROWS, LANES)]
    scratch += [vm(*padded)] * 3 + [vm(*full)] * 10
    scratch += [vm(*padded1)] * 2 + [vm(*full1)] * 10
    scratch += [vm(T2, ROWS + 2 * HALO, LANES)] + [vm(T2, ROWS, LANES)] * 3
    scratch += [vm(X, S + HALO, LANES)] * 2 + [vm(*full)] * 2
    scratch += [vm(2, C_ROWS + 1, LANES), vm(2, NS, C_ROWS + 1, LANES), vm(2, C_ROWS, LANES), vm(2, NS, C_ROWS, LANES)]
    scratch += [vm(4 * C_ROWS, LANES), vm(NS * 4 * C_ROWS, LANES)]
    scratch += [vm(2, 2, 2 * (X + T1), HALO, LANES)] * 2 + [vm(2, 4, T1, HALO, LANES)]
    scratch += [vm(1, LANES), vm(NS, 1, LANES), vm(2, P, S, LANES), vm(2, Z, LANES)]
    scratch += [sem(2, BLOCK + 2), sem(2, 3), sem(6), sem(6), sem(5, 2), sem(5, 2), sem(2, P), sem(2), sem(nx * ny * nz)]
    whole = pl.BlockSpec(memory_space=pltpu.VMEM)
    given = jnp.concatenate([v.reshape(LANES, Z) for v in (iterate, reaction, source)])
    fields, sums = pl.pallas_call(
        functools.partial(slab_kernel, (X, Y, Z), counts),
        out_shape=[jax.ShapeDtypeStruct((2, X, Y, Z), f32), jax.ShapeDtypeStruct((2 * TRIALS, LANES), f32)],
        in_specs=[pl.BlockSpec(memory_space=pltpu.SMEM), whole],
        out_specs=[whole] * 2,
        scratch_shapes=scratch,
        compiler_params=pltpu.CompilerParams(
            has_side_effects=True, collective_id=0, vmem_limit_bytes=32 * 1024 * 1024
        ),
        name="newton_step",
    )(trial_powers, given)
    return pl.pallas_call(
        hand_out,
        out_shape=[
            jax.ShapeDtypeStruct((X, Y, Z), f32),
            jax.ShapeDtypeStruct((X, Y, Z), f32),
            jax.ShapeDtypeStruct((TRIALS, X), f32),
            jax.ShapeDtypeStruct((TRIALS,), f32),
        ],
        in_specs=[whole] * 2,
        out_specs=[pl.BlockSpec(memory_space=pl.ANY)] * 4,
        scratch_shapes=[vm(TRIALS, X), pltpu.SMEM((TRIALS,), f32), sem(4)],
        compiler_params=pltpu.CompilerParams(vmem_limit_bytes=32 * 1024 * 1024),
        name="hand_out",
    )(fields, sums)


def solution(mesh):
    counts = tuple(mesh.shape[axis] for axis in ("gx", "gy", "gz"))
    grid = P("gx", "gy", "gz")

    def on_each(iterate, source, reaction, trial_powers):
        form = slab_on_device if slab_fits(counts, iterate.shape) else on_device
        return form(counts, iterate, source, reaction, trial_powers)

    return jax.shard_map(
        on_each,
        mesh=mesh,
        in_specs=(grid, grid, grid, P()),
        out_specs=(grid, grid, P(None, "gx"), P()),
        check_vma=False,
    )
```

```python
import functools

import jax
import jax.numpy as jnp
from jax import lax
from jax.experimental import pallas as pl
from jax.experimental.pallas import tpu as pltpu
from jax.sharding import PartitionSpec as P

ITERS = 4
LEVELS = 4
TRIALS = 4
MID = 1.15
HALF = 0.85
SIGMA = MID / HALF
RHO0 = 1.0 / SIGMA
RHO1 = 1.0 / (2.0 * SIGMA - RHO0)
RHO2 = 1.0 / (2.0 * SIGMA - RHO1)
ROUND = 3
KEPT = ROUND
DG, INV, XM, XP, YM, YP, ZM, ZP, YB, ZB = range(10)
MESH = pl.DeviceIdType.MESH


class Grid:
    def __init__(self, Y, Z):
        self.Y, self.Z = Y, Z

    def rows_of(self, x):
        return lax.rem(lax.broadcasted_iota(jnp.int32, (x * self.Y, self.Z), 0), self.Y)

    def lanes_of(self, x):
        return lax.broadcasted_iota(jnp.int32, (x * self.Y, self.Z), 1)

    def pair_x(self, v):
        Y = self.Y
        x = v.shape[0] // Y
        return cat([v[2 * i * Y : (2 * i + 1) * Y] + v[(2 * i + 1) * Y : (2 * i + 2) * Y] for i in range(x // 2)])

    def pick_x(self, v, odd):
        Y = self.Y
        x = v.shape[0] // Y
        return cat([v[(2 * i + odd) * Y : (2 * i + odd + 1) * Y] for i in range(x // 2)])

    def bit(self, v, level, axis):
        at = self.rows_of(v.shape[0] // self.Y) if axis == 0 else self.lanes_of(v.shape[0] // self.Y)
        return lax.rem(at, 2 << level) < (1 << level)

    def pair(self, v, level, axis):
        step = 1 << level
        return v + jnp.where(self.bit(v, level, axis), roll(v, -step, axis), roll(v, step, axis))

    def pick(self, v, level, axis, odd):
        step = 1 << level
        low = self.bit(v, level, axis)
        if odd:
            return jnp.where(low, roll(v, -step, axis), v)
        return jnp.where(low, v, roll(v, step, axis))

    def restrict(self, v, level):
        return self.pair(self.pair(self.pair_x(v), level, 0), level, 1)

    def prolong(self, v):
        Y = self.Y
        x = v.shape[0] // Y
        return cat([v[(i // 2) * Y : (i // 2 + 1) * Y] for i in range(2 * x)])

    def coarsen(self, ws, reaction, level):
        xm, xp, ym, yp, zm, zp = ws
        pair, pick = self.pair, self.pick
        ws = (
            pair(pair(self.pick_x(xm, 0), level, 0), level, 1),
            pair(pair(self.pick_x(xp, 1), level, 0), level, 1),
            pair(pick(self.pair_x(ym), level, 0, 0), level, 1),
            pair(pick(self.pair_x(yp), level, 0, 1), level, 1),
            pick(pair(self.pair_x(zm), level, 0), level, 1, 0),
            pick(pair(self.pair_x(zp), level, 0), level, 1, 1),
        )
        return ws, self.restrict(reaction, level)

    def put(self, w, level, ws, reaction):
        Y, Z = self.Y, self.Z
        xm, xp, ym, yp, zm, zp = ws
        step = 1 << level
        x = xm.shape[0] // Y
        rows, lanes = self.rows_of(x), self.lanes_of(x)
        diagonal = reaction + xm + xp + ym + yp + zm + zp
        zero = jnp.zeros_like(xm)
        w[DG] = diagonal
        w[INV] = 1.0 / diagonal
        w[XM] = xm
        w[XP] = xp
        w[YM] = jnp.where(rows < step, zero, ym)
        w[YP] = jnp.where(rows >= Y - step, zero, yp)
        w[ZM] = jnp.where(lanes < step, zero, zm)
        w[ZP] = jnp.where(lanes >= Z - step, zero, zp)
        if w.shape[0] > YB:
            w[YB] = jnp.where(rows < step, ym, jnp.where(rows >= Y - step, yp, zero))
            w[ZB] = jnp.where(lanes < step, zm, jnp.where(lanes >= Z - step, zp, zero))

    def inner(self, w, v, level):
        step = 1 << level
        acc = w[DG] * v
        acc = acc - w[YM] * roll(v, step, 0) - w[YP] * roll(v, -step, 0)
        acc = acc - w[ZM] * roll(v, step, 1) - w[ZP] * roll(v, -step, 1)
        Y = self.Y
        if v.shape[0] > Y:
            none = jnp.zeros((Y, self.Z), jnp.float32)
            acc = acc - w[XM] * cat([none, v[:-Y]]) - w[XP] * cat([v[Y:], none])
        return acc


def cat(parts):
    return parts[0] if len(parts) == 1 else jnp.concatenate(parts, axis=0)


def roll(v, shift, axis):
    return pltpu.roll(v, shift % v.shape[axis], axis)


def dot(a, b):
    return lax.dot_general(
        a, b, (((1,), (0,)), ((), ())), precision=lax.Precision.HIGHEST, preferred_element_type=jnp.float32
    )


def kernel(
    sizes, counts, tp_ref, it_ref, src_ref, rea_ref, dir_ref, rem_ref, le_ref, en_ref,
    sx, rx, sy, ry, sz, rz, ssem, rsem, lev0, lev1, glev2, glev3, p_ref, q_ref,
    phx, phy, phz, dhx, dhy, dhz, dot_all, en_all, red_ssem, red_rsem,
    picked, gat_pl, gat_x, set_pl, set_x, glob,
):
    X, Y, Z = sizes
    nx, ny, nz = counts
    planes = ny * nz
    levs = (lev0, lev1)
    L = len(levs)
    x_own, y_own, z_own = X >> L, Y >> L, Z >> L
    GY, GZ = ny * y_own, nz * z_own
    here, world = Grid(Y, Z), Grid(GY, GZ)
    rows_of, lanes_of = here.rows_of, here.lanes_of
    ix, iy, iz = lax.axis_index("gx"), lax.axis_index("gy"), lax.axis_index("gz")
    has = (ix > 0, ix < nx - 1, iy > 0, iy < ny - 1, iz > 0, iz < nz - 1)
    devs = (
        (ix - 1, iy, iz), (ix + 1, iy, iz), (ix, iy - 1, iz),
        (ix, iy + 1, iz), (ix, iy, iz - 1), (ix, iy, iz + 1),
    )
    send = (sx, sx, sy, sy, sz, sz)
    recv = (rx, rx, ry, ry, rz, rz)
    lane_y = lax.broadcasted_iota(jnp.int32, (Y, Z), 1)
    lane_1 = lax.broadcasted_iota(jnp.int32, (1, Z), 1)

    for d in range(6):
        @pl.when(jnp.logical_not(has[d]))
        def _():
            recv[d][:, d % 2] = jnp.zeros(recv[d].shape[:1] + recv[d].shape[2:], jnp.float32)

    def outgoing(d, slot):
        side = d % 2
        return pltpu.make_async_remote_copy(
            src_ref=send[d].at[slot, side],
            dst_ref=recv[d].at[slot, 1 - side],
            send_sem=ssem.at[slot, d],
            recv_sem=rsem.at[slot, d + 1 - 2 * side],
            device_id=devs[d],
            device_id_type=MESH,
        )

    def incoming(d, slot):
        side = d % 2
        return pltpu.make_async_remote_copy(
            src_ref=send[d].at[slot, side],
            dst_ref=recv[d].at[slot, side],
            send_sem=ssem.at[slot, d],
            recv_sem=rsem.at[slot, d],
            device_id=devs[d],
            device_id_type=MESH,
        )

    def go(d, slot):
        @pl.when(has[d])
        def _():
            outgoing(d, slot).start()

    def start(v, slot):
        x = v.shape[0] // Y
        sx[slot, 0] = v[:Y]
        sx[slot, 1] = v[-Y:]
        go(0, slot)
        go(1, slot)
        for i in range(x):
            sy[slot, 0, i : i + 1] = v[i * Y : i * Y + 1]
            sy[slot, 1, i : i + 1] = v[i * Y + Y - 1 : i * Y + Y]
        go(2, slot)
        go(3, slot)
        for side, lane in ((0, 0), (1, Z - 1)):
            packed = jnp.broadcast_to(v[:Y, lane : lane + 1], (Y, Z))
            for i in range(1, x):
                part = jnp.broadcast_to(v[i * Y : i * Y + Y, lane : lane + 1], (Y, Z))
                packed = jnp.where(lane_y == i, part, packed)
            sz[slot, side] = packed
        go(4, slot)
        go(5, slot)

    def finish(slot):
        for d in range(6):
            @pl.when(has[d])
            def _():
                copy = incoming(d, slot)
                copy.wait_recv()
                copy.wait_send()

    def wide_y(half, x):
        return cat([jnp.broadcast_to(half[i : i + 1], (Y, Z)) for i in range(x)])

    def wide_z(half, x):
        return cat([jnp.broadcast_to(half[:, i : i + 1], (Y, Z)) for i in range(x)])

    def beyond(w, acc, in_x0, in_x1, in_y, in_z):
        x = acc.shape[0] // Y
        acc = acc - w[YB] * in_y - w[ZB] * in_z
        low = w[XM, :Y] * in_x0
        high = w[XP, (x - 1) * Y :] * in_x1
        if x == 1:
            return acc - low - high
        return cat([acc[:Y] - low] + ([acc[Y:-Y]] if x > 2 else []) + [acc[-Y:] - high])

    def operate(v, level, slot):
        w = levs[level]
        x = X >> level
        start(v, slot)
        acc = here.inner(w, v, level)
        finish(slot)
        in_y = jnp.where(rows_of(x) < Y // 2, wide_y(ry[slot, 0], x), wide_y(ry[slot, 1], x))
        in_z = jnp.where(lanes_of(x) < Z // 2, wide_z(rz[slot, 0], x), wide_z(rz[slot, 1], x))
        return beyond(w, acc, rx[slot, 0], rx[slot, 1], in_y, in_z)

    turn = [0]

    def apply(v, level):
        slot = turn[0] % ROUND
        turn[0] += 1
        return operate(v, level, slot)

    def vcycle(r, level, part):
        w = levs[level]
        u = w[INV] * r * (1.0 / MID)
        total = u
        r = r - apply(u, level)
        u = RHO1 * RHO0 * u + 2.0 * RHO1 / HALF * w[INV] * r
        total = total + u
        r = r - apply(u, level)
        coarse = here.restrict(r, level)
        if level + 1 < L:
            e = here.prolong(vcycle(coarse, level + 1, part))
            r = r - apply(e, level)
        else:
            everywhere = collect(coarse, 1, part, gat_pl, gat_x, 4)
            e, ends = spread(world_cycle(everywhere[0], level + 1))
            r = r - beyond(w, here.inner(w, e, level), *ends)
        total = total + e
        u = w[INV] * r * (1.0 / MID)
        total = total + u
        r = r - apply(u, level)
        u = RHO1 * RHO0 * u + 2.0 * RHO1 / HALF * w[INV] * r
        return total + u

    def world_cycle(r, level):
        w = (glev2, glev3)[level - L]

        def apply(v):
            return world.inner(w, v, level - L)

        u = w[INV] * r * (1.0 / MID)
        total = u
        r = r - apply(u)
        u = RHO1 * RHO0 * u + 2.0 * RHO1 / HALF * w[INV] * r
        total = total + u
        r = r - apply(u)
        if level == LEVELS - 1:
            u = RHO2 * RHO1 * u + 2.0 * RHO2 / HALF * w[INV] * r
            return total + u
        e = world.prolong(world_cycle(world.restrict(r, level - L), level + 1))
        total = total + e
        r = r - apply(e)
        u = w[INV] * r * (1.0 / MID)
        total = total + u
        r = r - apply(u)
        u = RHO1 * RHO0 * u + 2.0 * RHO1 / HALF * w[INV] * r
        return total + u

    def hot(shape, wanted):
        at = lax.broadcasted_iota(jnp.int32, shape, 0)
        return jnp.where(at == wanted, 1.0, 0.0)

    def collect(v, fields, part, pl_ref, x_ref, which):
        count = fields * x_own * y_own
        picked[: fields * x_own * Y] = v
        own = picked[pl.ds(0, count, stride=1 << L), :]
        lane = lax.broadcasted_iota(jnp.int32, (Z, GZ), 1) - iz * z_own
        inside = jnp.logical_and(lane >= 0, lane < z_own)
        put = hot((Z, GZ), jnp.where(inside, lane * (1 << L), -1))
        pl_ref[part, my_plane] = dot(own, put)
        gather(pl_ref, part, planes, my_plane, in_plane, which)
        for j in range(ny):
            rows = pl_ref[part, j * nz]
            for k in range(1, nz):
                rows = rows + pl_ref[part, j * nz + k]
            for i in range(fields * x_own):
                x_ref[part, ix, i * GY + j * y_own : i * GY + (j + 1) * y_own] = rows[i * y_own : (i + 1) * y_own]
        gather(x_ref, part, nx, ix, in_column, which + 1)
        return [
            cat([x_ref[part, d, f * x_own * GY : (f + 1) * x_own * GY] for d in range(nx)]) for f in range(fields)
        ]

    def spread(v):
        lane = lax.broadcasted_iota(jnp.int32, (GZ, Z), 1)
        inside = hot((GZ, Z), iz * z_own + lane // (1 << L))
        outside = hot((GZ, Z), jnp.where(lane < Z // 2, iz * z_own - 1, iz * z_own + z_own))
        glob[0, GY : GY + nx * x_own * GY] = dot(v, inside)
        glob[1, GY : GY + nx * x_own * GY] = dot(v, outside)
        rows = rows_of(1)

        def layer(which, a):
            base = (ix * x_own + 1 + a) * GY + iy * y_own
            out = jnp.broadcast_to(glob[which, pl.ds(base, 1), :], (Y, Z))
            for j in range(1, y_own):
                row = jnp.broadcast_to(glob[which, pl.ds(base + j, 1), :], (Y, Z))
                out = jnp.where(rows < j << L, out, row)
            return out

        def rims(a):
            base = (ix * x_own + 1 + a) * GY + iy * y_own
            low = glob[0, pl.ds(base - 1, 1), :] * has_low
            high = glob[0, pl.ds(base + y_own, 1), :] * has_high
            return jnp.where(rows < Y // 2, jnp.broadcast_to(low, (Y, Z)), jnp.broadcast_to(high, (Y, Z)))

        has_low = jnp.where(iy > 0, 1.0, 0.0)
        has_high = jnp.where(iy < ny - 1, 1.0, 0.0)
        own = range(x_own)
        e = here.prolong(cat([layer(0, a) for a in own]))
        in_y = here.prolong(cat([rims(a) for a in own]))
        in_z = here.prolong(cat([layer(1, a) for a in own]))
        return e, (layer(0, -1), layer(0, x_own), in_y, in_z)

    def gather(ref, part, count, me, device, which):
        for j in range(count):
            @pl.when(me != j)
            def _():
                pltpu.make_async_remote_copy(
                    src_ref=ref.at[part, me],
                    dst_ref=ref.at[part, me],
                    send_sem=red_ssem.at[which, part],
                    recv_sem=red_rsem.at[which, part],
                    device_id=device(j),
                    device_id_type=MESH,
                ).start()
        if count > 1:
            others = ref.at[part, pl.ds(0, count - 1)]
            pltpu.make_async_copy(others, others, red_rsem.at[which, part]).wait()
            pltpu.make_async_copy(others, others, red_ssem.at[which, part]).wait()

    def in_plane(j):
        return (ix, j // nz, j % nz)

    def in_column(j):
        return (j, iy, iz)

    def in_grid(j):
        return (j // planes, j // nz % ny, j % nz)

    my_plane = iy * nz + iz
    me = ix * planes + my_plane

    def reduce_plane(ref, part, value, which):
        ref[part, my_plane] = value
        gather(ref, part, planes, my_plane, in_plane, which)
        return jnp.sum(ref[part], axis=0)

    def reduce_column(ref, part, value, which):
        ref[part, ix] = value
        gather(ref, part, nx, ix, in_column, which)
        return jnp.sum(ref[part], axis=0)

    def total_of(v):
        return jnp.sum(jnp.sum(v, axis=0, keepdims=True), axis=1, keepdims=True)

    def lane_of(row, i):
        return jnp.sum(jnp.where(lane_1 == i, row, 0.0), axis=1, keepdims=True)

    it = it_ref[...].reshape(X * Y, Z)
    reaction = rea_ref[...].reshape(X * Y, Z)
    start(it, KEPT)
    finish(KEPT)
    rows, lanes = rows_of(X), lanes_of(X)
    last_row, last_lane = rows == Y - 1, lanes == Z - 1
    n_xm = cat([rx[KEPT, 0], it[:-Y]])
    n_xp = cat([it[Y:], rx[KEPT, 1]])
    n_ym = jnp.where(rows == 0, wide_y(ry[KEPT, 0], X), roll(it, 1, 0))
    n_yp = jnp.where(last_row, wide_y(ry[KEPT, 1], X), roll(it, -1, 0))
    n_zm = jnp.where(lanes == 0, wide_z(rz[KEPT, 0], X), roll(it, 1, 1))
    n_zp = jnp.where(last_lane, wide_z(rz[KEPT, 1], X), roll(it, -1, 1))
    ws = []
    r = src_ref[...].reshape(X * Y, Z) - reaction * it
    for sign, n in ((-1, n_xm), (1, n_xp), (-1, n_ym), (1, n_yp), (-1, n_zm), (1, n_zp)):
        g = n - it
        square = g * g
        root = jnp.sqrt(1.0 + square)
        ws.append((1.0 + 2.0 * square) / root)
        r = r + g * root
    rem_ref[...] = r.reshape(X, Y, Z)
    here.put(levs[0], 0, ws, reaction)
    for level in range(L):
        ws, reaction = here.coarsen(ws, reaction, level)
        if level + 1 < L:
            here.put(levs[level + 1], level + 1, ws, reaction)
    glob[...] = jnp.zeros_like(glob)
    *ws, reaction = collect(cat(list(ws) + [reaction]), 7, 0, set_pl, set_x, 6)
    world.put(glev2, 0, ws, reaction)
    world.put(glev3, 1, *world.coarsen(ws, reaction, 0))
    for ref in (p_ref, q_ref, phx, phy, phz, dhx, dhy, dhz):
        ref[...] = jnp.zeros_like(ref)
    dir_ref[...] = jnp.zeros_like(dir_ref)

    def body(it_idx, carry):
        rz_old, pq_old = carry
        part = lax.rem(it_idx, 2)
        r = rem_ref[...].reshape(X * Y, Z)
        turn[0] = 0
        z = vcycle(r, 0, part)
        z_slot = turn[0] % ROUND
        az = apply(z, 0)
        q_old = q_ref[...]
        sums = jnp.where(
            lane_1 == 0,
            total_of(rem_ref[...].reshape(X * Y, Z) * z),
            jnp.where(lane_1 == 1, total_of(z * az), total_of(z * q_old)),
        )
        dot_all[part, me] = sums
        gather(dot_all, part, nx * planes, me, in_grid, 0)
        row = jnp.sum(dot_all[part], axis=0)
        rz_new, zaz, zq = lane_of(row, 0), lane_of(row, 1), lane_of(row, 2)
        beta = rz_new / rz_old
        pq = zaz + 2.0 * beta * zq + beta * beta * pq_old
        a = rz_new / pq
        p = z + beta * p_ref[...]
        q = az + beta * q_old
        p_ref[...] = p
        q_ref[...] = q
        dir_ref[...] = dir_ref[...] + (a * p).reshape(X, Y, Z)
        rem_ref[...] = rem_ref[...] - (a * q).reshape(X, Y, Z)
        for got, ph, dh in ((rx, phx, dhx), (ry, phy, dhy), (rz, phz, dhz)):
            for side in range(2):
                edge = got[z_slot, side] + beta * ph[side]
                ph[side] = edge
                dh[side] = dh[side] + a * edge
        return rz_new, pq

    one = jnp.ones((1, 1), jnp.float32)
    lax.fori_loop(0, ITERS, body, (one, jnp.zeros((1, 1), jnp.float32)))

    it = it_ref[...].reshape(X * Y, Z)
    step_dir = dir_ref[...].reshape(X * Y, Z)

    def energy(g):
        square = 1.0 + g * g
        return (square * jnp.sqrt(square) - 1.0) * (1.0 / 3.0)

    ends_y = jnp.where(jnp.logical_and(last_row, iy == ny - 1), 1.0, 0.0)
    ends_z = jnp.where(jnp.logical_and(last_lane, iz == nz - 1), 1.0, 0.0)
    ends_x = jnp.where(ix == nx - 1, 1.0, 0.0)
    across = lax.broadcasted_iota(jnp.int32, (X, Z), 0) == lax.broadcasted_iota(jnp.int32, (X, Z), 1)
    trial_rows = []
    for k in range(TRIALS):
        s = jnp.exp2(-jnp.full((1, Z), tp_ref[k], jnp.int32).astype(jnp.float32))
        v = it + s * step_dir
        low_x = cat([rx[KEPT, 0] + s * dhx[0], v[:-Y]])
        low_y = jnp.where(rows == 0, wide_y(ry[KEPT, 0] + s * dhy[0], X), roll(v, 1, 0))
        low_z = jnp.where(lanes == 0, wide_z(rz[KEPT, 0] + s * dhz[0], X), roll(v, 1, 1))
        at_end = energy(v)
        e = energy(v - low_x) + energy(v - low_y) + energy(v - low_z)
        e = e + at_end * (ends_y + ends_z)
        e = cat([e[:-Y], e[-Y:] + ends_x * at_end[-Y:]]) if X > 1 else e + ends_x * at_end
        e = e + 0.5 * rea_ref[...].reshape(X * Y, Z) * v * v - src_ref[...].reshape(X * Y, Z) * v
        by_layer = jnp.sum(jnp.sum(e.reshape(X, Y, Z), axis=1), axis=1, keepdims=True)
        trial_rows.append(jnp.sum(jnp.where(across, by_layer, 0.0), axis=0, keepdims=True))
    en_all[0, me] = jnp.concatenate(trial_rows, axis=0)
    gather(en_all, 0, nx * planes, me, in_grid, 2)
    layers = jnp.sum(en_all[0, pl.ds(ix * planes, planes)], axis=0)
    layers = layers / (Y * ny * Z * nz)
    le_ref[...] = layers[:, :X]
    overall = jnp.sum(en_all[0], axis=0) / (Y * ny * Z * nz)
    overall = jnp.sum(overall, axis=1, keepdims=True) / (X * nx)
    en_ref[...] = jnp.broadcast_to(overall, (TRIALS, Z))


def on_device(counts, iterate, source, reaction, trial_powers):
    X, Y, Z = iterate.shape
    nx, ny, nz = counts
    f32 = jnp.float32
    slots = ROUND + 1
    vm = pltpu.VMEM
    scratch = [vm((slots, 2, rows, Z), f32) for rows in (Y, Y, X, X, Y, Y)]
    scratch += [pltpu.SemaphoreType.DMA((slots, 6))] * 2
    x_own, y_own = X // 4, Y // 4
    GX, GY, GZ = nx * x_own, ny * y_own, nz * Z // 4
    scratch += [vm((10, (X >> level) * Y, Z), f32) for level in range(2)]
    scratch += [vm((8, (GX >> level) * GY, GZ), f32) for level in range(2)]
    scratch += [vm((X * Y, Z), f32)] * 2
    scratch += [vm((2, rows, Z), f32) for rows in (Y, X, Y)] * 2
    scratch += [
        vm((2, nx * ny * nz, 1, Z), f32),
        vm((1, nx * ny * nz, TRIALS, Z), f32),
        pltpu.SemaphoreType.DMA((8, 2)), pltpu.SemaphoreType.DMA((8, 2)),
        vm((7 * x_own * Y, Z), f32),
        vm((2, ny * nz, x_own * y_own, GZ), f32), vm((2, nx, x_own * GY, GZ), f32),
        vm((1, ny * nz, 7 * x_own * y_own, GZ), f32), vm((1, nx, 7 * x_own * GY, GZ), f32),
        vm((2, (GX + 2) * GY, Z), f32),
    ]
    whole = pl.BlockSpec(memory_space=pltpu.VMEM)
    out = pl.pallas_call(
        functools.partial(kernel, (X, Y, Z), counts),
        out_shape=[
            jax.ShapeDtypeStruct((X, Y, Z), f32),
            jax.ShapeDtypeStruct((X, Y, Z), f32),
            jax.ShapeDtypeStruct((TRIALS, X), f32),
            jax.ShapeDtypeStruct((TRIALS, Z), f32),
        ],
        in_specs=[pl.BlockSpec(memory_space=pltpu.SMEM), whole, whole, whole],
        out_specs=[whole] * 4,
        scratch_shapes=scratch,
        compiler_params=pltpu.CompilerParams(has_side_effects=True, vmem_limit_bytes=48 * 1024 * 1024),
        name="newton_step",
    )(trial_powers, iterate, source, reaction)
    return out[0], out[1], out[2], out[3][:, 0]


LANES = 128
HALO = 8
PLANES = 2
PAIR = 2
CHUNK = 4
F_DG, F_XM, F_YM, F_ZM, F_XP, F_YP, F_ZP, F_INV = range(8)
C_ONE = RHO1 * RHO0
C_TWO = 2.0 * RHO1 / HALF
C_THREE = RHO2 * RHO1
C_FOUR = 2.0 * RHO2 / HALF


def slab_fits(counts, shape):
    X, Y, Z = shape
    nx, ny, nz = counts
    per = PLANES * ny * PAIR
    rows = PAIR * Z // per
    return (
        X == 1 << (LEVELS - 1) and X * Y == LANES and nx * ny == X and nx >= PLANES and nz % PAIR == 0
        and rows * per == PAIR * Z and rows % (2 * HALO) == 0 and Z % rows == 0
    )


def slab_kernel(
    sizes, counts, tp_ref, given, fields_out, sums_out,
    turned, d_it, d_rs, f_it, f_rea, f_src, w0, w1, w2, w3,
    va, vb, vz, rr, az, sa, ra, sb, rb, sc, rc, s0, r0, sq, rq,
    ua, ub, r1in, rr1, sa1, ra1, sb1, rb1, sc1, rc1, s1, r1, sq1, rq1, e2, cres, cq, cnew,
    p_ref, dir_ref, q_ref, r_ref,
    msg, gath, early, egath, wmsg, wgath, hb, he, sh, enmsg, engath, outs, back,
    d_ssem, d_rsem, g_ssem, g_rsem, h_ssem, h_rsem, b_ssem, b_rsem, counted,
):
    X, Y, Z = sizes
    nx, ny, nz = counts
    P = nx * ny
    GY = ny * Y
    NZ = nz * Z
    PER = PLANES * ny
    NS = PER * nz
    S = NZ // NS
    BLOCK = Z // S
    W = S + 2 * HALO
    f32 = jnp.float32
    ix, iy, iz = lax.axis_index("gx"), lax.axis_index("gy"), lax.axis_index("gz")
    me = (ix * ny + iy) * nz + iz
    own_tile = ix * ny + iy
    base = (nx - PLANES) // 2

    def fold(value, turn, size):
        return value + lax.rem(turn, 2) * (size - 1 - 2 * value)

    def device_of(s):
        c = s // PAIR
        plane = c // PER
        q = fold(lax.rem(c, PER), plane, PER)
        y = q // PLANES
        return (base + fold(lax.rem(q, PLANES), y, PLANES), y, plane * PAIR + lax.rem(s, PAIR))

    works = jnp.logical_and(ix >= base, ix < base + PLANES)
    plane = iz // PAIR
    slab = fold(iy * PLANES + fold(ix - base, iy, PLANES), plane, PER)
    slab = (plane * PER + slab) * PAIR + lax.rem(iz, PAIR)
    slab = jnp.where(works, slab, -BLOCK - 1)
    block = slab // BLOCK
    j = lax.rem(slab, BLOCK)

    has_lo, has_hi = slab > 0, slab < NS - 1
    lo_dev, hi_dev = device_of(jnp.maximum(slab - 1, 0)), device_of(jnp.clip(slab + 1, 0, NS - 1))

    def lane(n):
        return lax.broadcasted_iota(jnp.int32, (n, LANES), 1)

    def row(n):
        return lax.broadcasted_iota(jnp.int32, (n, LANES), 0)

    def low_bit(n, step):
        return lax.rem(lane(n), 2 * step) < step

    def swap(v, step):
        return jnp.where(low_bit(v.shape[0], step), roll(v, -step, 1), roll(v, step, 1))

    def pair(v, step):
        return v + swap(v, step)

    def pick_low(v, step):
        return jnp.where(low_bit(v.shape[0], step), v, roll(v, step, 1))

    def pick_high(v, step):
        return jnp.where(low_bit(v.shape[0], step), roll(v, -step, 1), v)

    def block_transpose(tiles):
        n = tiles[0].shape[0]
        k = P // 2
        while k:
            low = low_bit(n, Y * k)
            new = list(tiles)
            for i in range(P):
                if not i & k:
                    a, b = tiles[i], tiles[i | k]
                    new[i] = jnp.where(low, a, roll(b, Y * k, 1))
                    new[i | k] = jnp.where(low, roll(a, -Y * k, 1), b)
            tiles = new
            k //= 2
        return tiles

    parts = ((pl.ds(0, 1), d_it, 2 * HALO), (pl.ds(1, 2), d_rs, HALO))

    def pieces(a):
        halo = parts[a][2]
        for jd in range(BLOCK):
            first = S * jd - (halo if jd > 0 else 0)
            last = S * jd + S + (halo if jd < BLOCK - 1 else 0)
            yield BLOCK * iz + jd, None, first, last - first, 0 if jd > 0 else halo, jd
        yield BLOCK * iz + BLOCK, iz < nz - 1, Z - halo, halo, 0, BLOCK
        yield BLOCK * iz - 1, iz > 0, 0, halo, halo + S, BLOCK + 1

    def piece(a, to, first, count, there, number):
        which, landed, _ = parts[a]
        return pltpu.make_async_remote_copy(
            src_ref=turned.at[which, pl.ds(first, count)],
            dst_ref=landed.at[:, own_tile, pl.ds(there, count)],
            send_sem=d_ssem.at[a, number],
            recv_sem=d_rsem.at[a, max(number - BLOCK + 1, 0)],
            device_id=device_of(jnp.clip(to, 0, NS - 1)),
            device_id_type=MESH,
        )

    def both(a, b):
        return b if a is None else jnp.logical_and(a, b)

    barrier = pltpu.get_barrier_semaphore()
    for other in range(nx * ny * nz):
        @pl.when(me != other)
        def _():
            pl.semaphore_signal(
                barrier, inc=1, device_id=(other // (ny * nz), other // nz % ny, other % nz), device_id_type=MESH
            )

    for a, (which, landed, halo) in enumerate(parts):
        for i in (0,) if a == 0 else (1, 2):
            turned[i] = given[i * LANES : (i + 1) * LANES].T
        if a == 0:
            pl.semaphore_wait(barrier, nx * ny * nz - 1)
        for to, exists, first, count, there, number in pieces(a):
            @pl.when(both(exists, to != slab))
            def _():
                piece(a, to, first, count, there, number).start()

            @pl.when(both(exists, to == slab))
            def _():
                landed[:, own_tile, there : there + count] = turned[which, first : first + count]

    @pl.when(works)
    def _():
        for ref in (va, vb, vz, ua, ub, r1in, e2, p_ref, dir_ref, q_ref, sq, rq, sq1, rq1, cq, w1):
            ref[...] = jnp.zeros_like(ref)
        w1[F_DG] = jnp.ones(w1.shape[1:], f32)
        for side, at in ((0, 0), (1, NS - 1)):
            @pl.when(slab == at)
            def _():
                for ref in (hb, he):
                    ref[:, side] = jnp.zeros(ref.shape[:1] + ref.shape[2:], f32)

    def wait_sent():
        for a in range(2):
            for to, exists, first, count, there, number in pieces(a):
                @pl.when(both(exists, to != slab))
                def _():
                    piece(a, to, first, count, there, number).wait_send()

    def wait_landed(a, wanted, kind, first, count, source):
        mine = jnp.where(source == iz, 1, 0)
        for own in range(2):
            @pl.when(jnp.logical_and(wanted, mine == own))
            def _():
                view = parts[a][1].at[:, pl.ds(0, P - own), pl.ds(first, count)]
                pltpu.make_async_copy(view, view, d_rsem.at[a, kind]).wait()

    def gather_block(a):
        for _, landed, halo in parts[a : a + 1]:
            @pl.when(slab == 0)
            def _():
                landed[:, :, :halo] = jnp.zeros((landed.shape[0], P, halo, LANES), f32)

            @pl.when(slab == NS - 1)
            def _():
                landed[:, :, halo + S :] = jnp.zeros((landed.shape[0], P, halo, LANES), f32)

            for jd in range(BLOCK):
                count = S + (halo if jd > 0 else 0) + (halo if jd < BLOCK - 1 else 0)
                wait_landed(a, j == jd, 0, 0 if jd > 0 else halo, count, block)
            wait_landed(a, jnp.logical_and(j == 0, has_lo), 1, 0, halo, block - 1)
            wait_landed(a, jnp.logical_and(j == BLOCK - 1, has_hi), 2, halo + S, halo, block + 1)
            for i, flat in ((0, f_it),) if a == 0 else ((0, f_rea), (1, f_src)):
                for at in range(0, S + 2 * halo, HALO):
                    tiles = block_transpose([landed[i, t, at : at + HALO] for t in range(P)])
                    for t in range(P):
                        flat[t, at : at + HALO] = tiles[t]

    def back_copy(which, t):
        return pltpu.make_async_remote_copy(
            src_ref=outs.at[which, t],
            dst_ref=back.at[which, pl.ds(pl.multiple_of(S * j, HALO), S)],
            send_sem=b_ssem.at[which],
            recv_sem=b_rsem.at[which],
            device_id=(t // ny, t % ny, block),
            device_id_type=MESH,
        )

    def back_here(which):
        @pl.when(block == iz)
        def _():
            back[which, pl.ds(pl.multiple_of(S * j, HALO), S)] = outs[which, own_tile]

    def energy_copy(dev):
        return pltpu.make_async_remote_copy(
            src_ref=enmsg, dst_ref=engath.at[slab],
            send_sem=g_ssem.at[5], recv_sem=g_rsem.at[5],
            device_id=dev, device_id_type=MESH,
        )

    WROWS = 4 * (X // 4) * (S // (4 * CHUNK))

    @pl.when(works)
    def _():
        gather_block(0)

        lanes = lane(W)
        z_at = slab * S + row(W) - HALO
        inside = jnp.logical_and(z_at >= 0, z_at < NZ)
        z_low = jnp.logical_and(z_at > 0, z_at < NZ)
        z_high = jnp.logical_and(z_at >= 0, z_at < NZ - 1)
        x_first, x_last = lanes < GY, lanes >= LANES - GY
        y_at = lax.rem(lanes, GY)
        y_first, y_last = y_at == 0, y_at == GY - 1

        def face(g):
            square = g * g
            one = 1.0 + square
            inverse = lax.rsqrt(one)
            return (one + square) * inverse, g * (one * inverse)

        def window(t):
            return f_it[t, HALO : HALO + W]

        low_w, low_p = face(window(0) - jnp.where(x_first, 0.0, roll(window(X - 1), GY, 1)))
        for t in range(X):
            c = window(t)
            beyond = window(t + 1) if t < X - 1 else jnp.where(x_last, 0.0, roll(window(0), -GY, 1))
            high_w, high_p = face(beyond - c)
            yl_w, yl_p = face(c - jnp.where(y_first, 0.0, roll(c, 1, 1)))
            yh_w, yh_p = face(jnp.where(y_last, 0.0, roll(c, -1, 1)) - c)
            zl_w, zl_p = face(c - f_it[t, HALO - 1 : HALO - 1 + W])
            zh_w, zh_p = face(f_it[t, HALO + 1 : HALO + 1 + W] - c)
            w0[F_DG, t] = low_w + high_w + yl_w + yh_w + zl_w + zh_w
            w0[F_XM, t] = jnp.where(x_first, 0.0, low_w) if t == 0 else low_w
            w0[F_XP, t] = jnp.where(x_last, 0.0, high_w) if t == X - 1 else high_w
            w0[F_YM, t] = jnp.where(y_first, 0.0, yl_w)
            w0[F_YP, t] = jnp.where(y_last, 0.0, yh_w)
            w0[F_ZM, t] = jnp.where(z_low, zl_w, 0.0)
            w0[F_ZP, t] = jnp.where(z_high, zh_w, 0.0)
            az[t] = (high_p - low_p) + (yh_p - yl_p) + (zh_p - zl_p)
            low_w, low_p = high_w, high_p

        gather_block(1)
        for t in range(X):
            rea = f_rea[t]
            diagonal = w0[F_DG, t] + rea
            w0[F_DG, t] = diagonal
            w0[F_INV, t] = 1.0 / diagonal
            r = jnp.where(inside, f_src[t] - rea * window(t) + az[t], 0.0)
            az[t] = r
            r_ref[t] = r

        def coarsen(get, step):
            def build(k):
                def both(field, t):
                    low, high = get(field, t)
                    return low + high
                lo, hi = 2 * k, 2 * k + 1
                xm = pair(both(F_XM, lo), step)
                ym_all = both(F_YM, lo) + both(F_YM, hi)
                zl0, zh0 = get(F_ZM, lo)
                zl1, zh1 = get(F_ZM, hi)
                between = pair(both(F_XM, hi), step) + pick_high(ym_all, step) + pair(zh0 + zh1, step)
                diagonal = pair(both(F_DG, lo) + both(F_DG, hi), step) - 2.0 * between
                return diagonal, xm, pick_low(ym_all, step), pair(zl0 + zl1, step)
            return build

        n1 = W // 2
        S1 = S // 2
        W1 = S1 + 2 * HALO
        T1 = X // 2
        at1 = (W1 - n1) // 2

        def halves0(field, t):
            return w0[field, t, pl.ds(0, n1, stride=2)], w0[field, t, pl.ds(1, n1, stride=2)]

        for k in range(T1):
            for field, value in zip((F_DG, F_XM, F_YM, F_ZM), coarsen(halves0, 1)(k)):
                w1[field, k, at1 : at1 + n1] = value

        def complete1():
            for k in range(T1):
                w1[F_INV, k] = 1.0 / w1[F_DG, k]
                w1[F_XP, k] = w1[F_XM, k + 1] if k < T1 - 1 else roll(w1[F_XM, 0], -GY, 1)
                w1[F_YP, k] = roll(w1[F_YM, k], -2, 1)
                w1[F_ZP, k] = roll(w1[F_ZM, k], -1, 0)

        complete1()

        S2 = S // 4
        T2 = X // 4
        LINES = S2 // CHUNK

        def halves1(field, t):
            return w1[field, t, pl.ds(HALO, S2, stride=2)], w1[field, t, pl.ds(HALO + 1, S2, stride=2)]

        own_chunk = lax.rem(lane(S2), CHUNK) == lax.rem(row(S2), CHUNK)

        def pack(ref, first, v):
            v = jnp.where(own_chunk, v, 0.0)
            for h in range(LINES):
                ref[first + h : first + h + 1] = jnp.sum(jnp.where(row(S2) // CHUNK == h, v, 0.0), axis=0, keepdims=True)

        for k in range(T2):
            for field, value in zip((F_DG, F_XM, F_YM, F_ZM), coarsen(halves1, 2)(k)):
                pack(wmsg, (field * T2 + k) * LINES, value)

        def sweep(w, v, step, use):
            T, n = w.shape[1], w.shape[2]
            for at in range(0, n, HALO):
                rows, shifted = slice(at, at + HALO), slice(at + HALO, at + 2 * HALO)
                c = [v[t, shifted] for t in range(T)]
                low = w[F_XM, 0, rows]
                for t in range(T):
                    below = c[t - 1] if t > 0 else roll(c[T - 1], GY, 1)
                    above = c[t + 1] if t < T - 1 else roll(c[0], -GY, 1)
                    high = w[F_XM, t + 1, rows] if t < T - 1 else w[F_XP, t, rows]
                    ym = w[F_YM, t, rows]
                    acc = w[F_DG, t, rows] * c[t] - low * below - high * above
                    acc = acc - ym * roll(c[t], step, 1) - roll(ym * c[t], -step, 1)
                    acc = acc - w[F_ZM, t, rows] * v[t, at + HALO - 1 : at + 2 * HALO - 1]
                    acc = acc - w[F_ZP, t, rows] * v[t, at + HALO + 1 : at + 2 * HALO + 1]
                    use(t, rows, shifted, c[t], acc)
                    low = high

        def before(w, r_of, u1, u2, rem1, s_out, r_out, step):
            T, n = w.shape[1], w.shape[2]
            for at in range(0, n, HALO):
                for t in range(T):
                    rows = slice(at, at + HALO)
                    u1[t, at + HALO : at + 2 * HALO] = w[F_INV, t, rows] * r_of[t, rows] * (1.0 / MID)

            def second(t, rows, shifted, first, image):
                r = r_of[t, rows] - image
                u = C_ONE * first + C_TWO * w[F_INV, t, rows] * r
                u2[t, shifted] = u
                s_out[t, rows] = first + u
                rem1[t, rows] = r

            def rest(t, rows, shifted, u, image):
                r_out[t, rows] = rem1[t, rows] - image

            sweep(w, u1, step, second)
            sweep(w, u2, step, rest)

        def after(w, e, u1, rem1, s_in, r_in, put, step):
            def first(t, rows, shifted, c, image):
                r = r_in[t, rows] - image
                rem1[t, rows] = r
                u1[t, shifted] = w[F_INV, t, rows] * r * (1.0 / MID)

            def second(t, rows, shifted, u, image):
                r = rem1[t, rows] - image
                put(t, rows, s_in[t, rows] + e[t, shifted] + (1.0 + C_ONE) * u + C_TWO * w[F_INV, t, rows] * r)

            sweep(w, e, step, first)
            sweep(w, u1, step, second)

        kept = ((az, sa, ra, sa1, ra1), (r_ref, sb, rb, sb1, rb1), (r_ref, sc, rc, sc1, rc1))

        def presmooth(f, ref, par):
            r_of, s_out, r_out, s1_out, r1_out = kept[f]
            before(w0, r_of, va, vb, rr, s_out, r_out, 1)
            for k in range(T1):
                total = None
                for t in (2 * k, 2 * k + 1):
                    part = r_out[t, pl.ds(0, n1, stride=2)] + r_out[t, pl.ds(1, n1, stride=2)]
                    total = part if total is None else total + part
                r1in[k, at1 : at1 + n1] = pair(total, 1)
            before(w1, r1in, ua, ub, rr1, s1_out, r1_out, 2)
            for k in range(T2):
                total = None
                for t in (2 * k, 2 * k + 1):
                    part = r1_out[t, pl.ds(HALO, S2, stride=2)] + r1_out[t, pl.ds(HALO + 1, S2, stride=2)]
                    total = part if total is None else total + part
                pack(ref.at[par], k * LINES, pair(total, 2))

        def to_workers(ref, out, sem):
            for s in range(NS):
                @pl.when(slab != s)
                def _():
                    pltpu.make_async_remote_copy(
                        src_ref=ref, dst_ref=out.at[slab], send_sem=g_ssem.at[sem], recv_sem=g_rsem.at[sem],
                        device_id=device_of(s), device_id_type=MESH,
                    ).start()
            out[slab] = ref[...]

        def from_workers(out, sem):
            others = out.at[pl.ds(0, NS - 1)]
            pltpu.make_async_copy(others, others, g_rsem.at[sem]).wait()
            pltpu.make_async_copy(others, others, g_ssem.at[sem]).wait()

        def unpack(out, packed):
            for k in range(T2):
                for s in range(NS):
                    out[k, s * LINES : (s + 1) * LINES] = packed[s, k * LINES : (k + 1) * LINES]

        per = 2 * (X + T1)
        halo_parts = tuple(
            ((of[3], 0, T1, S1), (of[4], T1, T1, S1), (of[1], 2 * T1, X, S), (of[2], 2 * T1 + X, X, S)) for of in kept
        )
        halo_at = (hb, he, he)

        def halo_send(f, par):
            for side, there, dev in ((0, has_lo, lo_dev), (1, has_hi, hi_dev)):
                @pl.when(there)
                def _():
                    for ref, first, count, size in halo_parts[f]:
                        start_row = HALO if side == 0 else size
                        pltpu.make_async_remote_copy(
                            src_ref=ref.at[:, pl.ds(start_row, HALO)],
                            dst_ref=halo_at[f].at[par, 1 - side, pl.ds(first, count)],
                            send_sem=h_ssem.at[2 * min(f, 1) + par, side],
                            recv_sem=h_rsem.at[2 * min(f, 1) + par, 1 - side],
                            device_id=dev,
                            device_id_type=MESH,
                        ).start()

        def halo_wait(view_of, sem):
            for side, there in ((0, has_lo), (1, has_hi)):
                @pl.when(there)
                def _():
                    view = view_of(side)
                    pltpu.make_async_copy(view, view, h_rsem.at[sem, side]).wait()
                    pltpu.make_async_copy(view, view, h_ssem.at[sem, side]).wait()

        chunk = lax.rem(lane(NS * LINES), CHUNK)

        def down2(v):
            return jnp.where(chunk == 0, roll(roll(v, 1 - CHUNK, 1), 1, 0), roll(v, 1, 1))

        def up2(v):
            return jnp.where(chunk == CHUNK - 1, roll(roll(v, CHUNK - 1, 1), -1, 0), roll(v, -1, 1))

        def down3(v):
            return jnp.where(chunk < CHUNK // 2, roll(roll(v, -(CHUNK // 2), 1), 1, 0), roll(v, CHUNK // 2, 1))

        def up3(v):
            return jnp.where(chunk >= CHUNK // 2, roll(roll(v, CHUNK // 2, 1), -1, 0), roll(v, -(CHUNK // 2), 1))

        def lap_all(w, vs, step, down, up):
            T = len(vs)
            out = []
            for t in range(T):
                v = vs[t]
                below = vs[t - 1] if t > 0 else roll(vs[T - 1], GY, 1)
                above = vs[t + 1] if t < T - 1 else roll(vs[0], -GY, 1)
                acc = w[F_DG, t] * v - w[F_XM, t] * below - w[F_XP, t] * above
                acc = acc - w[F_YM, t] * roll(v, step, 1) - w[F_YP, t] * roll(v, -step, 1)
                out.append(acc - w[F_ZM, t] * down(v) - w[F_ZP, t] * up(v))
            return out

        def complete_all(w, step, up):
            T = w.shape[1]
            for t in range(T):
                w[F_INV, t] = 1.0 / w[F_DG, t]
                w[F_XP, t] = w[F_XM, t + 1] if t < T - 1 else roll(w[F_XM, 0], -GY, 1)
                w[F_YP, t] = roll(w[F_YM, t], -step, 1)
                w[F_ZP, t] = up(w[F_ZM, t])

        def world():
            def apply2(v):
                return lap_all(w2, v, CHUNK, down2, up2)

            def apply3(v):
                return lap_all(w3, v, 2 * CHUNK, down3, up3)

            def scaled(w, r):
                return [w[F_INV, t] * r[t] for t in range(len(r))]

            def minus(a, b):
                return [x - y for x, y in zip(a, b)]

            def plus(*many):
                return [sum(vs[1:], vs[0]) for vs in zip(*many)]

            def first(w, r):
                return [d * (1.0 / MID) for d in scaled(w, r)]

            def follow(w, u, r, one, two):
                return [one * a + two * d for a, d in zip(u, scaled(w, r))]

            r = [cres[k] for k in range(T2)]
            u = first(w2, r)
            r = minus(r, apply2(u))
            u2 = follow(w2, u, r, C_ONE, C_TWO)
            total = plus(u, u2)
            r = minus(r, apply2(u2))
            rc = [pair(pair(r[0] + r[1], CHUNK), 1)]
            u = first(w3, rc)
            rc = minus(rc, apply3(u))
            v = follow(w3, u, rc, C_ONE, C_TWO)
            e = plus(u, v)
            rc = minus(rc, apply3(v))
            e = plus(e, follow(w3, v, rc, C_THREE, C_FOUR))
            e = [e[0]] * T2
            total = plus(total, e)
            r = minus(r, apply2(e))
            u = first(w2, r)
            r = minus(r, apply2(u))
            total = plus(total, u, follow(w2, u, r, C_ONE, C_TWO))
            for k in range(T2):
                e2[k, HALO : HALO + NS * LINES] = total[k]

        def precondition():
            own = lax.rem(lane(CHUNK), CHUNK) == row(CHUNK)
            for d in range(LINES + 2):
                for k in range(T2):
                    line = e2[k, pl.ds(slab * LINES + HALO - 1 + d, 1)]
                    v = jnp.where(own, jnp.broadcast_to(line, (CHUNK, LANES)), 0.0)
                    v = pair(pair(v, 1), 2)
                    for t in (2 * k, 2 * k + 1):
                        for half in range(2):
                            ua[t, pl.ds(HALO + 2 * CHUNK * d + half, CHUNK, stride=2)] = v

            def put1(k, rows, v):
                for t in (2 * k, 2 * k + 1):
                    for half in range(2):
                        va[t, pl.ds(2 * rows.start + half, HALO, stride=2)] = v

            def put0(t, rows, v):
                vz[t, rows.start + HALO : rows.stop + HALO] = v

            after(w1, ua, ub, rr1, s1, r1, put1, 2)
            after(w0, va, vb, rr, s0, r0, put0, 1)

        def total_of(v):
            return jnp.sum(jnp.sum(v, axis=0, keepdims=True), axis=1, keepdims=True)

        lane_1 = lane(1)

        def image_and_dots(par):
            sums = []

            def use(t, rows, shifted, z, image):
                az[t, rows] = image
                if HALO <= rows.start < HALO + S:
                    parts = (r_ref[t, rows] * z, z * image, z * q_ref[t, rows])
                    sums[:] = [a + b for a, b in zip(sums, parts)] if sums else parts

            sweep(w0, vz, 1, use)
            rz, zaz, zq = (total_of(v) for v in sums)
            msg[par, T2 * LINES :] = jnp.where(lane_1 == 0, rz, jnp.where(lane_1 == 1, zaz, zq))

        lane_1 = lane(1)

        def lane_of(v, i):
            return jnp.sum(jnp.where(lane_1 == i, v, 0.0), axis=1, keepdims=True)

        def scalars(par, rz_old, pq_old):
            sums = gath[par, 0, T2 * LINES :]
            for s in range(1, NS):
                sums = sums + gath[par, s, T2 * LINES :]
            rz, zaz, zq = lane_of(sums, 0), lane_of(sums, 1), lane_of(sums, 2)
            beta = rz / rz_old
            pq = zaz + 2.0 * beta * zq + beta * beta * pq_old
            return rz, pq, rz / pq, beta

        def advance(a, beta):
            for t in range(X):
                p = vz[t, HALO : HALO + HALO + S] + beta * p_ref[t]
                p_ref[t] = p
                dir_ref[t] = dir_ref[t] + a * p
                q = az[t] + beta * q_ref[t]
                q_ref[t] = q
                r_ref[t] = r_ref[t] - a * q

        def coarse_advance(par, a, beta, fresh):
            unpack(cnew, gath.at[par])
            if fresh:
                unpack(cres, egath.at[par])
            for k in range(T2):
                v = cnew[k] + beta * cq[k]
                cq[k] = v
                cres[k] = cres[k] - a * v

        def kept_advance(par, a, beta, fresh):
            for i, (keep, slope) in enumerate(((s1, sq1), (r1, rq1), (s0, sq), (r0, rq))):
                moved, first, count, size = halo_parts[0][i]
                true = halo_parts[1 + par][i][0]
                for t in range(count):
                    for side, rows in ((0, slice(0, HALO)), (None, slice(HALO, HALO + size)), (1, slice(HALO + size, 2 * HALO + size))):
                        got = moved[t, rows] if side is None else hb[par, side, first + t]
                        if a is None:
                            keep[t, rows] = got
                            continue
                        v = got + beta * slope[t, rows]
                        slope[t, rows] = v
                        if not fresh:
                            start = keep[t, rows]
                        else:
                            start = true[t, rows] if side is None else he[par, side, first + t]
                        keep[t, rows] = start - a * v

        for s in range(NS):
            @pl.when(slab != s)
            def _():
                pltpu.make_async_remote_copy(
                    src_ref=wmsg, dst_ref=wgath.at[pl.ds(pl.multiple_of(slab * WROWS, HALO), WROWS)],
                    send_sem=g_ssem.at[4], recv_sem=g_rsem.at[4], device_id=device_of(s), device_id_type=MESH,
                ).start()
        wgath[pl.ds(pl.multiple_of(slab * WROWS, HALO), WROWS)] = wmsg[...]
        for side, there, dev in ((0, has_lo, lo_dev), (1, has_hi, hi_dev)):
            @pl.when(there)
            def _():
                pltpu.make_async_remote_copy(
                    src_ref=w1.at[pl.ds(0, 4), :, pl.ds(HALO if side == 0 else S1, HALO)], dst_ref=sh.at[1 - side],
                    send_sem=h_ssem.at[4, side], recv_sem=h_rsem.at[4, 1 - side],
                    device_id=dev, device_id_type=MESH,
                ).start()
        presmooth(0, msg, 0)
        msg[0, T2 * LINES :] = jnp.zeros((1, LANES), f32)
        to_workers(msg.at[0], gath.at[0], 0)
        halo_send(0, 0)
        wait_sent()

        others = wgath.at[pl.ds(0, (NS - 1) * WROWS)]
        pltpu.make_async_copy(others, others, g_rsem.at[4]).wait()
        pltpu.make_async_copy(others, others, g_ssem.at[4]).wait()
        for field in range(4):
            for k in range(T2):
                for h in range(LINES):
                    line = (field * T2 + k) * LINES + h
                    w2[field, k, pl.ds(h, NS, stride=LINES)] = wgath[pl.ds(line, NS, stride=WROWS)]
        complete_all(w2, CHUNK, up2)
        dg, xm, ym, zm = F_DG, F_XM, F_YM, F_ZM
        ym_all = pair(w2[ym, 0] + w2[ym, 1], 1)
        zm_all = pair(w2[zm, 0] + w2[zm, 1], CHUNK)
        between = pair(pair(w2[xm, 1], CHUNK), 1) + pick_high(ym_all, CHUNK) + pick_high(zm_all, 1)
        w3[dg, 0] = pair(pair(w2[dg, 0] + w2[dg, 1], CHUNK), 1) - 2.0 * between
        w3[xm, 0] = pair(pair(w2[xm, 0], CHUNK), 1)
        w3[ym, 0] = pick_low(ym_all, CHUNK)
        w3[zm, 0] = pick_low(zm_all, 1)
        complete_all(w3, 2 * CHUNK, up3)
        halo_wait(lambda side: sh.at[side], 4)
        for side, there in ((0, has_lo), (1, has_hi)):
            @pl.when(there)
            def _():
                first = 0 if side == 0 else HALO + S1
                for field in range(4):
                    w1[field, :, first : first + HALO] = sh[side, field]
        complete1()
        from_workers(gath.at[0], 0)
        unpack(cres, gath.at[0])
        halo_wait(lambda side: hb.at[0, side], 0)
        kept_advance(0, None, None, False)

        rz, pq = jnp.ones((1, 1), f32), jnp.zeros((1, 1), f32)
        a = beta = None
        for it in range(ITERS):
            par, last, first = (it + 1) % 2, it == ITERS - 1, it == 0
            fresh = not (first or last)
            if fresh:
                presmooth(1 + par, early, par)
            world()
            if fresh:
                to_workers(early.at[par], egath.at[par], 2 + par)
                halo_send(1 + par, par)
            if not first:
                was = it % 2
                halo_wait(lambda side: hb.at[was, side], was)
                if it > 1:
                    halo_wait(lambda side: he.at[was, side], 2 + was)
                kept_advance(was, a, beta, it > 1)
            precondition()
            image_and_dots(par)
            if not last:
                presmooth(0, msg, par)
            to_workers(msg.at[par], gath.at[par], par)
            if not last:
                halo_send(0, par)
            from_workers(gath.at[par], par)
            rz, pq, a, beta = scalars(par, rz, pq)
            if fresh:
                from_workers(egath.at[par], 2 + par)
            if not last:
                coarse_advance(par, a, beta, fresh)
            advance(a, beta)

        def send_back(which):
            for at in range(0, S, HALO):
                ref = r_ref if which else dir_ref
                tiles = block_transpose([ref[t, HALO + at : 2 * HALO + at] for t in range(X)])
                for t in range(X):
                    outs[which, t, at : at + HALO] = tiles[t]
            for t in range(P):
                remote = jnp.logical_or(block != iz, own_tile != t)

                @pl.when(remote)
                def _():
                    back_copy(which, t).start()
            back_here(which)

        send_back(1)

        def energy(g):
            square = 1.0 + g * g
            return (square * (square * lax.rsqrt(square)) - 1.0) * (1.0 / 3.0)

        lanes = lane(S)
        y_at = lax.rem(lanes, GY)
        x_first, x_last, y_first = lanes < GY, lanes >= LANES - GY, y_at == 0
        ends = jnp.where(y_at == GY - 1, 1.0, 0.0) + jnp.where(slab * S + row(S) == NZ - 1, 1.0, 0.0)
        ends_x = ends + jnp.where(x_last, 1.0, 0.0)
        fetch = lax.rem(lane_1, GY)
        packed = jnp.zeros((1, LANES), f32)
        for k in range(TRIALS):
            s = jnp.exp2(-jnp.full((1, LANES), tp_ref[k], jnp.int32).astype(f32))

            def trial(t, shift):
                first = 2 * HALO - shift
                return f_it[t, first : first + S] + s * dir_ref[t, HALO - shift : HALO - shift + S]

            below = jnp.where(x_first, 0.0, roll(trial(X - 1, 0), GY, 1))
            for t in range(X):
                v = trial(t, 0)
                e = energy(v - below) + energy(v - trial(t, 1))
                e = e + energy(v - jnp.where(y_first, 0.0, roll(v, 1, 1)))
                e = e + energy(v) * (ends_x if t == X - 1 else ends)
                e = e + (0.5 * f_rea[t, HALO : HALO + S] * v - f_src[t, HALO : HALO + S]) * v
                column = jnp.sum(e, axis=0, keepdims=True)
                step = 1
                while step < GY:
                    column = pair(column, step)
                    step *= 2
                packed = packed + jnp.where(fetch == k * X + t, column, 0.0)
                below = v
        enmsg[...] = packed
        engath[slab] = packed
        for other in range(nx * ny * nz):
            @pl.when(me != other)
            def _():
                energy_copy((other // (ny * nz), other // nz % ny, other % nz)).start()
        send_back(0)

    @pl.when(jnp.logical_not(works))
    def _():
        wait_sent()

    for which in (1, 0):
        for own in range(2):
            @pl.when(jnp.where(block == iz, 1, 0) == own)
            def _():
                view = back.at[which, pl.ds(0, Z - own * S)]
                pltpu.make_async_copy(view, view, b_rsem.at[which]).wait()
        fields_out[which] = back[which].T.reshape(X, Y, Z)
    @pl.when(works)
    def _():
        others = engath.at[pl.ds(0, NS - 1)]
        pltpu.make_async_copy(others, others, g_rsem.at[5]).wait()
        sent = counted.at[pl.ds(0, nx * ny * nz - 1)]
        pltpu.make_async_copy(sent, sent, g_ssem.at[5]).wait()
        for which in range(2):
            for own in range(2):
                @pl.when(jnp.where(block == iz, 1, 0) == own)
                def _():
                    sent = outs.at[which, pl.ds(0, P - own)]
                    pltpu.make_async_copy(sent, sent, b_ssem.at[which]).wait()

    @pl.when(jnp.logical_not(works))
    def _():
        pltpu.make_async_copy(engath, engath, g_rsem.at[5]).wait()

    lane_1 = lane(1)
    fetch = lax.rem(lane_1, GY)
    layers = jnp.sum(engath[...], axis=0) / (GY * NZ)
    here = jnp.where(lane_1 // GY == ix, layers, 0.0)
    at_k = lax.broadcasted_iota(jnp.int32, (TRIALS * X, LANES), 0)
    mine = jnp.sum(jnp.where(lax.rem(lane(TRIALS * X), GY) == at_k, here, 0.0), axis=1, keepdims=True)
    mine = jnp.where(lane(TRIALS * X) == lax.rem(at_k, X), mine, 0.0)
    for k in range(TRIALS):
        sums_out[k : k + 1] = jnp.sum(mine[k * X : k * X + X], axis=0, keepdims=True)
        total = jnp.sum(jnp.where(fetch // X == k, layers, 0.0), axis=1, keepdims=True) / (X * nx)
        sums_out[TRIALS + k : TRIALS + k + 1] = jnp.broadcast_to(total, (1, LANES))


def hand_out(fields, sums, dir_out, rem_out, le_out, en_out, le, en, sem):
    copies = [pltpu.make_async_copy(fields.at[i], out, sem.at[i]) for i, out in ((0, dir_out), (1, rem_out))]
    for copy in copies:
        copy.start()
    le[...] = sums[:TRIALS, : le.shape[1]]
    for k in range(TRIALS):
        en[k] = jnp.max(sums[TRIALS + k : TRIALS + k + 1])
    copies += [pltpu.make_async_copy(le, le_out, sem.at[2]), pltpu.make_async_copy(en, en_out, sem.at[3])]
    for copy in copies[2:]:
        copy.start()
    for copy in copies:
        copy.wait()


def slab_on_device(counts, iterate, source, reaction, trial_powers):
    X, Y, Z = iterate.shape
    nx, ny, nz = counts
    P = nx * ny
    NS = PLANES * ny * nz
    S = nz * Z // NS
    BLOCK = Z // S
    W, W1 = S + 2 * HALO, S // 2 + 2 * HALO
    T1, T2, T3 = X // 2, X // 4, X // 8
    LINES = S // (4 * CHUNK)
    C_ROWS, ROWS = T2 * LINES, NS * LINES
    f32 = jnp.float32

    def vm(*shape):
        return pltpu.VMEM(shape, f32)

    def sem(*shape):
        return pltpu.SemaphoreType.DMA(shape)

    full, padded = (X, W, LANES), (X, W + 2 * HALO, LANES)
    full1, padded1 = (T1, W1, LANES), (T1, W1 + 2 * HALO, LANES)
    scratch = [vm(3, Z, LANES), vm(1, P, W + 2 * HALO, LANES), vm(2, P, W, LANES)]
    scratch += [vm(*padded), vm(*full), vm(*full)]
    scratch += [vm(8, *full), vm(8, *full1), vm(8, T2, ROWS, LANES), vm(8, T3, ROWS, LANES)]
    scratch += [vm(*padded)] * 3 + [vm(*full)] * 12
    scratch += [vm(*padded1)] * 2 + [vm(*full1)] * 12
    scratch += [vm(T2, ROWS + 2 * HALO, LANES)] + [vm(T2, ROWS, LANES)] * 3
    scratch += [vm(X, S + HALO, LANES)] * 2 + [vm(*full)] * 2
    scratch += [vm(2, C_ROWS + 1, LANES), vm(2, NS, C_ROWS + 1, LANES), vm(2, C_ROWS, LANES), vm(2, NS, C_ROWS, LANES)]
    scratch += [vm(4 * C_ROWS, LANES), vm(NS * 4 * C_ROWS, LANES)]
    scratch += [vm(2, 2, 2 * (X + T1), HALO, LANES)] * 2 + [vm(2, 4, T1, HALO, LANES)]
    scratch += [vm(1, LANES), vm(NS, 1, LANES), vm(2, P, S, LANES), vm(2, Z, LANES)]
    scratch += [sem(2, BLOCK + 2), sem(2, 3), sem(6), sem(6), sem(5, 2), sem(5, 2), sem(2), sem(2), vm(nx * ny * nz, 1, LANES)]
    whole = pl.BlockSpec(memory_space=pltpu.VMEM)
    given = jnp.concatenate([v.reshape(LANES, Z) for v in (iterate, reaction, source)])
    fields, sums = pl.pallas_call(
        functools.partial(slab_kernel, (X, Y, Z), counts),
        out_shape=[jax.ShapeDtypeStruct((2, X, Y, Z), f32), jax.ShapeDtypeStruct((2 * TRIALS, LANES), f32)],
        in_specs=[pl.BlockSpec(memory_space=pltpu.SMEM), whole],
        out_specs=[whole] * 2,
        scratch_shapes=scratch,
        compiler_params=pltpu.CompilerParams(
            has_side_effects=True, collective_id=0, vmem_limit_bytes=32 * 1024 * 1024
        ),
        name="newton_step",
    )(trial_powers, given)
    return pl.pallas_call(
        hand_out,
        out_shape=[
            jax.ShapeDtypeStruct((X, Y, Z), f32),
            jax.ShapeDtypeStruct((X, Y, Z), f32),
            jax.ShapeDtypeStruct((TRIALS, X), f32),
            jax.ShapeDtypeStruct((TRIALS,), f32),
        ],
        in_specs=[whole] * 2,
        out_specs=[pl.BlockSpec(memory_space=pl.ANY)] * 4,
        scratch_shapes=[vm(TRIALS, X), pltpu.SMEM((TRIALS,), f32), sem(4)],
        compiler_params=pltpu.CompilerParams(vmem_limit_bytes=32 * 1024 * 1024),
        name="hand_out",
    )(fields, sums)


def solution(mesh):
    counts = tuple(mesh.shape[axis] for axis in ("gx", "gy", "gz"))
    grid = P("gx", "gy", "gz")

    def on_each(iterate, source, reaction, trial_powers):
        form = slab_on_device if slab_fits(counts, iterate.shape) else on_device
        return form(counts, iterate, source, reaction, trial_powers)

    return jax.shard_map(
        on_each,
        mesh=mesh,
        in_specs=(grid, grid, grid, P()),
        out_specs=(grid, grid, P(None, "gx"), P()),
        check_vma=False,
    )
```

```python
import functools

import jax
import jax.numpy as jnp
from jax import lax
from jax.experimental import pallas as pl
from jax.experimental.pallas import tpu as pltpu
from jax.sharding import PartitionSpec as P

ITERS = 4
LEVELS = 4
TRIALS = 4
MID = 1.15
HALF = 0.85
SIGMA = MID / HALF
RHO0 = 1.0 / SIGMA
RHO1 = 1.0 / (2.0 * SIGMA - RHO0)
RHO2 = 1.0 / (2.0 * SIGMA - RHO1)
ROUND = 3
KEPT = ROUND
DG, INV, XM, XP, YM, YP, ZM, ZP, YB, ZB = range(10)
MESH = pl.DeviceIdType.MESH


class Grid:
    def __init__(self, Y, Z):
        self.Y, self.Z = Y, Z

    def rows_of(self, x):
        return lax.rem(lax.broadcasted_iota(jnp.int32, (x * self.Y, self.Z), 0), self.Y)

    def lanes_of(self, x):
        return lax.broadcasted_iota(jnp.int32, (x * self.Y, self.Z), 1)

    def pair_x(self, v):
        Y = self.Y
        x = v.shape[0] // Y
        return cat([v[2 * i * Y : (2 * i + 1) * Y] + v[(2 * i + 1) * Y : (2 * i + 2) * Y] for i in range(x // 2)])

    def pick_x(self, v, odd):
        Y = self.Y
        x = v.shape[0] // Y
        return cat([v[(2 * i + odd) * Y : (2 * i + odd + 1) * Y] for i in range(x // 2)])

    def bit(self, v, level, axis):
        at = self.rows_of(v.shape[0] // self.Y) if axis == 0 else self.lanes_of(v.shape[0] // self.Y)
        return lax.rem(at, 2 << level) < (1 << level)

    def pair(self, v, level, axis):
        step = 1 << level
        return v + jnp.where(self.bit(v, level, axis), roll(v, -step, axis), roll(v, step, axis))

    def pick(self, v, level, axis, odd):
        step = 1 << level
        low = self.bit(v, level, axis)
        if odd:
            return jnp.where(low, roll(v, -step, axis), v)
        return jnp.where(low, v, roll(v, step, axis))

    def restrict(self, v, level):
        return self.pair(self.pair(self.pair_x(v), level, 0), level, 1)

    def prolong(self, v):
        Y = self.Y
        x = v.shape[0] // Y
        return cat([v[(i // 2) * Y : (i // 2 + 1) * Y] for i in range(2 * x)])

    def coarsen(self, ws, reaction, level):
        xm, xp, ym, yp, zm, zp = ws
        pair, pick = self.pair, self.pick
        ws = (
            pair(pair(self.pick_x(xm, 0), level, 0), level, 1),
            pair(pair(self.pick_x(xp, 1), level, 0), level, 1),
            pair(pick(self.pair_x(ym), level, 0, 0), level, 1),
            pair(pick(self.pair_x(yp), level, 0, 1), level, 1),
            pick(pair(self.pair_x(zm), level, 0), level, 1, 0),
            pick(pair(self.pair_x(zp), level, 0), level, 1, 1),
        )
        return ws, self.restrict(reaction, level)

    def put(self, w, level, ws, reaction):
        Y, Z = self.Y, self.Z
        xm, xp, ym, yp, zm, zp = ws
        step = 1 << level
        x = xm.shape[0] // Y
        rows, lanes = self.rows_of(x), self.lanes_of(x)
        diagonal = reaction + xm + xp + ym + yp + zm + zp
        zero = jnp.zeros_like(xm)
        w[DG] = diagonal
        w[INV] = 1.0 / diagonal
        w[XM] = xm
        w[XP] = xp
        w[YM] = jnp.where(rows < step, zero, ym)
        w[YP] = jnp.where(rows >= Y - step, zero, yp)
        w[ZM] = jnp.where(lanes < step, zero, zm)
        w[ZP] = jnp.where(lanes >= Z - step, zero, zp)
        if w.shape[0] > YB:
            w[YB] = jnp.where(rows < step, ym, jnp.where(rows >= Y - step, yp, zero))
            w[ZB] = jnp.where(lanes < step, zm, jnp.where(lanes >= Z - step, zp, zero))

    def inner(self, w, v, level):
        step = 1 << level
        acc = w[DG] * v
        acc = acc - w[YM] * roll(v, step, 0) - w[YP] * roll(v, -step, 0)
        acc = acc - w[ZM] * roll(v, step, 1) - w[ZP] * roll(v, -step, 1)
        Y = self.Y
        if v.shape[0] > Y:
            none = jnp.zeros((Y, self.Z), jnp.float32)
            acc = acc - w[XM] * cat([none, v[:-Y]]) - w[XP] * cat([v[Y:], none])
        return acc


def cat(parts):
    return parts[0] if len(parts) == 1 else jnp.concatenate(parts, axis=0)


def roll(v, shift, axis):
    return pltpu.roll(v, shift % v.shape[axis], axis)


def dot(a, b):
    return lax.dot_general(
        a, b, (((1,), (0,)), ((), ())), precision=lax.Precision.HIGHEST, preferred_element_type=jnp.float32
    )


def kernel(
    sizes, counts, tp_ref, it_ref, src_ref, rea_ref, dir_ref, rem_ref, le_ref, en_ref,
    sx, rx, sy, ry, sz, rz, ssem, rsem, lev0, lev1, glev2, glev3, p_ref, q_ref,
    phx, phy, phz, dhx, dhy, dhz, dot_all, en_all, red_ssem, red_rsem,
    picked, gat_pl, gat_x, set_pl, set_x, glob,
):
    X, Y, Z = sizes
    nx, ny, nz = counts
    planes = ny * nz
    levs = (lev0, lev1)
    L = len(levs)
    x_own, y_own, z_own = X >> L, Y >> L, Z >> L
    GY, GZ = ny * y_own, nz * z_own
    here, world = Grid(Y, Z), Grid(GY, GZ)
    rows_of, lanes_of = here.rows_of, here.lanes_of
    ix, iy, iz = lax.axis_index("gx"), lax.axis_index("gy"), lax.axis_index("gz")
    has = (ix > 0, ix < nx - 1, iy > 0, iy < ny - 1, iz > 0, iz < nz - 1)
    devs = (
        (ix - 1, iy, iz), (ix + 1, iy, iz), (ix, iy - 1, iz),
        (ix, iy + 1, iz), (ix, iy, iz - 1), (ix, iy, iz + 1),
    )
    send = (sx, sx, sy, sy, sz, sz)
    recv = (rx, rx, ry, ry, rz, rz)
    lane_y = lax.broadcasted_iota(jnp.int32, (Y, Z), 1)
    lane_1 = lax.broadcasted_iota(jnp.int32, (1, Z), 1)

    for d in range(6):
        @pl.when(jnp.logical_not(has[d]))
        def _():
            recv[d][:, d % 2] = jnp.zeros(recv[d].shape[:1] + recv[d].shape[2:], jnp.float32)

    def outgoing(d, slot):
        side = d % 2
        return pltpu.make_async_remote_copy(
            src_ref=send[d].at[slot, side],
            dst_ref=recv[d].at[slot, 1 - side],
            send_sem=ssem.at[slot, d],
            recv_sem=rsem.at[slot, d + 1 - 2 * side],
            device_id=devs[d],
            device_id_type=MESH,
        )

    def incoming(d, slot):
        side = d % 2
        return pltpu.make_async_remote_copy(
            src_ref=send[d].at[slot, side],
            dst_ref=recv[d].at[slot, side],
            send_sem=ssem.at[slot, d],
            recv_sem=rsem.at[slot, d],
            device_id=devs[d],
            device_id_type=MESH,
        )

    def go(d, slot):
        @pl.when(has[d])
        def _():
            outgoing(d, slot).start()

    def start(v, slot):
        x = v.shape[0] // Y
        sx[slot, 0] = v[:Y]
        sx[slot, 1] = v[-Y:]
        go(0, slot)
        go(1, slot)
        for i in range(x):
            sy[slot, 0, i : i + 1] = v[i * Y : i * Y + 1]
            sy[slot, 1, i : i + 1] = v[i * Y + Y - 1 : i * Y + Y]
        go(2, slot)
        go(3, slot)
        for side, lane in ((0, 0), (1, Z - 1)):
            packed = jnp.broadcast_to(v[:Y, lane : lane + 1], (Y, Z))
            for i in range(1, x):
                part = jnp.broadcast_to(v[i * Y : i * Y + Y, lane : lane + 1], (Y, Z))
                packed = jnp.where(lane_y == i, part, packed)
            sz[slot, side] = packed
        go(4, slot)
        go(5, slot)

    def finish(slot):
        for d in range(6):
            @pl.when(has[d])
            def _():
                copy = incoming(d, slot)
                copy.wait_recv()
                copy.wait_send()

    def wide_y(half, x):
        return cat([jnp.broadcast_to(half[i : i + 1], (Y, Z)) for i in range(x)])

    def wide_z(half, x):
        return cat([jnp.broadcast_to(half[:, i : i + 1], (Y, Z)) for i in range(x)])

    def beyond(w, acc, in_x0, in_x1, in_y, in_z):
        x = acc.shape[0] // Y
        acc = acc - w[YB] * in_y - w[ZB] * in_z
        low = w[XM, :Y] * in_x0
        high = w[XP, (x - 1) * Y :] * in_x1
        if x == 1:
            return acc - low - high
        return cat([acc[:Y] - low] + ([acc[Y:-Y]] if x > 2 else []) + [acc[-Y:] - high])

    def operate(v, level, slot):
        w = levs[level]
        x = X >> level
        start(v, slot)
        acc = here.inner(w, v, level)
        finish(slot)
        in_y = jnp.where(rows_of(x) < Y // 2, wide_y(ry[slot, 0], x), wide_y(ry[slot, 1], x))
        in_z = jnp.where(lanes_of(x) < Z // 2, wide_z(rz[slot, 0], x), wide_z(rz[slot, 1], x))
        return beyond(w, acc, rx[slot, 0], rx[slot, 1], in_y, in_z)

    turn = [0]

    def apply(v, level):
        slot = turn[0] % ROUND
        turn[0] += 1
        return operate(v, level, slot)

    def vcycle(r, level, part):
        w = levs[level]
        u = w[INV] * r * (1.0 / MID)
        total = u
        r = r - apply(u, level)
        u = RHO1 * RHO0 * u + 2.0 * RHO1 / HALF * w[INV] * r
        total = total + u
        r = r - apply(u, level)
        coarse = here.restrict(r, level)
        if level + 1 < L:
            e = here.prolong(vcycle(coarse, level + 1, part))
            r = r - apply(e, level)
        else:
            everywhere = collect(coarse, 1, part, gat_pl, gat_x, 4)
            e, ends = spread(world_cycle(everywhere[0], level + 1))
            r = r - beyond(w, here.inner(w, e, level), *ends)
        total = total + e
        u = w[INV] * r * (1.0 / MID)
        total = total + u
        r = r - apply(u, level)
        u = RHO1 * RHO0 * u + 2.0 * RHO1 / HALF * w[INV] * r
        return total + u

    def world_cycle(r, level):
        w = (glev2, glev3)[level - L]

        def apply(v):
            return world.inner(w, v, level - L)

        u = w[INV] * r * (1.0 / MID)
        total = u
        r = r - apply(u)
        u = RHO1 * RHO0 * u + 2.0 * RHO1 / HALF * w[INV] * r
        total = total + u
        r = r - apply(u)
        if level == LEVELS - 1:
            u = RHO2 * RHO1 * u + 2.0 * RHO2 / HALF * w[INV] * r
            return total + u
        e = world.prolong(world_cycle(world.restrict(r, level - L), level + 1))
        total = total + e
        r = r - apply(e)
        u = w[INV] * r * (1.0 / MID)
        total = total + u
        r = r - apply(u)
        u = RHO1 * RHO0 * u + 2.0 * RHO1 / HALF * w[INV] * r
        return total + u

    def hot(shape, wanted):
        at = lax.broadcasted_iota(jnp.int32, shape, 0)
        return jnp.where(at == wanted, 1.0, 0.0)

    def collect(v, fields, part, pl_ref, x_ref, which):
        count = fields * x_own * y_own
        picked[: fields * x_own * Y] = v
        own = picked[pl.ds(0, count, stride=1 << L), :]
        lane = lax.broadcasted_iota(jnp.int32, (Z, GZ), 1) - iz * z_own
        inside = jnp.logical_and(lane >= 0, lane < z_own)
        put = hot((Z, GZ), jnp.where(inside, lane * (1 << L), -1))
        pl_ref[part, my_plane] = dot(own, put)
        gather(pl_ref, part, planes, my_plane, in_plane, which)
        for j in range(ny):
            rows = pl_ref[part, j * nz]
            for k in range(1, nz):
                rows = rows + pl_ref[part, j * nz + k]
            for i in range(fields * x_own):
                x_ref[part, ix, i * GY + j * y_own : i * GY + (j + 1) * y_own] = rows[i * y_own : (i + 1) * y_own]
        gather(x_ref, part, nx, ix, in_column, which + 1)
        return [
            cat([x_ref[part, d, f * x_own * GY : (f + 1) * x_own * GY] for d in range(nx)]) for f in range(fields)
        ]

    def spread(v):
        lane = lax.broadcasted_iota(jnp.int32, (GZ, Z), 1)
        inside = hot((GZ, Z), iz * z_own + lane // (1 << L))
        outside = hot((GZ, Z), jnp.where(lane < Z // 2, iz * z_own - 1, iz * z_own + z_own))
        glob[0, GY : GY + nx * x_own * GY] = dot(v, inside)
        glob[1, GY : GY + nx * x_own * GY] = dot(v, outside)
        rows = rows_of(1)

        def layer(which, a):
            base = (ix * x_own + 1 + a) * GY + iy * y_own
            out = jnp.broadcast_to(glob[which, pl.ds(base, 1), :], (Y, Z))
            for j in range(1, y_own):
                row = jnp.broadcast_to(glob[which, pl.ds(base + j, 1), :], (Y, Z))
                out = jnp.where(rows < j << L, out, row)
            return out

        def rims(a):
            base = (ix * x_own + 1 + a) * GY + iy * y_own
            low = glob[0, pl.ds(base - 1, 1), :] * has_low
            high = glob[0, pl.ds(base + y_own, 1), :] * has_high
            return jnp.where(rows < Y // 2, jnp.broadcast_to(low, (Y, Z)), jnp.broadcast_to(high, (Y, Z)))

        has_low = jnp.where(iy > 0, 1.0, 0.0)
        has_high = jnp.where(iy < ny - 1, 1.0, 0.0)
        own = range(x_own)
        e = here.prolong(cat([layer(0, a) for a in own]))
        in_y = here.prolong(cat([rims(a) for a in own]))
        in_z = here.prolong(cat([layer(1, a) for a in own]))
        return e, (layer(0, -1), layer(0, x_own), in_y, in_z)

    def gather(ref, part, count, me, device, which):
        for j in range(count):
            @pl.when(me != j)
            def _():
                pltpu.make_async_remote_copy(
                    src_ref=ref.at[part, me],
                    dst_ref=ref.at[part, me],
                    send_sem=red_ssem.at[which, part],
                    recv_sem=red_rsem.at[which, part],
                    device_id=device(j),
                    device_id_type=MESH,
                ).start()
        if count > 1:
            others = ref.at[part, pl.ds(0, count - 1)]
            pltpu.make_async_copy(others, others, red_rsem.at[which, part]).wait()
            pltpu.make_async_copy(others, others, red_ssem.at[which, part]).wait()

    def in_plane(j):
        return (ix, j // nz, j % nz)

    def in_column(j):
        return (j, iy, iz)

    def in_grid(j):
        return (j // planes, j // nz % ny, j % nz)

    my_plane = iy * nz + iz
    me = ix * planes + my_plane

    def reduce_plane(ref, part, value, which):
        ref[part, my_plane] = value
        gather(ref, part, planes, my_plane, in_plane, which)
        return jnp.sum(ref[part], axis=0)

    def reduce_column(ref, part, value, which):
        ref[part, ix] = value
        gather(ref, part, nx, ix, in_column, which)
        return jnp.sum(ref[part], axis=0)

    def total_of(v):
        return jnp.sum(jnp.sum(v, axis=0, keepdims=True), axis=1, keepdims=True)

    def lane_of(row, i):
        return jnp.sum(jnp.where(lane_1 == i, row, 0.0), axis=1, keepdims=True)

    it = it_ref[...].reshape(X * Y, Z)
    reaction = rea_ref[...].reshape(X * Y, Z)
    start(it, KEPT)
    finish(KEPT)
    rows, lanes = rows_of(X), lanes_of(X)
    last_row, last_lane = rows == Y - 1, lanes == Z - 1
    n_xm = cat([rx[KEPT, 0], it[:-Y]])
    n_xp = cat([it[Y:], rx[KEPT, 1]])
    n_ym = jnp.where(rows == 0, wide_y(ry[KEPT, 0], X), roll(it, 1, 0))
    n_yp = jnp.where(last_row, wide_y(ry[KEPT, 1], X), roll(it, -1, 0))
    n_zm = jnp.where(lanes == 0, wide_z(rz[KEPT, 0], X), roll(it, 1, 1))
    n_zp = jnp.where(last_lane, wide_z(rz[KEPT, 1], X), roll(it, -1, 1))
    ws = []
    r = src_ref[...].reshape(X * Y, Z) - reaction * it
    for sign, n in ((-1, n_xm), (1, n_xp), (-1, n_ym), (1, n_yp), (-1, n_zm), (1, n_zp)):
        g = n - it
        square = g * g
        root = jnp.sqrt(1.0 + square)
        ws.append((1.0 + 2.0 * square) / root)
        r = r + g * root
    rem_ref[...] = r.reshape(X, Y, Z)
    here.put(levs[0], 0, ws, reaction)
    for level in range(L):
        ws, reaction = here.coarsen(ws, reaction, level)
        if level + 1 < L:
            here.put(levs[level + 1], level + 1, ws, reaction)
    glob[...] = jnp.zeros_like(glob)
    *ws, reaction = collect(cat(list(ws) + [reaction]), 7, 0, set_pl, set_x, 6)
    world.put(glev2, 0, ws, reaction)
    world.put(glev3, 1, *world.coarsen(ws, reaction, 0))
    for ref in (p_ref, q_ref, phx, phy, phz, dhx, dhy, dhz):
        ref[...] = jnp.zeros_like(ref)
    dir_ref[...] = jnp.zeros_like(dir_ref)

    def body(it_idx, carry):
        rz_old, pq_old = carry
        part = lax.rem(it_idx, 2)
        r = rem_ref[...].reshape(X * Y, Z)
        turn[0] = 0
        z = vcycle(r, 0, part)
        z_slot = turn[0] % ROUND
        az = apply(z, 0)
        q_old = q_ref[...]
        sums = jnp.where(
            lane_1 == 0,
            total_of(rem_ref[...].reshape(X * Y, Z) * z),
            jnp.where(lane_1 == 1, total_of(z * az), total_of(z * q_old)),
        )
        dot_all[part, me] = sums
        gather(dot_all, part, nx * planes, me, in_grid, 0)
        row = jnp.sum(dot_all[part], axis=0)
        rz_new, zaz, zq = lane_of(row, 0), lane_of(row, 1), lane_of(row, 2)
        beta = rz_new / rz_old
        pq = zaz + 2.0 * beta * zq + beta * beta * pq_old
        a = rz_new / pq
        p = z + beta * p_ref[...]
        q = az + beta * q_old
        p_ref[...] = p
        q_ref[...] = q
        dir_ref[...] = dir_ref[...] + (a * p).reshape(X, Y, Z)
        rem_ref[...] = rem_ref[...] - (a * q).reshape(X, Y, Z)
        for got, ph, dh in ((rx, phx, dhx), (ry, phy, dhy), (rz, phz, dhz)):
            for side in range(2):
                edge = got[z_slot, side] + beta * ph[side]
                ph[side] = edge
                dh[side] = dh[side] + a * edge
        return rz_new, pq

    one = jnp.ones((1, 1), jnp.float32)
    lax.fori_loop(0, ITERS, body, (one, jnp.zeros((1, 1), jnp.float32)))

    it = it_ref[...].reshape(X * Y, Z)
    step_dir = dir_ref[...].reshape(X * Y, Z)

    def energy(g):
        square = 1.0 + g * g
        return (square * jnp.sqrt(square) - 1.0) * (1.0 / 3.0)

    ends_y = jnp.where(jnp.logical_and(last_row, iy == ny - 1), 1.0, 0.0)
    ends_z = jnp.where(jnp.logical_and(last_lane, iz == nz - 1), 1.0, 0.0)
    ends_x = jnp.where(ix == nx - 1, 1.0, 0.0)
    across = lax.broadcasted_iota(jnp.int32, (X, Z), 0) == lax.broadcasted_iota(jnp.int32, (X, Z), 1)
    trial_rows = []
    for k in range(TRIALS):
        s = jnp.exp2(-jnp.full((1, Z), tp_ref[k], jnp.int32).astype(jnp.float32))
        v = it + s * step_dir
        low_x = cat([rx[KEPT, 0] + s * dhx[0], v[:-Y]])
        low_y = jnp.where(rows == 0, wide_y(ry[KEPT, 0] + s * dhy[0], X), roll(v, 1, 0))
        low_z = jnp.where(lanes == 0, wide_z(rz[KEPT, 0] + s * dhz[0], X), roll(v, 1, 1))
        at_end = energy(v)
        e = energy(v - low_x) + energy(v - low_y) + energy(v - low_z)
        e = e + at_end * (ends_y + ends_z)
        e = cat([e[:-Y], e[-Y:] + ends_x * at_end[-Y:]]) if X > 1 else e + ends_x * at_end
        e = e + 0.5 * rea_ref[...].reshape(X * Y, Z) * v * v - src_ref[...].reshape(X * Y, Z) * v
        by_layer = jnp.sum(jnp.sum(e.reshape(X, Y, Z), axis=1), axis=1, keepdims=True)
        trial_rows.append(jnp.sum(jnp.where(across, by_layer, 0.0), axis=0, keepdims=True))
    en_all[0, me] = jnp.concatenate(trial_rows, axis=0)
    gather(en_all, 0, nx * planes, me, in_grid, 2)
    layers = jnp.sum(en_all[0, pl.ds(ix * planes, planes)], axis=0)
    layers = layers / (Y * ny * Z * nz)
    le_ref[...] = layers[:, :X]
    overall = jnp.sum(en_all[0], axis=0) / (Y * ny * Z * nz)
    overall = jnp.sum(overall, axis=1, keepdims=True) / (X * nx)
    en_ref[...] = jnp.broadcast_to(overall, (TRIALS, Z))


def on_device(counts, iterate, source, reaction, trial_powers):
    X, Y, Z = iterate.shape
    nx, ny, nz = counts
    f32 = jnp.float32
    slots = ROUND + 1
    vm = pltpu.VMEM
    scratch = [vm((slots, 2, rows, Z), f32) for rows in (Y, Y, X, X, Y, Y)]
    scratch += [pltpu.SemaphoreType.DMA((slots, 6))] * 2
    x_own, y_own = X // 4, Y // 4
    GX, GY, GZ = nx * x_own, ny * y_own, nz * Z // 4
    scratch += [vm((10, (X >> level) * Y, Z), f32) for level in range(2)]
    scratch += [vm((8, (GX >> level) * GY, GZ), f32) for level in range(2)]
    scratch += [vm((X * Y, Z), f32)] * 2
    scratch += [vm((2, rows, Z), f32) for rows in (Y, X, Y)] * 2
    scratch += [
        vm((2, nx * ny * nz, 1, Z), f32),
        vm((1, nx * ny * nz, TRIALS, Z), f32),
        pltpu.SemaphoreType.DMA((8, 2)), pltpu.SemaphoreType.DMA((8, 2)),
        vm((7 * x_own * Y, Z), f32),
        vm((2, ny * nz, x_own * y_own, GZ), f32), vm((2, nx, x_own * GY, GZ), f32),
        vm((1, ny * nz, 7 * x_own * y_own, GZ), f32), vm((1, nx, 7 * x_own * GY, GZ), f32),
        vm((2, (GX + 2) * GY, Z), f32),
    ]
    whole = pl.BlockSpec(memory_space=pltpu.VMEM)
    out = pl.pallas_call(
        functools.partial(kernel, (X, Y, Z), counts),
        out_shape=[
            jax.ShapeDtypeStruct((X, Y, Z), f32),
            jax.ShapeDtypeStruct((X, Y, Z), f32),
            jax.ShapeDtypeStruct((TRIALS, X), f32),
            jax.ShapeDtypeStruct((TRIALS, Z), f32),
        ],
        in_specs=[pl.BlockSpec(memory_space=pltpu.SMEM), whole, whole, whole],
        out_specs=[whole] * 4,
        scratch_shapes=scratch,
        compiler_params=pltpu.CompilerParams(has_side_effects=True, vmem_limit_bytes=48 * 1024 * 1024),
        name="newton_step",
    )(trial_powers, iterate, source, reaction)
    return out[0], out[1], out[2], out[3][:, 0]


LANES = 128
HALO = 8
PLANES = 2
PAIR = 2
CHUNK = 4
F_DG, F_XM, F_YM, F_ZM, F_XP, F_YP, F_ZP, F_INV = range(8)
C_ONE = RHO1 * RHO0
C_TWO = 2.0 * RHO1 / HALF
C_THREE = RHO2 * RHO1
C_FOUR = 2.0 * RHO2 / HALF


def slab_fits(counts, shape):
    X, Y, Z = shape
    nx, ny, nz = counts
    per = PLANES * ny * PAIR
    rows = PAIR * Z // per
    return (
        X == 1 << (LEVELS - 1) and X * Y == LANES and nx * ny == X and nx >= PLANES and nz % PAIR == 0
        and rows * per == PAIR * Z and rows % (2 * HALO) == 0 and Z % rows == 0
    )


def slab_kernel(
    sizes, counts, tp_ref, given, fields_out, sums_out,
    turned, d_it, d_rs, f_it, f_rea, f_src, w0, w1, w2, w3,
    va, vb, vz, rr, az, sa, ra, sb, rb, sc, rc, s0, r0, sq, rq,
    ua, ub, r1in, rr1, sa1, ra1, sb1, rb1, sc1, rc1, s1, r1, sq1, rq1, e2, cres, cq, cnew,
    p_ref, dir_ref, q_ref, r_ref,
    msg, gath, early, egath, wmsg, wgath, hb, he, sh, enmsg, engath, outs, back,
    d_ssem, d_rsem, g_ssem, g_rsem, h_ssem, h_rsem, b_ssem, b_rsem, counted, columns,
):
    X, Y, Z = sizes
    nx, ny, nz = counts
    P = nx * ny
    GY = ny * Y
    NZ = nz * Z
    PER = PLANES * ny
    NS = PER * nz
    S = NZ // NS
    BLOCK = Z // S
    W = S + 2 * HALO
    f32 = jnp.float32
    ix, iy, iz = lax.axis_index("gx"), lax.axis_index("gy"), lax.axis_index("gz")
    me = (ix * ny + iy) * nz + iz
    own_tile = ix * ny + iy
    base = (nx - PLANES) // 2

    def fold(value, turn, size):
        return value + lax.rem(turn, 2) * (size - 1 - 2 * value)

    def device_of(s):
        c = s // PAIR
        plane = c // PER
        q = fold(lax.rem(c, PER), plane, PER)
        y = q // PLANES
        return (base + fold(lax.rem(q, PLANES), y, PLANES), y, plane * PAIR + lax.rem(s, PAIR))

    works = jnp.logical_and(ix >= base, ix < base + PLANES)
    plane = iz // PAIR
    slab = fold(iy * PLANES + fold(ix - base, iy, PLANES), plane, PER)
    slab = (plane * PER + slab) * PAIR + lax.rem(iz, PAIR)
    slab = jnp.where(works, slab, -BLOCK - 1)
    block = slab // BLOCK
    j = lax.rem(slab, BLOCK)

    has_lo, has_hi = slab > 0, slab < NS - 1
    lo_dev, hi_dev = device_of(jnp.maximum(slab - 1, 0)), device_of(jnp.clip(slab + 1, 0, NS - 1))

    def lane(n):
        return lax.broadcasted_iota(jnp.int32, (n, LANES), 1)

    def row(n):
        return lax.broadcasted_iota(jnp.int32, (n, LANES), 0)

    def low_bit(n, step):
        return lax.rem(lane(n), 2 * step) < step

    def swap(v, step):
        return jnp.where(low_bit(v.shape[0], step), roll(v, -step, 1), roll(v, step, 1))

    def pair(v, step):
        return v + swap(v, step)

    def pick_low(v, step):
        return jnp.where(low_bit(v.shape[0], step), v, roll(v, step, 1))

    def pick_high(v, step):
        return jnp.where(low_bit(v.shape[0], step), roll(v, -step, 1), v)

    def block_transpose(tiles):
        n = tiles[0].shape[0]
        k = P // 2
        while k:
            low = low_bit(n, Y * k)
            new = list(tiles)
            for i in range(P):
                if not i & k:
                    a, b = tiles[i], tiles[i | k]
                    new[i] = jnp.where(low, a, roll(b, Y * k, 1))
                    new[i | k] = jnp.where(low, roll(a, -Y * k, 1), b)
            tiles = new
            k //= 2
        return tiles

    parts = ((pl.ds(0, 1), d_it, 2 * HALO), (pl.ds(1, 2), d_rs, HALO))

    def pieces(a):
        halo = parts[a][2]
        for jd in range(BLOCK):
            first = S * jd - (halo if jd > 0 else 0)
            last = S * jd + S + (halo if jd < BLOCK - 1 else 0)
            yield BLOCK * iz + jd, None, first, last - first, 0 if jd > 0 else halo, jd
        yield BLOCK * iz + BLOCK, iz < nz - 1, Z - halo, halo, 0, BLOCK
        yield BLOCK * iz - 1, iz > 0, 0, halo, halo + S, BLOCK + 1

    def piece(a, to, first, count, there, number):
        which, landed, _ = parts[a]
        return pltpu.make_async_remote_copy(
            src_ref=turned.at[which, pl.ds(first, count)],
            dst_ref=landed.at[:, own_tile, pl.ds(there, count)],
            send_sem=d_ssem.at[a, number],
            recv_sem=d_rsem.at[a, max(number - BLOCK + 1, 0)],
            device_id=device_of(jnp.clip(to, 0, NS - 1)),
            device_id_type=MESH,
        )

    def both(a, b):
        return b if a is None else jnp.logical_and(a, b)

    barrier = pltpu.get_barrier_semaphore()
    for other in range(nx * ny * nz):
        @pl.when(me != other)
        def _():
            pl.semaphore_signal(
                barrier, inc=1, device_id=(other // (ny * nz), other // nz % ny, other % nz), device_id_type=MESH
            )

    for a, (which, landed, halo) in enumerate(parts):
        for i in (0,) if a == 0 else (1, 2):
            turned[i] = given[i * LANES : (i + 1) * LANES].T
        if a == 0:
            pl.semaphore_wait(barrier, nx * ny * nz - 1)
        for to, exists, first, count, there, number in pieces(a):
            @pl.when(both(exists, to != slab))
            def _():
                piece(a, to, first, count, there, number).start()

            @pl.when(both(exists, to == slab))
            def _():
                landed[:, own_tile, there : there + count] = turned[which, first : first + count]

    @pl.when(works)
    def _():
        for ref in (va, vb, vz, ua, ub, r1in, e2, p_ref, dir_ref, q_ref, sq, rq, sq1, rq1, cq, w1):
            ref[...] = jnp.zeros_like(ref)
        w1[F_DG] = jnp.ones(w1.shape[1:], f32)
        for side, at in ((0, 0), (1, NS - 1)):
            @pl.when(slab == at)
            def _():
                for ref in (hb, he):
                    ref[:, side] = jnp.zeros(ref.shape[:1] + ref.shape[2:], f32)

    def wait_sent():
        for a in range(2):
            for to, exists, first, count, there, number in pieces(a):
                @pl.when(both(exists, to != slab))
                def _():
                    piece(a, to, first, count, there, number).wait_send()

    def wait_landed(a, wanted, kind, first, count, source):
        mine = jnp.where(source == iz, 1, 0)
        for own in range(2):
            @pl.when(jnp.logical_and(wanted, mine == own))
            def _():
                view = parts[a][1].at[:, pl.ds(0, P - own), pl.ds(first, count)]
                pltpu.make_async_copy(view, view, d_rsem.at[a, kind]).wait()

    def gather_block(a):
        for _, landed, halo in parts[a : a + 1]:
            @pl.when(slab == 0)
            def _():
                landed[:, :, :halo] = jnp.zeros((landed.shape[0], P, halo, LANES), f32)

            @pl.when(slab == NS - 1)
            def _():
                landed[:, :, halo + S :] = jnp.zeros((landed.shape[0], P, halo, LANES), f32)

            for jd in range(BLOCK):
                count = S + (halo if jd > 0 else 0) + (halo if jd < BLOCK - 1 else 0)
                wait_landed(a, j == jd, 0, 0 if jd > 0 else halo, count, block)
            wait_landed(a, jnp.logical_and(j == 0, has_lo), 1, 0, halo, block - 1)
            wait_landed(a, jnp.logical_and(j == BLOCK - 1, has_hi), 2, halo + S, halo, block + 1)
            for i, flat in ((0, f_it),) if a == 0 else ((0, f_rea), (1, f_src)):
                for at in range(0, S + 2 * halo, HALO):
                    tiles = block_transpose([landed[i, t, at : at + HALO] for t in range(P)])
                    for t in range(P):
                        flat[t, at : at + HALO] = tiles[t]

    def back_copy(which, t):
        return pltpu.make_async_remote_copy(
            src_ref=outs.at[which, t],
            dst_ref=back.at[which, pl.ds(pl.multiple_of(S * j, HALO), S)],
            send_sem=b_ssem.at[which],
            recv_sem=b_rsem.at[which],
            device_id=(t // ny, t % ny, block),
            device_id_type=MESH,
        )

    def back_here(which):
        @pl.when(block == iz)
        def _():
            back[which, pl.ds(pl.multiple_of(S * j, HALO), S)] = outs[which, own_tile]

    def energy_copy(dev):
        return pltpu.make_async_remote_copy(
            src_ref=enmsg, dst_ref=engath.at[slab],
            send_sem=g_ssem.at[5], recv_sem=g_rsem.at[5],
            device_id=dev, device_id_type=MESH,
        )

    WROWS = 4 * (X // 4) * (S // (4 * CHUNK))

    @pl.when(works)
    def _():
        gather_block(0)

        lanes = lane(W)
        z_at = slab * S + row(W) - HALO
        inside = jnp.logical_and(z_at >= 0, z_at < NZ)
        z_low = jnp.logical_and(z_at > 0, z_at < NZ)
        z_high = jnp.logical_and(z_at >= 0, z_at < NZ - 1)
        x_first, x_last = lanes < GY, lanes >= LANES - GY
        y_at = lax.rem(lanes, GY)
        y_first, y_last = y_at == 0, y_at == GY - 1

        def face(g):
            square = g * g
            one = 1.0 + square
            inverse = lax.rsqrt(one)
            return (one + square) * inverse, g * (one * inverse)

        def window(t):
            return f_it[t, HALO : HALO + W]

        low_w, low_p = face(window(0) - jnp.where(x_first, 0.0, roll(window(X - 1), GY, 1)))
        for t in range(X):
            c = window(t)
            beyond = window(t + 1) if t < X - 1 else jnp.where(x_last, 0.0, roll(window(0), -GY, 1))
            high_w, high_p = face(beyond - c)
            yl_w, yl_p = face(c - jnp.where(y_first, 0.0, roll(c, 1, 1)))
            yh_w, yh_p = face(jnp.where(y_last, 0.0, roll(c, -1, 1)) - c)
            zl_w, zl_p = face(c - f_it[t, HALO - 1 : HALO - 1 + W])
            zh_w, zh_p = face(f_it[t, HALO + 1 : HALO + 1 + W] - c)
            w0[F_DG, t] = low_w + high_w + yl_w + yh_w + zl_w + zh_w
            w0[F_XM, t] = jnp.where(x_first, 0.0, low_w) if t == 0 else low_w
            w0[F_XP, t] = jnp.where(x_last, 0.0, high_w) if t == X - 1 else high_w
            w0[F_YM, t] = jnp.where(y_first, 0.0, yl_w)
            w0[F_YP, t] = jnp.where(y_last, 0.0, yh_w)
            w0[F_ZM, t] = jnp.where(z_low, zl_w, 0.0)
            w0[F_ZP, t] = jnp.where(z_high, zh_w, 0.0)
            az[t] = (high_p - low_p) + (yh_p - yl_p) + (zh_p - zl_p)
            low_w, low_p = high_w, high_p

        gather_block(1)
        for t in range(X):
            rea = f_rea[t]
            diagonal = w0[F_DG, t] + rea
            w0[F_DG, t] = diagonal
            w0[F_INV, t] = 1.0 / diagonal
            r = jnp.where(inside, f_src[t] - rea * window(t) + az[t], 0.0)
            az[t] = r
            r_ref[t] = r

        def coarsen(get, step):
            def build(k):
                def both(field, t):
                    low, high = get(field, t)
                    return low + high
                lo, hi = 2 * k, 2 * k + 1
                xm = pair(both(F_XM, lo), step)
                ym_all = both(F_YM, lo) + both(F_YM, hi)
                zl0, zh0 = get(F_ZM, lo)
                zl1, zh1 = get(F_ZM, hi)
                between = pair(both(F_XM, hi), step) + pick_high(ym_all, step) + pair(zh0 + zh1, step)
                diagonal = pair(both(F_DG, lo) + both(F_DG, hi), step) - 2.0 * between
                return diagonal, xm, pick_low(ym_all, step), pair(zl0 + zl1, step)
            return build

        n1 = W // 2
        S1 = S // 2
        W1 = S1 + 2 * HALO
        T1 = X // 2
        at1 = (W1 - n1) // 2

        def halves0(field, t):
            return w0[field, t, pl.ds(0, n1, stride=2)], w0[field, t, pl.ds(1, n1, stride=2)]

        for k in range(T1):
            for field, value in zip((F_DG, F_XM, F_YM, F_ZM), coarsen(halves0, 1)(k)):
                w1[field, k, at1 : at1 + n1] = value

        def complete1():
            for k in range(T1):
                w1[F_INV, k] = 1.0 / w1[F_DG, k]
                w1[F_XP, k] = w1[F_XM, k + 1] if k < T1 - 1 else roll(w1[F_XM, 0], -GY, 1)
                w1[F_YP, k] = roll(w1[F_YM, k], -2, 1)
                w1[F_ZP, k] = roll(w1[F_ZM, k], -1, 0)

        complete1()

        S2 = S // 4
        T2 = X // 4
        LINES = S2 // CHUNK

        def halves1(field, t):
            return w1[field, t, pl.ds(HALO, S2, stride=2)], w1[field, t, pl.ds(HALO + 1, S2, stride=2)]

        own_chunk = lax.rem(lane(S2), CHUNK) == lax.rem(row(S2), CHUNK)

        def pack(ref, first, v):
            v = jnp.where(own_chunk, v, 0.0)
            for h in range(LINES):
                ref[first + h : first + h + 1] = jnp.sum(jnp.where(row(S2) // CHUNK == h, v, 0.0), axis=0, keepdims=True)

        for k in range(T2):
            for field, value in zip((F_DG, F_XM, F_YM, F_ZM), coarsen(halves1, 2)(k)):
                pack(wmsg, (field * T2 + k) * LINES, value)

        def sweep(w, v, step, use):
            T, n = w.shape[1], w.shape[2]
            for at in range(0, n, HALO):
                rows, shifted = slice(at, at + HALO), slice(at + HALO, at + 2 * HALO)
                c = [v[t, shifted] for t in range(T)]
                low = w[F_XM, 0, rows]
                for t in range(T):
                    below = c[t - 1] if t > 0 else roll(c[T - 1], GY, 1)
                    above = c[t + 1] if t < T - 1 else roll(c[0], -GY, 1)
                    high = w[F_XM, t + 1, rows] if t < T - 1 else w[F_XP, t, rows]
                    ym = w[F_YM, t, rows]
                    acc = w[F_DG, t, rows] * c[t] - low * below - high * above
                    acc = acc - ym * roll(c[t], step, 1) - roll(ym * c[t], -step, 1)
                    acc = acc - w[F_ZM, t, rows] * v[t, at + HALO - 1 : at + 2 * HALO - 1]
                    acc = acc - w[F_ZP, t, rows] * v[t, at + HALO + 1 : at + 2 * HALO + 1]
                    use(t, rows, shifted, c[t], acc)
                    low = high

        def before(w, r_of, u1, u2, rem1, s_out, r_out, step):
            T, n = w.shape[1], w.shape[2]
            for at in range(0, n, HALO):
                for t in range(T):
                    rows = slice(at, at + HALO)
                    u1[t, at + HALO : at + 2 * HALO] = w[F_INV, t, rows] * r_of[t, rows] * (1.0 / MID)

            def second(t, rows, shifted, first, image):
                r = r_of[t, rows] - image
                u = C_ONE * first + C_TWO * w[F_INV, t, rows] * r
                u2[t, shifted] = u
                s_out[t, rows] = first + u
                rem1[t, rows] = r

            def rest(t, rows, shifted, u, image):
                r_out[t, rows] = rem1[t, rows] - image

            sweep(w, u1, step, second)
            sweep(w, u2, step, rest)

        def after(w, e, u1, rem1, s_in, r_in, put, step):
            def first(t, rows, shifted, c, image):
                r = r_in[t, rows] - image
                rem1[t, rows] = r
                u1[t, shifted] = w[F_INV, t, rows] * r * (1.0 / MID)

            def second(t, rows, shifted, u, image):
                r = rem1[t, rows] - image
                put(t, rows, s_in[t, rows] + e[t, shifted] + (1.0 + C_ONE) * u + C_TWO * w[F_INV, t, rows] * r)

            sweep(w, e, step, first)
            sweep(w, u1, step, second)

        kept = ((az, sa, ra, sa1, ra1), (r_ref, sb, rb, sb1, rb1), (r_ref, sc, rc, sc1, rc1))

        def presmooth(f, ref, par):
            r_of, s_out, r_out, s1_out, r1_out = kept[f]
            before(w0, r_of, va, vb, rr, s_out, r_out, 1)
            for k in range(T1):
                total = None
                for t in (2 * k, 2 * k + 1):
                    part = r_out[t, pl.ds(0, n1, stride=2)] + r_out[t, pl.ds(1, n1, stride=2)]
                    total = part if total is None else total + part
                r1in[k, at1 : at1 + n1] = pair(total, 1)
            before(w1, r1in, ua, ub, rr1, s1_out, r1_out, 2)
            for k in range(T2):
                total = None
                for t in (2 * k, 2 * k + 1):
                    part = r1_out[t, pl.ds(HALO, S2, stride=2)] + r1_out[t, pl.ds(HALO + 1, S2, stride=2)]
                    total = part if total is None else total + part
                pack(ref.at[par], k * LINES, pair(total, 2))

        def to_workers(ref, out, sem):
            for s in range(NS):
                @pl.when(slab != s)
                def _():
                    pltpu.make_async_remote_copy(
                        src_ref=ref, dst_ref=out.at[slab], send_sem=g_ssem.at[sem], recv_sem=g_rsem.at[sem],
                        device_id=device_of(s), device_id_type=MESH,
                    ).start()
            out[slab] = ref[...]

        def from_workers(out, sem):
            others = out.at[pl.ds(0, NS - 1)]
            pltpu.make_async_copy(others, others, g_rsem.at[sem]).wait()
            pltpu.make_async_copy(others, others, g_ssem.at[sem]).wait()

        def unpack(out, packed):
            for k in range(T2):
                for s in range(NS):
                    out[k, s * LINES : (s + 1) * LINES] = packed[s, k * LINES : (k + 1) * LINES]

        per = 2 * (X + T1)
        halo_parts = tuple(
            ((of[3], 0, T1, S1), (of[4], T1, T1, S1), (of[1], 2 * T1, X, S), (of[2], 2 * T1 + X, X, S)) for of in kept
        )
        halo_at = (hb, he, he)

        def halo_send(f, par):
            for side, there, dev in ((0, has_lo, lo_dev), (1, has_hi, hi_dev)):
                @pl.when(there)
                def _():
                    for ref, first, count, size in halo_parts[f]:
                        start_row = HALO if side == 0 else size
                        pltpu.make_async_remote_copy(
                            src_ref=ref.at[:, pl.ds(start_row, HALO)],
                            dst_ref=halo_at[f].at[par, 1 - side, pl.ds(first, count)],
                            send_sem=h_ssem.at[2 * min(f, 1) + par, side],
                            recv_sem=h_rsem.at[2 * min(f, 1) + par, 1 - side],
                            device_id=dev,
                            device_id_type=MESH,
                        ).start()

        def halo_wait(view_of, sem):
            for side, there in ((0, has_lo), (1, has_hi)):
                @pl.when(there)
                def _():
                    view = view_of(side)
                    pltpu.make_async_copy(view, view, h_rsem.at[sem, side]).wait()
                    pltpu.make_async_copy(view, view, h_ssem.at[sem, side]).wait()

        chunk = lax.rem(lane(NS * LINES), CHUNK)

        def down2(v):
            return jnp.where(chunk == 0, roll(roll(v, 1 - CHUNK, 1), 1, 0), roll(v, 1, 1))

        def up2(v):
            return jnp.where(chunk == CHUNK - 1, roll(roll(v, CHUNK - 1, 1), -1, 0), roll(v, -1, 1))

        def down3(v):
            return jnp.where(chunk < CHUNK // 2, roll(roll(v, -(CHUNK // 2), 1), 1, 0), roll(v, CHUNK // 2, 1))

        def up3(v):
            return jnp.where(chunk >= CHUNK // 2, roll(roll(v, CHUNK // 2, 1), -1, 0), roll(v, -(CHUNK // 2), 1))

        def lap_all(w, vs, step, down, up):
            T = len(vs)
            out = []
            for t in range(T):
                v = vs[t]
                below = vs[t - 1] if t > 0 else roll(vs[T - 1], GY, 1)
                above = vs[t + 1] if t < T - 1 else roll(vs[0], -GY, 1)
                acc = w[F_DG, t] * v - w[F_XM, t] * below - w[F_XP, t] * above
                acc = acc - w[F_YM, t] * roll(v, step, 1) - w[F_YP, t] * roll(v, -step, 1)
                out.append(acc - w[F_ZM, t] * down(v) - w[F_ZP, t] * up(v))
            return out

        def complete_all(w, step, up):
            T = w.shape[1]
            for t in range(T):
                w[F_INV, t] = 1.0 / w[F_DG, t]
                w[F_XP, t] = w[F_XM, t + 1] if t < T - 1 else roll(w[F_XM, 0], -GY, 1)
                w[F_YP, t] = roll(w[F_YM, t], -step, 1)
                w[F_ZP, t] = up(w[F_ZM, t])

        def world():
            def apply2(v):
                return lap_all(w2, v, CHUNK, down2, up2)

            def apply3(v):
                return lap_all(w3, v, 2 * CHUNK, down3, up3)

            def scaled(w, r):
                return [w[F_INV, t] * r[t] for t in range(len(r))]

            def minus(a, b):
                return [x - y for x, y in zip(a, b)]

            def plus(*many):
                return [sum(vs[1:], vs[0]) for vs in zip(*many)]

            def first(w, r):
                return [d * (1.0 / MID) for d in scaled(w, r)]

            def follow(w, u, r, one, two):
                return [one * a + two * d for a, d in zip(u, scaled(w, r))]

            r = [cres[k] for k in range(T2)]
            u = first(w2, r)
            r = minus(r, apply2(u))
            u2 = follow(w2, u, r, C_ONE, C_TWO)
            total = plus(u, u2)
            r = minus(r, apply2(u2))
            rc = [pair(pair(r[0] + r[1], CHUNK), 1)]
            u = first(w3, rc)
            rc = minus(rc, apply3(u))
            v = follow(w3, u, rc, C_ONE, C_TWO)
            e = plus(u, v)
            rc = minus(rc, apply3(v))
            e = plus(e, follow(w3, v, rc, C_THREE, C_FOUR))
            e = [e[0]] * T2
            total = plus(total, e)
            r = minus(r, apply2(e))
            u = first(w2, r)
            r = minus(r, apply2(u))
            total = plus(total, u, follow(w2, u, r, C_ONE, C_TWO))
            for k in range(T2):
                e2[k, HALO : HALO + NS * LINES] = total[k]

        def precondition():
            own = lax.rem(lane(CHUNK), CHUNK) == row(CHUNK)
            for d in range(LINES + 2):
                for k in range(T2):
                    line = e2[k, pl.ds(slab * LINES + HALO - 1 + d, 1)]
                    v = jnp.where(own, jnp.broadcast_to(line, (CHUNK, LANES)), 0.0)
                    v = pair(pair(v, 1), 2)
                    for t in (2 * k, 2 * k + 1):
                        for half in range(2):
                            ua[t, pl.ds(HALO + 2 * CHUNK * d + half, CHUNK, stride=2)] = v

            def put1(k, rows, v):
                for t in (2 * k, 2 * k + 1):
                    for half in range(2):
                        va[t, pl.ds(2 * rows.start + half, HALO, stride=2)] = v

            def put0(t, rows, v):
                vz[t, rows.start + HALO : rows.stop + HALO] = v

            after(w1, ua, ub, rr1, s1, r1, put1, 2)
            after(w0, va, vb, rr, s0, r0, put0, 1)

        def total_of(v):
            return jnp.sum(jnp.sum(v, axis=0, keepdims=True), axis=1, keepdims=True)

        lane_1 = lane(1)

        def image_and_dots(par):
            sums = []

            def use(t, rows, shifted, z, image):
                az[t, rows] = image
                if HALO <= rows.start < HALO + S:
                    parts = (r_ref[t, rows] * z, z * image, z * q_ref[t, rows])
                    sums[:] = [a + b for a, b in zip(sums, parts)] if sums else parts

            sweep(w0, vz, 1, use)
            rz, zaz, zq = (total_of(v) for v in sums)
            msg[par, T2 * LINES :] = jnp.where(lane_1 == 0, rz, jnp.where(lane_1 == 1, zaz, zq))

        lane_1 = lane(1)

        def lane_of(v, i):
            return jnp.sum(jnp.where(lane_1 == i, v, 0.0), axis=1, keepdims=True)

        def scalars(par, rz_old, pq_old):
            sums = gath[par, 0, T2 * LINES :]
            for s in range(1, NS):
                sums = sums + gath[par, s, T2 * LINES :]
            rz, zaz, zq = lane_of(sums, 0), lane_of(sums, 1), lane_of(sums, 2)
            beta = rz / rz_old
            pq = zaz + 2.0 * beta * zq + beta * beta * pq_old
            return rz, pq, rz / pq, beta

        def advance(a, beta):
            for t in range(X):
                p = vz[t, HALO : HALO + HALO + S] + beta * p_ref[t]
                p_ref[t] = p
                dir_ref[t] = dir_ref[t] + a * p
                q = az[t] + beta * q_ref[t]
                q_ref[t] = q
                r_ref[t] = r_ref[t] - a * q

        def coarse_advance(par, a, beta, fresh):
            unpack(cnew, gath.at[par])
            if fresh:
                unpack(cres, egath.at[par])
            for k in range(T2):
                v = cnew[k] + beta * cq[k]
                cq[k] = v
                cres[k] = cres[k] - a * v

        def kept_advance(par, a, beta, fresh):
            for i, (keep, slope) in enumerate(((s1, sq1), (r1, rq1), (s0, sq), (r0, rq))):
                moved, first, count, size = halo_parts[0][i]
                true = halo_parts[1 + par][i][0]
                for t in range(count):
                    for side, rows in ((0, slice(0, HALO)), (None, slice(HALO, HALO + size)), (1, slice(HALO + size, 2 * HALO + size))):
                        got = moved[t, rows] if side is None else hb[par, side, first + t]
                        if a is None:
                            keep[t, rows] = got
                            continue
                        v = got + beta * slope[t, rows]
                        slope[t, rows] = v
                        if not fresh:
                            start = keep[t, rows]
                        else:
                            start = true[t, rows] if side is None else he[par, side, first + t]
                        keep[t, rows] = start - a * v

        for s in range(NS):
            @pl.when(slab != s)
            def _():
                pltpu.make_async_remote_copy(
                    src_ref=wmsg, dst_ref=wgath.at[pl.ds(pl.multiple_of(slab * WROWS, HALO), WROWS)],
                    send_sem=g_ssem.at[4], recv_sem=g_rsem.at[4], device_id=device_of(s), device_id_type=MESH,
                ).start()
        wgath[pl.ds(pl.multiple_of(slab * WROWS, HALO), WROWS)] = wmsg[...]
        for side, there, dev in ((0, has_lo, lo_dev), (1, has_hi, hi_dev)):
            @pl.when(there)
            def _():
                pltpu.make_async_remote_copy(
                    src_ref=w1.at[pl.ds(0, 4), :, pl.ds(HALO if side == 0 else S1, HALO)], dst_ref=sh.at[1 - side],
                    send_sem=h_ssem.at[4, side], recv_sem=h_rsem.at[4, 1 - side],
                    device_id=dev, device_id_type=MESH,
                ).start()
        presmooth(0, msg, 0)
        msg[0, T2 * LINES :] = jnp.zeros((1, LANES), f32)
        to_workers(msg.at[0], gath.at[0], 0)
        halo_send(0, 0)
        wait_sent()

        others = wgath.at[pl.ds(0, (NS - 1) * WROWS)]
        pltpu.make_async_copy(others, others, g_rsem.at[4]).wait()
        pltpu.make_async_copy(others, others, g_ssem.at[4]).wait()
        for field in range(4):
            for k in range(T2):
                for h in range(LINES):
                    line = (field * T2 + k) * LINES + h
                    w2[field, k, pl.ds(h, NS, stride=LINES)] = wgath[pl.ds(line, NS, stride=WROWS)]
        complete_all(w2, CHUNK, up2)
        dg, xm, ym, zm = F_DG, F_XM, F_YM, F_ZM
        ym_all = pair(w2[ym, 0] + w2[ym, 1], 1)
        zm_all = pair(w2[zm, 0] + w2[zm, 1], CHUNK)
        between = pair(pair(w2[xm, 1], CHUNK), 1) + pick_high(ym_all, CHUNK) + pick_high(zm_all, 1)
        w3[dg, 0] = pair(pair(w2[dg, 0] + w2[dg, 1], CHUNK), 1) - 2.0 * between
        w3[xm, 0] = pair(pair(w2[xm, 0], CHUNK), 1)
        w3[ym, 0] = pick_low(ym_all, CHUNK)
        w3[zm, 0] = pick_low(zm_all, 1)
        complete_all(w3, 2 * CHUNK, up3)
        halo_wait(lambda side: sh.at[side], 4)
        for side, there in ((0, has_lo), (1, has_hi)):
            @pl.when(there)
            def _():
                first = 0 if side == 0 else HALO + S1
                for field in range(4):
                    w1[field, :, first : first + HALO] = sh[side, field]
        complete1()
        from_workers(gath.at[0], 0)
        unpack(cres, gath.at[0])
        halo_wait(lambda side: hb.at[0, side], 0)
        kept_advance(0, None, None, False)

        rz, pq = jnp.ones((1, 1), f32), jnp.zeros((1, 1), f32)
        a = beta = None
        for it in range(ITERS):
            par, last, first = (it + 1) % 2, it == ITERS - 1, it == 0
            fresh = not (first or last)
            if fresh:
                presmooth(1 + par, early, par)
            world()
            if fresh:
                to_workers(early.at[par], egath.at[par], 2 + par)
                halo_send(1 + par, par)
            if not first:
                was = it % 2
                halo_wait(lambda side: hb.at[was, side], was)
                if it > 1:
                    halo_wait(lambda side: he.at[was, side], 2 + was)
                kept_advance(was, a, beta, it > 1)
            precondition()
            image_and_dots(par)
            if not last:
                presmooth(0, msg, par)
            to_workers(msg.at[par], gath.at[par], par)
            if not last:
                halo_send(0, par)
            from_workers(gath.at[par], par)
            rz, pq, a, beta = scalars(par, rz, pq)
            if fresh:
                from_workers(egath.at[par], 2 + par)
            if not last:
                coarse_advance(par, a, beta, fresh)
            advance(a, beta)

        def send_back(which):
            for at in range(0, S, HALO):
                ref = r_ref if which else dir_ref
                tiles = block_transpose([ref[t, HALO + at : 2 * HALO + at] for t in range(X)])
                for t in range(X):
                    outs[which, t, at : at + HALO] = tiles[t]
            for t in range(P):
                remote = jnp.logical_or(block != iz, own_tile != t)

                @pl.when(remote)
                def _():
                    back_copy(which, t).start()
            back_here(which)

        send_back(1)

        def energy(g):
            square = 1.0 + g * g
            return (square * (square * lax.rsqrt(square)) - 1.0) * (1.0 / 3.0)

        lanes = lane(S)
        y_at = lax.rem(lanes, GY)
        x_first, x_last, y_first = lanes < GY, lanes >= LANES - GY, y_at == 0
        ends = jnp.where(y_at == GY - 1, 1.0, 0.0) + jnp.where(slab * S + row(S) == NZ - 1, 1.0, 0.0)
        ends_x = ends + jnp.where(x_last, 1.0, 0.0)
        fetch = lax.rem(lane_1, GY)
        for k in range(TRIALS):
            s = jnp.exp2(-jnp.full((1, LANES), tp_ref[k], jnp.int32).astype(f32))

            def trial(t, shift):
                first = 2 * HALO - shift
                return f_it[t, first : first + S] + s * dir_ref[t, HALO - shift : HALO - shift + S]

            below = jnp.where(x_first, 0.0, roll(trial(X - 1, 0), GY, 1))
            for t in range(X):
                v = trial(t, 0)
                e = energy(v - below) + energy(v - trial(t, 1))
                e = e + energy(v - jnp.where(y_first, 0.0, roll(v, 1, 1)))
                e = e + energy(v) * (ends_x if t == X - 1 else ends)
                e = e + (0.5 * f_rea[t, HALO : HALO + S] * v - f_src[t, HALO : HALO + S]) * v
                columns[k * X + t : k * X + t + 1] = jnp.sum(e, axis=0, keepdims=True)
                below = v
        over_y = columns[...]
        step = 1
        while step < GY:
            over_y = pair(over_y, step)
            step *= 2
        chosen = lax.rem(lane(TRIALS * X), GY) == row(TRIALS * X)
        packed = jnp.sum(jnp.where(chosen, over_y, 0.0), axis=0, keepdims=True)
        enmsg[...] = packed
        engath[slab] = packed
        for other in range(nx * ny * nz):
            @pl.when(me != other)
            def _():
                energy_copy((other // (ny * nz), other // nz % ny, other % nz)).start()
        send_back(0)

    @pl.when(jnp.logical_not(works))
    def _():
        wait_sent()

    for which in (1, 0):
        for own in range(2):
            @pl.when(jnp.where(block == iz, 1, 0) == own)
            def _():
                view = back.at[which, pl.ds(0, Z - own * S)]
                pltpu.make_async_copy(view, view, b_rsem.at[which]).wait()
        fields_out[which] = back[which].T.reshape(X, Y, Z)
    @pl.when(works)
    def _():
        others = engath.at[pl.ds(0, NS - 1)]
        pltpu.make_async_copy(others, others, g_rsem.at[5]).wait()
        sent = counted.at[pl.ds(0, nx * ny * nz - 1)]
        pltpu.make_async_copy(sent, sent, g_ssem.at[5]).wait()
        for which in range(2):
            for own in range(2):
                @pl.when(jnp.where(block == iz, 1, 0) == own)
                def _():
                    sent = outs.at[which, pl.ds(0, P - own)]
                    pltpu.make_async_copy(sent, sent, b_ssem.at[which]).wait()

    @pl.when(jnp.logical_not(works))
    def _():
        pltpu.make_async_copy(engath, engath, g_rsem.at[5]).wait()

    lane_1 = lane(1)
    fetch = lax.rem(lane_1, GY)
    layers = jnp.sum(engath[...], axis=0) / (GY * NZ)
    here = jnp.where(lane_1 // GY == ix, layers, 0.0)
    at_k = lax.broadcasted_iota(jnp.int32, (TRIALS * X, LANES), 0)
    mine = jnp.sum(jnp.where(lax.rem(lane(TRIALS * X), GY) == at_k, here, 0.0), axis=1, keepdims=True)
    mine = jnp.where(lane(TRIALS * X) == lax.rem(at_k, X), mine, 0.0)
    for k in range(TRIALS):
        sums_out[k : k + 1] = jnp.sum(mine[k * X : k * X + X], axis=0, keepdims=True)
        total = jnp.sum(jnp.where(fetch // X == k, layers, 0.0), axis=1, keepdims=True) / (X * nx)
        sums_out[TRIALS + k : TRIALS + k + 1] = jnp.broadcast_to(total, (1, LANES))


def hand_out(fields, sums, dir_out, rem_out, le_out, en_out, le, en, sem):
    copies = [pltpu.make_async_copy(fields.at[i], out, sem.at[i]) for i, out in ((0, dir_out), (1, rem_out))]
    for copy in copies:
        copy.start()
    le[...] = sums[:TRIALS, : le.shape[1]]
    for k in range(TRIALS):
        en[k] = jnp.max(sums[TRIALS + k : TRIALS + k + 1])
    copies += [pltpu.make_async_copy(le, le_out, sem.at[2]), pltpu.make_async_copy(en, en_out, sem.at[3])]
    for copy in copies[2:]:
        copy.start()
    for copy in copies:
        copy.wait()


def slab_on_device(counts, iterate, source, reaction, trial_powers):
    X, Y, Z = iterate.shape
    nx, ny, nz = counts
    P = nx * ny
    NS = PLANES * ny * nz
    S = nz * Z // NS
    BLOCK = Z // S
    W, W1 = S + 2 * HALO, S // 2 + 2 * HALO
    T1, T2, T3 = X // 2, X // 4, X // 8
    LINES = S // (4 * CHUNK)
    C_ROWS, ROWS = T2 * LINES, NS * LINES
    f32 = jnp.float32

    def vm(*shape):
        return pltpu.VMEM(shape, f32)

    def sem(*shape):
        return pltpu.SemaphoreType.DMA(shape)

    full, padded = (X, W, LANES), (X, W + 2 * HALO, LANES)
    full1, padded1 = (T1, W1, LANES), (T1, W1 + 2 * HALO, LANES)
    scratch = [vm(3, Z, LANES), vm(1, P, W + 2 * HALO, LANES), vm(2, P, W, LANES)]
    scratch += [vm(*padded), vm(*full), vm(*full)]
    scratch += [vm(8, *full), vm(8, *full1), vm(8, T2, ROWS, LANES), vm(8, T3, ROWS, LANES)]
    scratch += [vm(*padded)] * 3 + [vm(*full)] * 12
    scratch += [vm(*padded1)] * 2 + [vm(*full1)] * 12
    scratch += [vm(T2, ROWS + 2 * HALO, LANES)] + [vm(T2, ROWS, LANES)] * 3
    scratch += [vm(X, S + HALO, LANES)] * 2 + [vm(*full)] * 2
    scratch += [vm(2, C_ROWS + 1, LANES), vm(2, NS, C_ROWS + 1, LANES), vm(2, C_ROWS, LANES), vm(2, NS, C_ROWS, LANES)]
    scratch += [vm(4 * C_ROWS, LANES), vm(NS * 4 * C_ROWS, LANES)]
    scratch += [vm(2, 2, 2 * (X + T1), HALO, LANES)] * 2 + [vm(2, 4, T1, HALO, LANES)]
    scratch += [vm(1, LANES), vm(NS, 1, LANES), vm(2, P, S, LANES), vm(2, Z, LANES)]
    scratch += [sem(2, BLOCK + 2), sem(2, 3), sem(6), sem(6), sem(5, 2), sem(5, 2), sem(2), sem(2), vm(nx * ny * nz, 1, LANES), vm(TRIALS * X, LANES)]
    whole = pl.BlockSpec(memory_space=pltpu.VMEM)
    given = jnp.concatenate([v.reshape(LANES, Z) for v in (iterate, reaction, source)])
    fields, sums = pl.pallas_call(
        functools.partial(slab_kernel, (X, Y, Z), counts),
        out_shape=[jax.ShapeDtypeStruct((2, X, Y, Z), f32), jax.ShapeDtypeStruct((2 * TRIALS, LANES), f32)],
        in_specs=[pl.BlockSpec(memory_space=pltpu.SMEM), whole],
        out_specs=[whole] * 2,
        scratch_shapes=scratch,
        compiler_params=pltpu.CompilerParams(
            has_side_effects=True, collective_id=0, vmem_limit_bytes=32 * 1024 * 1024
        ),
        name="newton_step",
    )(trial_powers, given)
    return pl.pallas_call(
        hand_out,
        out_shape=[
            jax.ShapeDtypeStruct((X, Y, Z), f32),
            jax.ShapeDtypeStruct((X, Y, Z), f32),
            jax.ShapeDtypeStruct((TRIALS, X), f32),
            jax.ShapeDtypeStruct((TRIALS,), f32),
        ],
        in_specs=[whole] * 2,
        out_specs=[pl.BlockSpec(memory_space=pl.ANY)] * 4,
        scratch_shapes=[vm(TRIALS, X), pltpu.SMEM((TRIALS,), f32), sem(4)],
        compiler_params=pltpu.CompilerParams(vmem_limit_bytes=32 * 1024 * 1024),
        name="hand_out",
    )(fields, sums)


def solution(mesh):
    counts = tuple(mesh.shape[axis] for axis in ("gx", "gy", "gz"))
    grid = P("gx", "gy", "gz")

    def on_each(iterate, source, reaction, trial_powers):
        form = slab_on_device if slab_fits(counts, iterate.shape) else on_device
        return form(counts, iterate, source, reaction, trial_powers)

    return jax.shard_map(
        on_each,
        mesh=mesh,
        in_specs=(grid, grid, grid, P()),
        out_specs=(grid, grid, P(None, "gx"), P()),
        check_vma=False,
    )
```
